32 devices in a mesh: dp: 2 (over y), row: 4 (over x, core), col: 4 (over z).
Axes of the slice: x: 2, y: 2, z: 4, core: 2. Of those that a mesh axis runs over, the one named last changes fastest.
Arguments:
- inputs: bfloat16 [2, 8192, 1024], P('dp', None, ('row', 'col')), may hold values from -6 to 6
- segments: int32 [2, 8192], P('dp'), may hold values from 0 to 7, never falling along the last dimension, each value on 1 to 2000 neighbouring positions
- cotangent: bfloat16 [2, 8192, 1024], P('dp', None, ('row', 'col')), may hold values from -6 to 6
- pregain: bfloat16 [1024], P(('row', 'col')), may hold values from 0.5 to 1.5
- innerweight: bfloat16 [1024, 32, 128], P('row', 'col'), may hold values from -0.1875 to 0.1875
- rateweight: bfloat16 [1024, 32], P('row', 'col'), may hold values from -0.1875 to 0.1875
- stateweight: bfloat16 [1024, 256], P(('row', 'col')), may hold values from -0.1875 to 0.1875
- innerconv: bfloat16 [5, 32, 64], P(None, ('col', 'row')), may hold values from -3 to 3
- stateconv: bfloat16 [5, 256], replicated, may hold values from -3 to 3
- headparams: bfloat16 [3, 32], P(None, ('col', 'row')), may hold values from -6.91 to 2.5, as said below
- postgain: bfloat16 [32, 64], P(('col', 'row')), may hold values from 0.5 to 1.5
- outweight: bfloat16 [32, 64, 1024], P('col', None, 'row'), may hold values from -0.125 to 0.125
- moment_pregain: float32 [1024], P(('row', 'col')), may hold values from -640 to 640
- square_pregain: float32 [1024], P(('row', 'col')), may hold values from 2500 to 40000
- moment_innerweight: float32 [1024, 32, 128], P('row', 'col'), may hold values from -640 to 640
- square_innerweight: float32 [1024, 32, 128], P('row', 'col'), may hold values from 2500 to 40000
- moment_rateweight: float32 [1024, 32], P('row', 'col'), may hold values from -640 to 640
- square_rateweight: float32 [1024, 32], P('row', 'col'), may hold values from 2500 to 40000
- moment_stateweight: float32 [1024, 256], P(('row', 'col')), may hold values from -640 to 640
- square_stateweight: float32 [1024, 256], P(('row', 'col')), may hold values from 2500 to 40000
- moment_innerconv: float32 [5, 32, 64], P(None, ('col', 'row')), may hold values from -640 to 640
- square_innerconv: float32 [5, 32, 64], P(None, ('col', 'row')), may hold values from 2500 to 40000
- moment_stateconv: float32 [5, 256], replicated, may hold values from -640 to 640
- square_stateconv: float32 [5, 256], replicated, may hold values from 2500 to 40000
- moment_headparams: float32 [3, 32], P(None, ('col', 'row')), may hold values from -1792 to 1792
- square_headparams: float32 [3, 32], P(None, ('col', 'row')), may hold values from 22500 to 360000
- moment_postgain: float32 [32, 64], P(('col', 'row')), may hold values from -640 to 640
- square_postgain: float32 [32, 64], P(('col', 'row')), may hold values from 2500 to 40000
- moment_outweight: float32 [32, 64, 1024], P('col', None, 'row'), may hold values from -896 to 896
- square_outweight: float32 [32, 64, 1024], P('col', None, 'row'), may hold values from 5600 to 90000
Outputs:
- result: float32 [2, 8192, 1024], P('dp', None, ('row', 'col'))
- grad_input: float32 [2, 8192, 1024], P('dp', None, ('row', 'col'))
- grad_pregain: float32 [1024], P(('row', 'col'))
- first_pregain: float32 [1024], P(('row', 'col'))
- second_pregain: float32 [1024], P(('row', 'col'))
- delta_pregain: float32 [1024], P(('row', 'col'))
- grad_innerweight: float32 [1024, 32, 128], P('row', 'col')
- first_innerweight: float32 [1024, 32, 128], P('row', 'col')
- second_innerweight: float32 [1024, 32, 128], P('row', 'col')
- delta_innerweight: float32 [1024, 32, 128], P('row', 'col')
- grad_rateweight: float32 [1024, 32], P('row', 'col')
- first_rateweight: float32 [1024, 32], P('row', 'col')
- second_rateweight: float32 [1024, 32], P('row', 'col')
- delta_rateweight: float32 [1024, 32], P('row', 'col')
- grad_stateweight: float32 [1024, 256], P(('row', 'col'))
- first_stateweight: float32 [1024, 256], P(('row', 'col'))
- second_stateweight: float32 [1024, 256], P(('row', 'col'))
- delta_stateweight: float32 [1024, 256], P(('row', 'col'))
- grad_innerconv: float32 [5, 32, 64], P(None, ('col', 'row'))
- first_innerconv: float32 [5, 32, 64], P(None, ('col', 'row'))
- second_innerconv: float32 [5, 32, 64], P(None, ('col', 'row'))
- delta_innerconv: float32 [5, 32, 64], P(None, ('col', 'row'))
- grad_stateconv: float32 [5, 256], replicated
- first_stateconv: float32 [5, 256], replicated
- second_stateconv: float32 [5, 256], replicated
- delta_stateconv: float32 [5, 256], replicated
- grad_headparams: float32 [3, 32], P(None, ('col', 'row'))
- first_headparams: float32 [3, 32], P(None, ('col', 'row'))
- second_headparams: float32 [3, 32], P(None, ('col', 'row'))
- delta_headparams: float32 [3, 32], P(None, ('col', 'row'))
- grad_postgain: float32 [32, 64], P(('col', 'row'))
- first_postgain: float32 [32, 64], P(('col', 'row'))
- second_postgain: float32 [32, 64], P(('col', 'row'))
- delta_postgain: float32 [32, 64], P(('col', 'row'))
- grad_outweight: float32 [32, 64, 1024], P('col', None, 'row')
- first_outweight: float32 [32, 64, 1024], P('col', None, 'row')
- second_outweight: float32 [32, 64, 1024], P('col', None, 'row')
- delta_outweight: float32 [32, 64, 1024], P('col', None, 'row')
The draws below stay inside these ranges and needn't reach their ends.
Inputs may be any that keep to these rules, and one draw needn't show every extreme that they name: `segments`: in every sequence the document numbers never fall; each of the 8 documents holds 1 to 2000 tokens and one holds exactly 2000. `headparams`: row 0 lies in 0 to 2.5, row 1 in -6.91 to -2.25, row 2 in 0.5 to 1.5.
All inputs are finite; a program needn't handle non-finite values.
Results may differ from the reference program's by a relative error of at most 0.01.
Values may be sent and summed in bfloat16 or wider, within the bound.
A program may use at most 320 MiB of HBM per device.

```python
import math
import jax
import jax.numpy as jnp
import numpy as np
from jax import lax

D = 1024
HEADS = 32
HEADP = 64
STATE = 128
TAPS = 4
GROUP = 256
LENGTH = 8192
DOCS = 8
MOST = 2000
STEP = 4
SEQUENCES = 2


def draw_headparams(key, part):
    key_decay, key_rate, key_skip = jax.random.split(key, 3)
    log_rates = jax.random.uniform(key_decay, (HEADS,), jnp.float32, 0.0, 2.5)
    step_sizes = jnp.exp(jax.random.uniform(key_rate, (HEADS,), jnp.float32, math.log(0.001), math.log(0.1)))
    offsets = jnp.log(jnp.expm1(step_sizes))
    skip_gains = jax.random.uniform(key_skip, (HEADS,), jnp.float32, 0.5, 1.5)
    return jnp.stack([log_rates, offsets, skip_gains]).astype(jnp.bfloat16)


def level_of(own_key, dims, cuts, smallest, top_value):
    factor_of, own = 1.0, jax.random.fold_in(own_key, 6)
    for dim, shards_of in cuts:
        heights = jnp.exp(jax.random.uniform(jax.random.fold_in(own, dim), (shards_of,), jnp.float32, smallest / len(cuts), top_value / len(cuts)))
        factor_of = factor_of * jnp.repeat(heights, dims[dim] // shards_of).reshape([-1 if axis == dim else 1 for axis in range(len(dims))])
    return factor_of


def split_up(count, total, bound, lean):
    portions = [(1 << 20) // math.isqrt(rank ** lean) + 1 for rank in range(2, count + 1)]
    surplus, given = total - bound - (count - 1), [1] * (count - 1)
    while surplus > 0:
        candidates = [i for i in range(count - 1) if given[i] < bound]
        pool, budget = sum([portions[i] for i in candidates]), surplus
        for i in candidates:
            more = min(bound - given[i], max(1, budget * portions[i] // pool), surplus)
            given[i] = given[i] + more
            surplus = surplus - more
    return np.array([bound] + given)


def uneven(own_key, number_of, total, most, slope):
    if number_of == 2:
        one = jax.random.randint(own_key, (), max(1, total - most), min(most, total - 1) + 1)
        return jnp.stack([one, total - one])
    lengths = jnp.asarray(split_up(number_of, total, most, slope), jnp.int32)
    couples = (number_of - 1) // 2
    donor, receiver = lengths[1:1 + 2 * couples:2], lengths[2:2 + 2 * couples:2]
    room = jnp.minimum(donor - 1, most - receiver)
    passed = jax.random.randint(jax.random.fold_in(own_key, 1), (couples,), 0, 1 << 20) % (room + 1)
    lengths = lengths.at[1:1 + 2 * couples:2].set(donor - passed).at[2:2 + 2 * couples:2].set(receiver + passed)
    return lengths[jax.random.permutation(jax.random.fold_in(own_key, 2), number_of)]


def centred(rng, extent, deviation, bound, shards=(), kind=jnp.bfloat16):
    factor_of = level_of(rng, extent, shards, -0.22, 0.18) if shards else 1.0
    entries = jax.random.normal(rng, extent, jnp.float32) * deviation * factor_of
    return jnp.minimum(jnp.maximum(entries, -bound), bound).astype(kind)


def setup_inputs(seed: int = 0) -> dict:
    key_of = jax.random.split(jax.random.key(seed), 31)
    inputs = centred(key_of[0], (SEQUENCES, LENGTH, D), 1.0, 6.0, ((0, 2), (2, 16)))
    segments = jax.vmap(lambda own: jnp.searchsorted(jnp.cumsum(uneven(own, DOCS, LENGTH, MOST, 1)), jnp.arange(LENGTH), side="right"))(jax.random.split(key_of[1], SEQUENCES)).reshape((SEQUENCES, LENGTH)).astype(jnp.int32)
    cotangent = centred(key_of[2], (SEQUENCES, LENGTH, D), 1.0, 6.0, ((0, 2), (2, 16)))
    pregain = jnp.clip(1.0 + 0.1 * jax.random.normal(key_of[3], (D,), jnp.float32), 0.5, 1.5).astype(jnp.bfloat16)
    innerweight = centred(key_of[4], (D, HEADS, 2 * HEADP), D ** -0.5, 0.1875, ((0, 4), (1, 4)))
    rateweight = centred(key_of[5], (D, HEADS), D ** -0.5, 0.1875, ((0, 4), (1, 4)))
    stateweight = centred(key_of[6], (D, 2 * STATE), D ** -0.5, 0.1875, ((0, 16),))
    innerconv = centred(key_of[7], (TAPS + 1, HEADS, HEADP), 0.5, 3.0, ((1, 16),))
    stateconv = centred(key_of[8], (TAPS + 1, 2 * STATE), 0.5, 3.0)
    headparams = draw_headparams(jax.random.fold_in(key_of[30], 71), 0)
    postgain = jnp.clip(1.0 + 0.1 * jax.random.normal(key_of[10], (HEADS, HEADP), jnp.float32), 0.5, 1.5).astype(jnp.bfloat16)
    outweight = centred(key_of[11], (HEADS, HEADP, D), (HEADS * HEADP) ** -0.5, 0.125, ((0, 4), (2, 4)))
    moment_pregain = centred(key_of[12], (D,), 100.0, 640.0, ((0, 16),), jnp.float32)
    square_pregain = jnp.clip(jnp.exp(math.log(40000.0) - 2.7725887 * jax.random.uniform(key_of[13], (D,), jnp.float32) ** level_of(key_of[13], (D,), ((0, 16),), -0.2, 0.2)), 2500.0, 40000.0)
    moment_innerweight = centred(key_of[14], (D, HEADS, 2 * HEADP), 100.0, 640.0, ((0, 4), (1, 4)), jnp.float32)
    square_innerweight = jnp.clip(jnp.exp(math.log(40000.0) - 2.7725887 * jax.random.uniform(key_of[15], (D, HEADS, 2 * HEADP), jnp.float32) ** level_of(key_of[15], (D, HEADS, 2 * HEADP), ((0, 4), (1, 4)), -0.2, 0.2)), 2500.0, 40000.0)
    moment_rateweight = centred(key_of[16], (D, HEADS), 100.0, 640.0, ((0, 4), (1, 4)), jnp.float32)
    square_rateweight = jnp.clip(jnp.exp(math.log(40000.0) - 2.7725887 * jax.random.uniform(key_of[17], (D, HEADS), jnp.float32) ** level_of(key_of[17], (D, HEADS), ((0, 4), (1, 4)), -0.2, 0.2)), 2500.0, 40000.0)
    moment_stateweight = centred(key_of[18], (D, 2 * STATE), 100.0, 640.0, ((0, 16),), jnp.float32)
    square_stateweight = jnp.clip(jnp.exp(math.log(40000.0) - 2.7725887 * jax.random.uniform(key_of[19], (D, 2 * STATE), jnp.float32) ** level_of(key_of[19], (D, 2 * STATE), ((0, 16),), -0.2, 0.2)), 2500.0, 40000.0)
    moment_innerconv = centred(key_of[20], (TAPS + 1, HEADS, HEADP), 100.0, 640.0, ((1, 16),), jnp.float32)
    square_innerconv = jnp.clip(jnp.exp(math.log(40000.0) - 2.7725887 * jax.random.uniform(key_of[21], (TAPS + 1, HEADS, HEADP), jnp.float32) ** level_of(key_of[21], (TAPS + 1, HEADS, HEADP), ((1, 16),), -0.2, 0.2)), 2500.0, 40000.0)
    moment_stateconv = centred(key_of[22], (TAPS + 1, 2 * STATE), 100.0, 640.0, (), jnp.float32)
    square_stateconv = jnp.clip(jnp.exp(jax.random.uniform(key_of[23], (TAPS + 1, 2 * STATE), jnp.float32, math.log(2500.0), math.log(40000.0))), 2500.0, 40000.0)
    moment_headparams = centred(key_of[24], (3, HEADS), 300.0, 1792.0, ((1, 16),), jnp.float32)
    square_headparams = jnp.clip(jnp.exp(math.log(360000.0) - 2.7725887 * jax.random.uniform(key_of[25], (3, HEADS), jnp.float32) ** level_of(key_of[25], (3, HEADS), ((1, 16),), -0.2, 0.2)), 22500.0, 360000.0)
    moment_postgain = centred(key_of[26], (HEADS, HEADP), 100.0, 640.0, ((0, 16),), jnp.float32)
    square_postgain = jnp.clip(jnp.exp(math.log(40000.0) - 2.7725887 * jax.random.uniform(key_of[27], (HEADS, HEADP), jnp.float32) ** level_of(key_of[27], (HEADS, HEADP), ((0, 16),), -0.2, 0.2)), 2500.0, 40000.0)
    moment_outweight = centred(key_of[28], (HEADS, HEADP, D), 150.0, 896.0, ((0, 4), (2, 4)), jnp.float32)
    square_outweight = jnp.clip(jnp.exp(math.log(90000.0) - 2.777043 * jax.random.uniform(key_of[29], (HEADS, HEADP, D), jnp.float32) ** level_of(key_of[29], (HEADS, HEADP, D), ((0, 4), (2, 4)), -0.2, 0.2)), 5600.0, 90000.0)
    return {"inputs": inputs, "segments": segments, "cotangent": cotangent, "pregain": pregain, "innerweight": innerweight, "rateweight": rateweight, "stateweight": stateweight, "innerconv": innerconv, "stateconv": stateconv, "headparams": headparams, "postgain": postgain, "outweight": outweight, "moment_pregain": moment_pregain, "square_pregain": square_pregain, "moment_innerweight": moment_innerweight, "square_innerweight": square_innerweight, "moment_rateweight": moment_rateweight, "square_rateweight": square_rateweight, "moment_stateweight": moment_stateweight, "square_stateweight": square_stateweight, "moment_innerconv": moment_innerconv, "square_innerconv": square_innerconv, "moment_stateconv": moment_stateconv, "square_stateconv": square_stateconv, "moment_headparams": moment_headparams, "square_headparams": square_headparams, "moment_postgain": moment_postgain, "square_postgain": square_postgain, "moment_outweight": moment_outweight, "square_outweight": square_outweight}


EXACT_PRECISION = lax.Precision.HIGHEST
NORM_EPSILON = 1e-05
ADAM_EPSILON = 1e-08
BETA_FIRST = 0.5
BETA_SECOND = 0.5
LEARN_RATE = 0.02
WEIGHT_DECAY = 0.1

@jax.custom_vjp
def low(v):
    return lax.optimization_barrier(v.astype(jnp.bfloat16)).astype(jnp.float32)

@jax.custom_vjp
def lowpass_backward(v):
    return v

def low_keep(v):
    return (low(v), None)

def low_pass(kept, grad):
    return (grad,)

def back_keep(v):
    return (v, None)

def back_low(kept, grad):
    return (low(grad),)
low.defvjp(low_keep, low_pass)
lowpass_backward.defvjp(back_keep, back_low)

def shifted(values, offset):
    padding = jnp.zeros_like(values[:, :offset])
    return jnp.concatenate([padding, values[:, :-offset]], axis=1)

def conv_mix(values, kernel, segments):
    extra = (1,) * (values.ndim - 2)
    last_row = kernel.shape[0] - 1
    total = values * kernel[0] + kernel[last_row]
    for offset in range(1, last_row):
        earlier = shifted(values, offset)
        seg_prev = jnp.concatenate([jnp.full_like(segments[:, :offset], -1), segments[:, :-offset]], axis=1)
        same_doc = (seg_prev == segments).reshape(segments.shape + extra)
        total = total + jnp.where(same_doc, earlier, 0.0) * kernel[offset]
    return total

def scan_sequence(pieces):
    values, rates, log_decay, bvalues, cvalues, segrow = pieces
    length = values.shape[0]
    head_count = values.shape[1]
    head_width = values.shape[2]
    nstate = bvalues.shape[1]
    blocks = length // GROUP
    blocked = values.reshape(blocks, GROUP, head_count, head_width)
    rate_blocks = rates.reshape(blocks, GROUP, head_count)
    cumulative = jnp.cumsum(log_decay.reshape(blocks, GROUP, head_count), axis=1)
    bblocks = bvalues.reshape(blocks, GROUP, nstate)
    cblocks = cvalues.reshape(blocks, GROUP, nstate)
    seg_blocks = segrow.reshape(blocks, GROUP)
    rowpos = lax.broadcasted_iota(jnp.int32, (GROUP, GROUP), 0)
    colpos = lax.broadcasted_iota(jnp.int32, (GROUP, GROUP), 1)
    same_doc = (seg_blocks[:, :, None] == seg_blocks[:, None, :]) & (colpos <= rowpos)
    cum_heads = jnp.swapaxes(cumulative, 1, 2)
    differ = cum_heads[:, :, :, None] - cum_heads[:, :, None, :]
    doc_mask = same_doc[:, None]
    decays = jnp.where(doc_mask, jnp.exp(jnp.where(doc_mask, differ, 0.0)), 0.0)
    scores = jnp.einsum('btn,bsn->bts', cblocks, bblocks, precision=EXACT_PRECISION)
    weights = scores[:, None] * decays * jnp.swapaxes(rate_blocks, 1, 2)[:, :, None, :]
    inner_out = jnp.einsum('bhts,bshp->bthp', weights, blocked, precision=EXACT_PRECISION)
    last_cum = cumulative[:, -1]
    last_seg = seg_blocks[:, -1]
    to_end = jnp.exp(last_cum[:, None, :] - cumulative) * (seg_blocks == last_seg[:, None])[:, :, None] * rate_blocks
    local_state = jnp.einsum('bsh,bsn,bshp->bhnp', to_end, bblocks, blocked, precision=EXACT_PRECISION)
    prev_seg = jnp.concatenate([jnp.full((1,), -1, jnp.int32), last_seg[:-1].astype(jnp.int32)])
    carry_gain = jnp.where((last_seg == prev_seg)[:, None], jnp.exp(last_cum), 0.0)

    def advance(carried, parts):
        gain_now, local_now = parts
        return (gain_now[:, None, None] * carried + local_now, carried)
    start = jnp.zeros((head_count, nstate, head_width), values.dtype)
    _, entering = lax.scan(advance, start, (carry_gain, local_state))
    keep_tok = seg_blocks == prev_seg[:, None]
    factor = jnp.where(keep_tok[:, :, None], jnp.exp(cumulative), 0.0)
    outer_out = jnp.einsum('btn,bhnp->bthp', cblocks, entering, precision=EXACT_PRECISION) * factor[..., None]
    return (inner_out + outer_out).reshape(length, head_count, head_width)

def mixer(innerproj, ratein, statein, innerconv, stateconv, headparams, segments):
    half = innerproj.shape[-1] // 2
    gatez = innerproj[..., :half]
    preact = innerproj[..., half:]
    values = jax.nn.silu(conv_mix(preact, innerconv, segments))
    states = jax.nn.silu(conv_mix(statein, stateconv, segments))
    nstate = states.shape[-1] // 2
    bvalues = states[..., :nstate]
    cvalues = states[..., nstate:]
    rates = jax.nn.softplus(ratein + headparams[1])
    log_decay = -jnp.exp(headparams[0]) * rates
    scanned = lax.map(jax.checkpoint(scan_sequence), (values, rates, log_decay, bvalues, cvalues, segments))
    mixed = scanned + headparams[2][:, None] * values
    return mixed * jax.nn.silu(gatez)

def forward(inputs, pregain, innerweight, rateweight, stateweight, innerconv, stateconv, headparams, postgain, outweight, segments):
    normalized_rows = low(inputs * pregain)
    rootinv = lax.rsqrt(lax.optimization_barrier(jnp.sum(inputs * inputs, axis=-1)) / D + NORM_EPSILON)
    inner_unprocessed = lowpass_backward(jnp.einsum('yjz,zxa->yjxa', normalized_rows, innerweight, precision=EXACT_PRECISION))
    rate_unprocessed = lowpass_backward(jnp.einsum('jvo,og->jvg', normalized_rows, rateweight, precision=EXACT_PRECISION))
    state_unprocessed = lowpass_backward(jnp.einsum('jph,hv->jpv', normalized_rows, stateweight, precision=EXACT_PRECISION))
    innerproj = rootinv[..., None, None] * inner_unprocessed
    ratein = rootinv[..., None] * rate_unprocessed
    statein = low(rootinv[..., None] * state_unprocessed)
    gated = mixer(innerproj, ratein, statein, innerconv, stateconv, headparams, segments)
    count = gated.shape[2] * gated.shape[3]
    rootgate = lax.rsqrt(lax.optimization_barrier(jnp.sum(gated * gated, axis=(2, 3))) / count + NORM_EPSILON)
    norm_output_rows = low(gated * rootgate[..., None, None] * postgain)
    return inputs + jnp.einsum('ktmz,mzv->ktv', norm_output_rows, outweight, precision=EXACT_PRECISION)

def adamw_step(grad, moment, square, weight):
    first_new = BETA_FIRST * moment + (1.0 - BETA_FIRST) * grad
    second_new = BETA_SECOND * square + (1.0 - BETA_SECOND) * grad * grad
    fix_first = 1.0 - BETA_FIRST ** STEP
    fix_second = 1.0 - BETA_SECOND ** STEP
    delta = -LEARN_RATE * (first_new / fix_first / (jnp.sqrt(second_new / fix_second) + ADAM_EPSILON) + WEIGHT_DECAY * weight)
    return (first_new, second_new, delta)

def reference(inputs, segments, cotangent, pregain, innerweight, rateweight, stateweight, innerconv, stateconv, headparams, postgain, outweight, moment_pregain, square_pregain, moment_innerweight, square_innerweight, moment_rateweight, square_rateweight, moment_stateweight, square_stateweight, moment_innerconv, square_innerconv, moment_stateconv, square_stateconv, moment_headparams, square_headparams, moment_postgain, square_postgain, moment_outweight, square_outweight):
    floats = tuple((param.astype(jnp.float32) for param in (pregain, innerweight, rateweight, stateweight, innerconv, stateconv, headparams, postgain, outweight)))

    def whole(values, *weights):
        return forward(values, *weights, segments)
    result, pullback = jax.vjp(whole, inputs.astype(jnp.float32), *floats)
    grads = pullback(cotangent.astype(jnp.float32))
    grad_input = grads[0]
    grad_pregain, grad_innerweight, grad_rateweight, grad_stateweight, grad_innerconv, grad_stateconv, grad_headparams, grad_postgain, grad_outweight = grads[1:]
    first_pregain, second_pregain, delta_pregain = adamw_step(grad_pregain, moment_pregain, square_pregain, floats[0])
    first_innerweight, second_innerweight, delta_innerweight = adamw_step(grad_innerweight, moment_innerweight, square_innerweight, floats[1])
    first_rateweight, second_rateweight, delta_rateweight = adamw_step(grad_rateweight, moment_rateweight, square_rateweight, floats[2])
    first_stateweight, second_stateweight, delta_stateweight = adamw_step(grad_stateweight, moment_stateweight, square_stateweight, floats[3])
    first_innerconv, second_innerconv, delta_innerconv = adamw_step(grad_innerconv, moment_innerconv, square_innerconv, floats[4])
    first_stateconv, second_stateconv, delta_stateconv = adamw_step(grad_stateconv, moment_stateconv, square_stateconv, floats[5])
    first_headparams, second_headparams, delta_headparams = adamw_step(grad_headparams, moment_headparams, square_headparams, floats[6])
    first_postgain, second_postgain, delta_postgain = adamw_step(grad_postgain, moment_postgain, square_postgain, floats[7])
    first_outweight, second_outweight, delta_outweight = adamw_step(grad_outweight, moment_outweight, square_outweight, floats[8])
    return (result, grad_input, grad_pregain, first_pregain, second_pregain, delta_pregain, grad_innerweight, first_innerweight, second_innerweight, delta_innerweight, grad_rateweight, first_rateweight, second_rateweight, delta_rateweight, grad_stateweight, first_stateweight, second_stateweight, delta_stateweight, grad_innerconv, first_innerconv, second_innerconv, delta_innerconv, grad_stateconv, first_stateconv, second_stateconv, delta_stateconv, grad_headparams, first_headparams, second_headparams, delta_headparams, grad_postgain, first_postgain, second_postgain, delta_postgain, grad_outweight, first_outweight, second_outweight, delta_outweight)
```

```python
import functools

import jax
import jax.numpy as jnp
from jax import lax
from jax.experimental import pallas as pl
from jax.experimental.pallas import tpu as pltpu
from jax.sharding import PartitionSpec as P

HEADP = 64
NSTATE = 128
GROUP = 256
MOST = 2000
STEP = 4
HALO = 16
NORM_EPSILON = 1e-05
ADAM_EPSILON = 1e-08
BETA_FIRST = 0.5
BETA_SECOND = 0.5
LEARN_RATE = 0.02
WEIGHT_DECAY = 0.1
FAR = -1e30

F32 = jnp.float32
BF16 = jnp.bfloat16


def dot(a, b, ca, cb):
    return lax.dot_general(a, b, (((ca,), (cb,)), ((), ())), preferred_element_type=F32)


def mm(a, b):
    return dot(a, b, 1, 0)


def mm_nt(a, b):
    return dot(a, b, 1, 1)


def mm_tn(a, b):
    return dot(a, b, 0, 0)


def sigmoid(v):
    return 0.5 * jnp.tanh(0.5 * v) + 0.5


def halves(v):
    high = v.astype(BF16)
    return high, (v - high.astype(F32)).astype(BF16)


def stack_parts(v, count):
    parts = []
    for _ in range(count):
        high = v.astype(BF16).astype(F32)
        parts.append(high)
        v = v - high
    return parts


def expand(rows, spread):
    high, low = stack_parts(rows, 2)
    return mm_tn(jnp.concatenate([high, low], 0).astype(BF16), spread)


def head_sums(v, spread):
    high, low = halves(v)
    sums = mm_nt(spread, high) + mm_nt(spread, low)
    return sums[: sums.shape[0] // 2]


def lane_sums(v):
    total = v[:, :128]
    for at in range(128, v.shape[1], 128):
        total = total + v[:, at : at + 128]
    high, low = halves(total)
    return mm_nt(jnp.ones((16, 256), BF16), jnp.concatenate([high, low], 1))[:8]


def running(rows, triangle, product=mm):
    count = rows.shape[0]
    parts = stack_parts(rows, 3) + [jnp.zeros_like(rows)]
    sums = product(jnp.concatenate(parts, 0).astype(BF16), triangle)
    return sums[:count] + sums[count : 2 * count] + sums[2 * count : 3 * count]


def softplus(v):
    return jnp.maximum(v, 0.0) + jnp.log1p(jnp.exp(-jnp.abs(v)))


def row_norm(xs, width):
    total = None
    for xf in xs:
        part = jnp.sum(xf * xf, axis=1, keepdims=True)
        total = part if total is None else total + part
    return lax.rsqrt(total / width + NORM_EPSILON)


def chunk_decay(cum, rates, tok):
    last = cum[:, GROUP - 1 : GROUP]
    tail = (tok[0:1] == tok[0:1, GROUP - 1 : GROUP]).astype(F32)
    to_end = jnp.exp(last - cum) * tail
    enter = jnp.exp(cum) * tok[7:8]
    return to_end, enter


def fwd1_kernel(
    x_ref, xh_ref, gain_ref, wmain_ref, wstate_ref, wrate_ref, tok_ref, head_ref,
    kin_ref, kst_ref, tri_ref, spread_ref,
    gate_ref, pre_ref, st_ref, uv_ref, us_ref, bc_ref, rows_ref, sent_ref, prod_ref, fin_ref, total_ref, preh_ref, sth_ref, rinvh_ref,
    ext, state, prod,
):
    k = pl.program_id(0)
    blocks, _, depth = x_ref.shape
    width = blocks * depth
    hl = gate_ref.shape[1]
    heads = hl // HEADP

    def project(xs):
        xf = [v.astype(F32) for v in xs]
        rinv = row_norm(xf, width)
        xn = [
            (v * gain_ref[:, i * depth : (i + 1) * depth]).astype(BF16)
            for i, v in enumerate(xf)
        ]
        main = state_in = None
        for i, v in enumerate(xn):
            at = pl.ds(i * depth, depth)
            a, b = mm(v, wmain_ref[at, :]), mm(v, wstate_ref[at, :])
            main = a if main is None else main + a
            state_in = b if state_in is None else state_in + b
        return xn, rinv, main * rinv, (state_in * rinv).astype(BF16)

    @pl.when(k == 0)
    def _():
        _, rinv, main, state_in = project([xh_ref[i] for i in range(blocks)])
        pre = main[:, hl:].astype(BF16)
        preh_ref[...] = pre.astype(BF16)
        sth_ref[...] = state_in
        rinvh_ref[...] = jnp.broadcast_to(rinv, (HALO, 128))
        ext[0:8, :hl] = pre.astype(F32)[HALO - 8 :]
        ext[0:8, hl:] = state_in.astype(F32)[HALO - 8 :]
        state[...] = jnp.zeros_like(state)
        prod[...] = jnp.ones_like(prod)

    xn, rinv, main, state_in = project([x_ref[i] for i in range(blocks)])
    gate_ref[...] = main[:, :hl]
    pre = main[:, hl:]
    pre_ref[...] = pre
    st_ref[...] = state_in
    ext[8:, :hl] = pre.astype(F32)
    ext[8:, hl:] = state_in.astype(F32)
    tok = tok_ref[...]
    cols = tok.T
    kernel = jnp.concatenate([kin_ref[...], kst_ref[...]], 1)
    u = ext[8:, :] * kernel[0:1] + kernel[4:5]
    for j in range(1, 4):
        u = u + ext[pl.ds(8 - j, GROUP), :] * cols[:, j : j + 1] * kernel[j : j + 1]
    ext[0:8, :] = ext[GROUP : GROUP + 8, :]
    uv_ref[...] = u[:, :hl]
    us_ref[...] = u[:, hl:]
    u = u.astype(F32)
    act = u * sigmoid(u)
    values = act[:, :hl]
    bc = act[:, hl:].astype(BF16)
    bc_ref[...] = bc
    rate = None
    for i, v in enumerate(xn):
        part = mm_nt(wrate_ref[:, i * depth : (i + 1) * depth], v)
        rate = part if rate is None else rate + part
    rinv_row = jnp.broadcast_to(rinv, (GROUP, 128)).T[0:heads]
    rin = rate[:heads] * rinv_row + head_ref[heads : 2 * heads, 0:1]
    rates = softplus(rin)
    cum = running(head_ref[0:heads, 0:1] * rates, tri_ref[...])
    rows_ref[0:heads] = rin
    rows_ref[heads : 2 * heads] = rates
    rows_ref[2 * heads : 3 * heads] = cum
    rows_ref[3 * heads :] = rinv_row
    to_end, _ = chunk_decay(cum, rates, tok)
    both = expand(to_end * rates, spread_ref[...])
    scaled = (values * both).astype(BF16)
    carry = jnp.exp(cum[:, GROUP - 1 :]) * tok[7:8, GROUP - 1 :]
    carry = expand(jnp.broadcast_to(carry, (heads, 128)), spread_ref[...])[0:8]
    sent_ref[0] = state[...].astype(BF16)
    prod_ref[0] = prod[...]
    state[...] = state[...] * carry[0:1] + mm_tn(bc[:, :NSTATE], scaled)
    prod[...] = prod[...] * carry
    fin_ref[...] = state[...]
    total_ref[...] = prod[...]


def pair_lanes(shape):
    return lax.broadcasted_iota(jnp.int32, shape, 1) < HEADP


def chunk_mask(tok, cols):
    rowpos = lax.broadcasted_iota(jnp.int32, (GROUP, GROUP), 0)
    colpos = lax.broadcasted_iota(jnp.int32, (GROUP, GROUP), 1)
    same = (cols[:, 0:1] == tok[0:1, :]) & (colpos <= rowpos)
    return jnp.where(same, 0.0, FAR)


def fwd2_kernel(
    gate_ref, uv_ref, bc_ref, rows_ref, tok_ref, sent_ref, prod_ref, sin_ref, cot_ref, post_ref, skip_ref,
    woutt_ref, spread_ref,
    scan_ref, out_ref, dn_ref, stat_ref,
):
    hl = gate_ref.shape[1]
    heads = hl // HEADP
    blocks, _, depth = cot_ref.shape
    tok = tok_ref[...]
    cum = rows_ref[2 * heads : 3 * heads]
    rates = rows_ref[heads : 2 * heads]
    _, enter = chunk_decay(cum, rates, tok)
    spread = spread_ref[...]
    cols = jnp.concatenate([tok, cum], 0).T
    mask = chunk_mask(tok, cols)
    bm, cm = bc_ref[:, :NSTATE], bc_ref[:, NSTATE:]
    scores = mm_nt(cm, bm)
    u = uv_ref[...].astype(F32)
    values = u * sigmoid(u)
    scaled = (values * expand(rates, spread)).astype(BF16)
    entering = (sent_ref[0].astype(F32) + prod_ref[0, 0:1] * sin_ref[...]).astype(BF16)
    outer = mm(cm, entering) * expand(enter, spread)
    first = pair_lanes((GROUP, 128))
    pieces = []
    for pair in range(heads // 2):
        vp = scaled[:, pair * 128 : (pair + 1) * 128]
        ys = []
        for h in (2 * pair, 2 * pair + 1):
            decay = jnp.exp(cols[:, 8 + h : 9 + h] - cum[h : h + 1, :] + mask)
            ys.append(mm((scores * decay).astype(BF16), vp))
        pieces.append(jnp.where(first, ys[0], ys[1]))
    scan = jnp.concatenate(pieces, 1) + outer
    scan_ref[...] = scan
    g = gate_ref[...].astype(F32)
    gated = (scan + skip_ref[...] * values) * (g * sigmoid(g))
    post = post_ref[...]
    dn = None
    for i in range(blocks):
        part = mm(cot_ref[i], woutt_ref[pl.ds(i * depth, depth), :])
        dn = part if dn is None else dn + part
    dn = dn.astype(BF16)
    dn_ref[...] = dn
    normed = gated * post
    stat_ref[0:8] = lane_sums(gated * gated)
    stat_ref[8:16] = lane_sums(dn.astype(F32) * normed)
    normed = normed.astype(BF16)
    for i in range(blocks):
        out_ref[i] = mm_nt(normed, woutt_ref[pl.ds(i * depth, depth), :]).astype(BF16)


def bwd1_kernel(
    gate_ref, uv_ref, bc_ref, rows_ref, tok_ref, scan_ref, dn_ref, scal_ref, cot_ref, post_ref, skip_ref, spread_ref,
    dy_ref, dg_ref, leave_ref, prodb_ref, first_ref, gout_ref, sums_ref, root_ref,
    adj, prod,
):
    step = pl.program_id(0)
    hl = gate_ref.shape[1]
    heads = hl // HEADP
    blocks, _, depth = cot_ref.shape
    tok = tok_ref[...]
    cum = rows_ref[2 * heads : 3 * heads]
    spread = spread_ref[...]

    @pl.when(step == 0)
    def _():
        adj[...] = jnp.zeros_like(adj)
        prod[...] = jnp.ones_like(prod)
        gout_ref[...] = jnp.zeros_like(gout_ref)
        sums_ref[...] = jnp.zeros_like(sums_ref)

    enter = jnp.exp(cum) * tok[7:8]
    scal = scal_ref[...]
    cols = jnp.concatenate([scal, rows_ref[3 * heads :]], 0).T
    rootgate, pull, rinv = cols[:, 0:1], cols[:, 1:2], cols[:, 8:9]
    u = uv_ref[...].astype(F32)
    values = u * sigmoid(u)
    mixed = scan_ref[...] + skip_ref[...] * values
    g = gate_ref[...].astype(F32)
    sg = sigmoid(g)
    act = g * sg
    gated = mixed * act
    post = post_ref[...]
    dn = dn_ref[...].astype(F32)
    dgated = rootgate * (dn * post) - gated * pull
    dy = dgated * act
    dyb = dy.astype(BF16)
    dy_ref[...] = dyb
    dgate = dgated * mixed * (sg + act * (1.0 - sg)) * rinv
    dg_ref[...] = dgate.astype(BF16)
    root_ref[...] = lane_sums(dgate * g)
    ng = gated * rootgate
    sums_ref[0:8] += jnp.sum((dn * ng).reshape(GROUP // 8, 8, hl), 0)
    sums_ref[8:16] += jnp.sum((dy * values).reshape(GROUP // 8, 8, hl), 0)
    normout = (ng * post).astype(BF16)
    for i in range(blocks):
        gout_ref[pl.ds(i * depth, depth), :] += mm_tn(cot_ref[i], normout)
    cm = bc_ref[:, NSTATE:]
    weighted = (dyb.astype(F32) * expand(enter, spread)).astype(BF16)
    carry = jnp.exp(cum[:, GROUP - 1 :]) * tok[7:8, GROUP - 1 :]
    carry = expand(jnp.broadcast_to(carry, (heads, 128)), spread)[0:8]
    leave_ref[0] = adj[...].astype(BF16)
    prodb_ref[0] = prod[...]
    adj[...] = adj[...] * carry[0:1] + mm_tn(cm, weighted)
    prod[...] = prod[...] * carry
    first_ref[...] = adj[...]


def bwd2_kernel(
    x_ref, xh_ref, gain_ref, wmain_ref, wstate_ref, wrate_ref, tok_ref, head_ref, hmask_ref, hrinv_ref,
    kin_ref, kst_ref, tri_ref, spread_ref, skip_ref,
    pre_ref, st_ref, preh_ref, sth_ref, uv_ref, us_ref, bc_ref, rows_ref, sent_ref, prod_ref, sin_ref,
    scan_ref, dy_ref, dg_ref, leave_ref, prodb_ref, din_ref, root_ref,
    gin_ref, ginh_ref, gw_ref, gr_ref, gk_ref, gh_ref, gp_ref,
    ext,
):
    step = pl.program_id(0)
    steps = pl.num_programs(0)
    hl = uv_ref.shape[1]
    heads = hl // HEADP
    blocks, _, depth = x_ref.shape
    tok = tok_ref[...]
    spread = spread_ref[...]
    rin = rows_ref[0:heads]
    rates = rows_ref[heads : 2 * heads]
    cum = rows_ref[2 * heads : 3 * heads]
    rinv_row = rows_ref[3 * heads :]
    cols = jnp.concatenate([tok, cum, rinv_row], 0).T
    rinv = cols[:, 16:17]

    @pl.when(step == 0)
    def _():
        ext[GROUP:, :] = jnp.zeros_like(ext[GROUP:, :])
        gw_ref[...] = jnp.zeros_like(gw_ref)
        gr_ref[...] = jnp.zeros_like(gr_ref)
        gk_ref[...] = jnp.zeros_like(gk_ref)
        gh_ref[...] = jnp.zeros_like(gh_ref)
        gp_ref[...] = jnp.zeros_like(gp_ref)

    to_end, enter = chunk_decay(cum, rates, tok)
    mask = chunk_mask(tok, cols)
    bm, cm = bc_ref[:, :NSTATE], bc_ref[:, NSTATE:]
    scores = mm_nt(cm, bm)
    u = uv_ref[...].astype(F32)
    sg = sigmoid(u)
    values = u * sg
    rexp = expand(rates, spread)
    scaled = (values * rexp).astype(BF16)
    dyb = dy_ref[...]
    entering = (sent_ref[0].astype(F32) + prod_ref[0, 0:1] * sin_ref[...]).astype(BF16)
    leaving = (leave_ref[0].astype(F32) + prodb_ref[0, 0:1] * din_ref[...]).astype(BF16)

    first = pair_lanes((GROUP, 128))
    dscores = jnp.zeros((GROUP, GROUP), F32)
    pieces = []
    for pair in range(heads // 2):
        vp = scaled[:, pair * 128 : (pair + 1) * 128]
        dp = dyb[:, pair * 128 : (pair + 1) * 128]
        dvs = []
        for h in (2 * pair, 2 * pair + 1):
            decay = jnp.exp(cols[:, 8 + h : 9 + h] - cum[h : h + 1, :] + mask)
            weight = (scores * decay).astype(BF16)
            own = first if h % 2 == 0 else ~first
            dh = jnp.where(own, dp, jnp.zeros_like(dp))
            dscores = dscores + mm_nt(dh, vp) * decay
            dvs.append(mm_tn(weight, dp))
        pieces.append(jnp.where(first, dvs[0], dvs[1]))
    tend = expand(to_end, spread)
    inside = jnp.concatenate(pieces, 1)
    onward = mm(bm, leaving) * tend
    dscaled = inside + onward
    dsb = dscores.astype(BF16)
    dyf = dyb.astype(F32)
    weighted = (dyf * expand(enter, spread)).astype(BF16)
    ended = (values * (tend * rexp)).astype(BF16)
    dcm = mm(dsb, bm) + mm_nt(weighted, entering)
    dbm = mm_tn(dsb, cm) + mm_nt(ended, leaving)
    dvalues = dscaled * rexp + skip_ref[...] * dyf

    kept = scaled.astype(F32)
    dcum = head_sums(dyf * scan_ref[...] - kept * inside, spread)
    dend = head_sums(kept * onward, spread)
    drates = head_sums(values * dscaled, spread)
    through = leaving.astype(F32) * entering.astype(F32)
    through = head_sums(jnp.sum(through.reshape(NSTATE // 8, 8, hl), 0), spread)
    through = jnp.sum(through, axis=1, keepdims=True) * (
        jnp.exp(cum[:, GROUP - 1 :]) * tok[7:8, GROUP - 1 :]
    )
    ddec = running(dcum, tri_ref[...], mm_nt) + running(dend, tri_ref[...]) - dend + through
    drates = drates + head_ref[0:heads, 0:1] * ddec
    drin = drates * sigmoid(rin)
    gh_ref[0:heads] += ddec * (head_ref[0:heads, 0:1] * rates)
    gh_ref[heads : 2 * heads] += drin

    us = us_ref[...].astype(F32)
    ss = sigmoid(us)
    dstates = jnp.concatenate([dbm, dcm], 1)
    ext[0:GROUP, :hl] = dvalues * (sg + values * (1.0 - sg))
    ext[0:GROUP, hl:] = dstates * (ss + us * ss * (1.0 - ss))
    kernel = jnp.concatenate([kin_ref[...], kst_ref[...]], 1)
    source = jnp.concatenate([pre_ref[...], st_ref[...]], 1).astype(F32)
    du = ext[0:GROUP, :]
    gk_ref[32:40] += jnp.sum(du.reshape(GROUP // 8, 8, du.shape[1]), 0)
    gk_ref[0:8] += jnp.sum((du * source).reshape(GROUP // 8, 8, du.shape[1]), 0)
    dsource = du * kernel[0:1]
    for j in range(1, 4):
        moved = ext[pl.ds(j, GROUP), :] * cols[:, 3 + j : 4 + j]
        gk_ref[8 * j : 8 * j + 8] += jnp.sum(
            (moved * source).reshape(GROUP // 8, 8, du.shape[1]), 0
        )
        dsource = dsource + moved * kernel[j : j + 1]
    low = dsource * rinv
    lowb = low.astype(BF16)
    root = lane_sums(low * source) + root_ref[...] + jnp.sum(
        drin * (rin - head_ref[heads : 2 * heads, 0:1]), 0, keepdims=True
    ) * rinv_row[0:1]
    root = (root * rinv_row[0:1]).T[:, 0:1] / (blocks * depth)
    ratelow = (drin * rinv_row).astype(F32)
    ratelow = jnp.concatenate([ratelow, jnp.zeros_like(ratelow)], 0).astype(BF16)
    gates = dg_ref[...]
    for i in range(blocks):
        at = pl.ds(i * depth, depth)
        xf = x_ref[i].astype(F32)
        gain = gain_ref[:, i * depth : (i + 1) * depth]
        xn = (xf * gain).astype(BF16)
        gw_ref[at, 0:hl] += mm_tn(xn, gates)
        gw_ref[at, hl:] += mm_tn(xn, lowb)
        gr_ref[:, i * depth : (i + 1) * depth] += mm(ratelow, xn)
        dn = (
            mm_nt(gates, wmain_ref[at, 0:hl])
            + mm_nt(lowb[:, :hl], wmain_ref[at, hl:])
            + mm_nt(lowb[:, hl:], wstate_ref[at, :])
            + mm_tn(ratelow, wrate_ref[:, i * depth : (i + 1) * depth])
        )
        gp_ref[:, i * depth : (i + 1) * depth] += jnp.sum(
            (dn * xf).reshape(GROUP // 8, 8, depth), 0
        )
        gin_ref[i] = (dn * gain - xf * root).astype(BF16)

    ext[GROUP : GROUP + 8, :] = ext[0:8, :]

    @pl.when(step == steps - 1)
    def _():
        wide = ext.shape[1]
        source_h = jnp.concatenate([preh_ref[...], sth_ref[...]], 1).astype(F32)
        head8 = ext[GROUP : GROUP + 8, :]
        ext[0:HALO, :] = jnp.zeros((HALO, wide), F32)
        ext[HALO : HALO + 8, :] = head8
        dsource_h = jnp.zeros((HALO, wide), F32)
        for j in range(1, 4):
            moved = ext[pl.ds(j, HALO), :] * hmask_ref[:, j : j + 1]
            gk_ref[8 * j : 8 * j + 8] += jnp.sum(
                (moved * source_h).reshape(HALO // 8, 8, wide), 0
            )
            dsource_h = dsource_h + moved * kernel[j : j + 1]
        rinv_h = hrinv_ref[:, 0:1]
        low_h = dsource_h * rinv_h
        lowb_h = low_h.astype(BF16)
        root_h = jnp.sum(low_h * source_h, axis=1, keepdims=True) * rinv_h / (blocks * depth)
        for i in range(blocks):
            at = pl.ds(i * depth, depth)
            xf = xh_ref[i].astype(F32)
            gain = gain_ref[:, i * depth : (i + 1) * depth]
            xn = (xf * gain).astype(BF16)
            gw_ref[at, hl:] += mm_tn(xn, lowb_h)
            dn = mm_nt(lowb_h[:, :hl], wmain_ref[at, hl:]) + mm_nt(
                lowb_h[:, hl:], wstate_ref[at, :]
            )
            gp_ref[:, i * depth : (i + 1) * depth] += jnp.sum(
                (dn * xf).reshape(HALO // 8, 8, depth), 0
            )
            ginh_ref[i] = (dn * gain - xf * root_h).astype(BF16)


def call(kernel, steps, ins, outs, scratch, reverse, name):
    def spec(block, axis):
        def index(step):
            at = steps - 1 - step if reverse else step
            return tuple(at if a == axis else 0 for a in range(len(block)))

        return pl.BlockSpec(block, index)

    return pl.pallas_call(
        kernel,
        grid=(steps,),
        in_specs=[spec(block, axis) for _, block, axis in ins],
        out_specs=[spec(block, axis) for _, _, block, axis in outs],
        out_shape=[jax.ShapeDtypeStruct(shape, dtype) for shape, dtype, _, _ in outs],
        scratch_shapes=scratch,
        compiler_params=pltpu.CompilerParams(
            dimension_semantics=("arbitrary",), vmem_limit_bytes=60 * 1024 * 1024
        ),
        name=name,
    )(*[array for array, _, _ in ins])


def whole(array):
    return (array, array.shape, None)


def lanes(array):
    return (array, array.shape[:-1] + (GROUP,), array.ndim - 1)


def sublanes(array):
    return (array, array.shape[:-2] + (GROUP,) + array.shape[-1:], array.ndim - 2)


def each(array):
    return (array, (1,) + array.shape[1:], 0)


def out_whole(shape, dtype):
    return (shape, dtype, shape, None)


def out_sub(shape, dtype):
    return (shape, dtype, shape[:-2] + (GROUP,) + shape[-1:], len(shape) - 2)


def out_lanes(shape, dtype):
    return (shape, dtype, shape[:-1] + (GROUP,), len(shape) - 1)


def out_each(shape, dtype):
    return (shape, dtype, (1,) + shape[1:], 0)


def adamw_step(grad, moment, square, weight):
    first_new = BETA_FIRST * moment + (1.0 - BETA_FIRST) * grad
    second_new = BETA_SECOND * square + (1.0 - BETA_SECOND) * grad * grad
    fix_first = 1.0 - BETA_FIRST**STEP
    fix_second = 1.0 - BETA_SECOND**STEP
    delta = -LEARN_RATE * (
        first_new / fix_first / (jnp.sqrt(second_new / fix_second) + ADAM_EPSILON)
        + WEIGHT_DECAY * weight
    )
    return (first_new, second_new, delta)


def local(
    inputs, segments, cotangent, pregain, innerweight, rateweight, stateweight, innerconv, stateconv, headparams,
    postgain, outweight, *moments,
):
    nrow, ncol = lax.axis_size("row"), lax.axis_size("col")
    row, col = lax.axis_index("row"), lax.axis_index("col")
    length, own = inputs.shape[1], inputs.shape[2]
    width = own * nrow * ncol
    stored = innerweight.shape[1]
    total_heads = stored * ncol
    heads = total_heads // nrow
    hl = heads * HEADP
    count = total_heads * HEADP
    tokens = length // ncol
    steps = tokens // GROUP
    depth = width // nrow
    fold = ncol // nrow
    hops = (MOST - 2) // tokens + 1

    window = jnp.pad(segments[0], (HALO, HALO), constant_values=-1)
    window = lax.dynamic_slice_in_dim(window, col * tokens, tokens + 2 * HALO, 0)
    mine = window[HALO : HALO + tokens]
    flags = [mine]
    for j in (-1, -2, -3, 1, 2, 3):
        flags.append(window[HALO + j : HALO + j + tokens] == mine)
    before = window[HALO - 1 : HALO - 1 + tokens : GROUP]
    flags.append((mine.reshape(steps, GROUP) == before[:, None]).reshape(tokens))
    tok = jnp.stack([f.astype(F32) for f in flags])
    hmask = jnp.stack([(window[j : j + HALO] == window[:HALO]).astype(F32) for j in range(8)], 1)
    hmask = jnp.pad(hmask, ((0, 0), (0, 120)))

    block_heads = headparams.shape[1]
    smalls = [pregain, innerconv, headparams, postgain, rateweight, stateweight]
    flat = jnp.concatenate([a.reshape(-1) for a in smalls])
    sizes = [a.size for a in smalls]
    pad = -flat.size % 2048
    packed = jnp.pad(flat, (0, pad)).reshape(-1, 128)
    gathered = lax.all_gather(packed, ("row", "col"), axis=0).reshape(nrow, ncol, -1)
    parts, at = [], 0
    for size in sizes:
        parts.append(gathered[:, :, at : at + size])
        at += size
    gain = parts[0].reshape(1, width).astype(F32)
    iconv = parts[1].reshape(nrow, ncol, 5, block_heads, HEADP).transpose(2, 1, 0, 3, 4)
    iconv = lax.dynamic_slice_in_dim(iconv.reshape(5, count), row * hl, hl, 1).astype(F32)
    hp = parts[2].reshape(nrow, ncol, 3, block_heads).transpose(2, 1, 0, 3)
    hp = lax.dynamic_slice_in_dim(hp.reshape(3, total_heads), row * heads, heads, 1).astype(F32)
    post = parts[3].reshape(nrow, ncol, block_heads * HEADP).transpose(1, 0, 2)
    post = lax.dynamic_slice_in_dim(post.reshape(1, count), row * hl, hl, 1).astype(F32)
    wrate = parts[4].reshape(nrow, ncol, depth, stored).transpose(1, 3, 0, 2)
    wrate = lax.dynamic_slice_in_dim(wrate.reshape(total_heads, width), row * heads, heads, 0)
    wrate = jnp.pad(wrate, ((0, 16 - heads), (0, 0)))
    wstate = parts[5].reshape(width, 2 * NSTATE)
    sconv = stateconv.astype(F32)
    head = jnp.broadcast_to(
        jnp.concatenate([-jnp.exp(hp[0]), hp[1]])[:, None], (2 * heads, 128)
    )
    skip = jnp.repeat(hp[2], HEADP)[None]

    split = innerweight.reshape(depth, stored, 2, HEADP)
    sent = jnp.concatenate(
        [
            split[:, :, 0].reshape(depth, -1),
            split[:, :, 1].reshape(depth, -1),
            outweight.reshape(stored * HEADP, depth).T,
        ],
        1,
    )
    sub = depth // fold
    sent = sent.reshape(fold, sub, -1)
    came = []
    for m in range(fold):
        perm = []
        for r in range(nrow):
            for c in range(ncol):
                perm.append((r * ncol + c, (c // fold) * ncol + r * fold + (m + c) % fold))
        piece = lax.dynamic_index_in_dim(sent, (m + col) % fold, 0, False)
        came.append(lax.ppermute(piece, ("row", "col"), perm))
    came = jnp.stack(came)
    came = jnp.stack(
        [lax.dynamic_index_in_dim(came, (col - i) % fold, 0, False) for i in range(fold)]
    )
    came = came.reshape(fold, sub, 3, stored * HEADP).transpose(1, 2, 0, 3).reshape(sub, 3 * hl)
    weights = lax.all_gather(came, "col", axis=0, tiled=True)
    wmain, woutt = weights[:, : 2 * hl], weights[:, 2 * hl :]

    padded = jnp.pad(inputs[0], ((HALO, 0), (0, 0)))
    pieces = jnp.stack([padded[i * tokens : (i + 1) * tokens + HALO] for i in range(ncol)])
    pieces = lax.all_to_all(pieces, "col", 0, 0).transpose(1, 0, 2).reshape(tokens + HALO, depth)
    xall = lax.all_gather(pieces, "row", axis=0)
    xh, x = xall[:, :HALO], xall[:, HALO:]
    pieces = lax.all_to_all(cotangent[0].reshape(ncol, tokens, own), "col", 0, 0)
    cot = lax.all_gather(pieces.transpose(1, 0, 2).reshape(tokens, depth), "row", axis=0)

    spread = jnp.repeat(jnp.eye(heads, dtype=BF16), HEADP, 1)
    spread = jnp.concatenate([spread, spread], 0)
    triangle = jnp.triu(jnp.ones((GROUP, GROUP), BF16))
    ns2 = 2 * NSTATE

    gate, pre, st, uv, us, bc, rows, states, prod, fin, total, preh, sth, rinvh = call(
        fwd1_kernel,
        steps,
        [sublanes(x), whole(xh), whole(gain), whole(wmain), whole(wstate), whole(wrate), lanes(tok), whole(head),
         whole(iconv), whole(sconv), whole(triangle), whole(spread)],
        [out_sub((tokens, hl), F32), out_sub((tokens, hl), F32), out_sub((tokens, ns2), BF16),
         out_sub((tokens, hl), F32), out_sub((tokens, ns2), F32), out_sub((tokens, ns2), BF16),
         out_lanes((4 * heads, tokens), F32),
         out_each((steps, NSTATE, hl), BF16), out_each((steps, 8, hl), F32),
         out_whole((NSTATE, hl), F32), out_whole((8, hl), F32), out_whole((HALO, hl), BF16), out_whole((HALO, ns2), BF16),
         out_whole((HALO, 128), F32)],
        [pltpu.VMEM((GROUP + 8, hl + ns2), F32), pltpu.VMEM((NSTATE, hl), F32), pltpu.VMEM((8, hl), F32)],
        False,
        "fwd1",
    )
    total = total[0:1]
    ahead = [(i, i + 1) for i in range(ncol - 1)]
    back = [(i + 1, i) for i in range(ncol - 1)]
    sin = lax.ppermute(fin, "col", ahead)
    for _ in range(hops - 1):
        sin = lax.ppermute(fin + total * sin, "col", ahead)

    scan, out, dn, stat = call(
        fwd2_kernel,
        steps,
        [sublanes(gate), sublanes(uv), sublanes(bc), lanes(rows), lanes(tok), each(states), each(prod), whole(sin),
         sublanes(cot), whole(post), whole(skip), whole(woutt), whole(spread)],
        [out_sub((tokens, hl), F32), out_sub((nrow, tokens, depth), BF16), out_sub((tokens, hl), BF16),
         out_lanes((16, tokens), F32)],
        [],
        False,
        "fwd2",
    )
    stat = lax.psum(jnp.stack([stat[0], stat[8]]), "row")
    rootgate = lax.rsqrt(stat[0] / count + NORM_EPSILON)
    pull = rootgate * rootgate * rootgate * stat[1] / count
    scal = jnp.pad(jnp.stack([rootgate, pull]), ((0, 6), (0, 0)))

    mixed = lax.psum_scatter(out, "row", scatter_dimension=0, tiled=False)
    mixed = (mixed.astype(F32) * rootgate[:, None]).astype(BF16)
    mixed = lax.all_to_all(mixed.reshape(tokens, ncol, own).transpose(1, 0, 2), "col", 0, 0)
    result = inputs.astype(F32) + mixed.reshape(1, length, own).astype(F32)

    dy, dg, leave, prodb, first, gout, sums, root = call(
        bwd1_kernel,
        steps,
        [sublanes(gate), sublanes(uv), sublanes(bc), lanes(rows), lanes(tok), sublanes(scan), sublanes(dn),
         lanes(scal), sublanes(cot), whole(post), whole(skip), whole(spread)],
        [out_sub((tokens, hl), BF16), out_sub((tokens, hl), BF16), out_each((steps, NSTATE, hl), BF16),
         out_each((steps, 8, hl), F32), out_whole((NSTATE, hl), F32), out_whole((width, hl), F32),
         out_whole((16, hl), F32), out_lanes((8, tokens), F32)],
        [pltpu.VMEM((NSTATE, hl), F32), pltpu.VMEM((8, hl), F32)],
        True,
        "bwd1",
    )
    din = lax.ppermute(first, "col", back)
    for _ in range(hops - 1):
        din = lax.ppermute(first + total * din, "col", back)

    gin, ginh, gw, gr, gk, gh, gp = call(
        bwd2_kernel,
        steps,
        [sublanes(x), whole(xh), whole(gain), whole(wmain), whole(wstate), whole(wrate), lanes(tok), whole(head),
         whole(hmask), whole(rinvh), whole(iconv), whole(sconv), whole(triangle), whole(spread), whole(skip),
         sublanes(pre), sublanes(st), whole(preh), whole(sth), sublanes(uv), sublanes(us), sublanes(bc), lanes(rows),
         each(states), each(prod), whole(sin), sublanes(scan), sublanes(dy), sublanes(dg),
         each(leave), each(prodb), whole(din), lanes(root)],
        [out_sub((nrow, tokens, depth), BF16), out_whole((nrow, HALO, depth), BF16),
         out_whole((width, 2 * hl + ns2), F32), out_whole((16, width), F32), out_whole((40, hl + ns2), F32),
         out_whole((2 * heads, GROUP), F32), out_whole((8, width), F32)],
        [pltpu.VMEM((GROUP + 8, hl + ns2), F32)],
        True,
        "bwd2",
    )

    gin = lax.psum_scatter(jnp.concatenate([gin, ginh], 1), "row", scatter_dimension=0, tiled=False)
    gin = gin.reshape(tokens + HALO, ncol, own).transpose(1, 0, 2)
    gin = lax.all_to_all(gin, "col", 0, 0).astype(F32)
    body, halo = gin[:, :tokens], gin[:, tokens:]
    halo = jnp.concatenate([halo[1:], jnp.zeros_like(halo[:1])], 0)
    body = jnp.concatenate([body[:, : tokens - HALO], body[:, tokens - HALO :] + halo], 1)
    grad_input = cotangent.astype(F32) + body.reshape(1, length, own)

    def home(grad):
        grad = lax.psum_scatter(grad.astype(BF16), "col", scatter_dimension=0, tiled=True)
        grad = lax.psum(grad.astype(F32), "dp").astype(BF16)
        per = grad.shape[1] // hl
        grad = grad.reshape(sub, per, fold, stored * HEADP).transpose(2, 0, 1, 3).reshape(fold, sub, -1)
        got = []
        for m in range(fold):
            perm = []
            for r in range(nrow):
                for c in range(ncol):
                    perm.append(((c // fold) * ncol + r * fold + (m + c) % fold, r * ncol + c))
            piece = lax.dynamic_index_in_dim(grad, (col - m) % fold, 0, False)
            got.append(lax.ppermute(piece, ("row", "col"), perm))
        got = jnp.stack(got)
        got = jnp.stack(
            [lax.dynamic_index_in_dim(got, (j - col) % fold, 0, False) for j in range(fold)]
        )
        return got.reshape(depth, per, stored, HEADP).astype(F32)

    gout = home(gout)[:, 0].transpose(1, 2, 0)
    ginner = home(gw[:, : 2 * hl]).transpose(0, 2, 1, 3).reshape(depth, stored, 2 * HEADP)
    gstate = lax.psum_scatter(gw[:, 2 * hl :], ("row", "col"), scatter_dimension=0, tiled=True)
    gstate = lax.psum(gstate, "dp")

    def place(part, size):
        blank = jnp.zeros((part.shape[0], size), F32)
        return lax.dynamic_update_slice(blank, part, (0, row * part.shape[1]))

    gk = jnp.sum(gk.reshape(5, 8, -1), 1)
    gh = jnp.sum(gh, 1).reshape(2, heads)
    sums = jnp.sum(sums.reshape(2, 8, hl), 1)
    gskip = jnp.sum(sums[1].reshape(1, heads, HEADP), 2)
    small = [
        jnp.sum(gp, 0),
        place(gr[:heads].T, total_heads),
        place(gk[:, :hl], count),
        gk[:, hl:],
        place(jnp.concatenate([gh, gskip]), total_heads),
        place(sums[0:1], count),
    ]
    flat = jnp.concatenate([a.reshape(-1) for a in small])
    pad = -flat.size % 1024
    flat = lax.psum(jnp.pad(flat, (0, pad)).reshape(-1, 128), ("dp", "row", "col")).reshape(-1)
    back_parts, at = [], 0
    for a in small:
        back_parts.append(flat[at : at + a.size].reshape(a.shape))
        at += a.size
    feature = (row * ncol + col) * own
    block = col * nrow + row
    gpre = lax.dynamic_slice_in_dim(back_parts[0], feature, own, 0)
    grate = lax.dynamic_slice(back_parts[1], (row * depth, col * stored), (depth, stored))
    giconv = lax.dynamic_slice_in_dim(back_parts[2], block * block_heads * HEADP, block_heads * HEADP, 1)
    giconv = giconv.reshape(5, block_heads, HEADP)
    gsconv = back_parts[3]
    ghead = lax.dynamic_slice_in_dim(back_parts[4], block * block_heads, block_heads, 1)
    gpost = lax.dynamic_slice_in_dim(back_parts[5], block * block_heads * HEADP, block_heads * HEADP, 1)
    gpost = gpost.reshape(block_heads, HEADP)

    grads = (gpre, ginner, grate, gstate, giconv, gsconv, ghead, gpost, gout)
    params = (
        pregain, innerweight, rateweight, stateweight, innerconv, stateconv, headparams, postgain, outweight,
    )
    outputs = [result, grad_input]
    for i, (grad, param) in enumerate(zip(grads, params)):
        outputs.append(grad)
        outputs.extend(adamw_step(grad, moments[2 * i], moments[2 * i + 1], param.astype(F32)))
    return tuple(outputs)


def solution(mesh):
    tokens = P("dp", None, ("row", "col"))
    weights = (
        P(("row", "col")),
        P("row", "col", None),
        P("row", "col"),
        P(("row", "col"), None),
        P(None, ("col", "row"), None),
        P(),
        P(None, ("col", "row")),
        P(("col", "row"), None),
        P("col", None, "row"),
    )
    return jax.shard_map(
        local,
        mesh=mesh,
        in_specs=(tokens, P("dp", None), tokens)
        + weights
        + tuple(w for w in weights for _ in range(2)),
        out_specs=(tokens, tokens) + tuple(w for w in weights for _ in range(4)),
        check_vma=False,
    )
```

```python
import functools

import jax
import jax.numpy as jnp
from jax import lax
from jax.experimental import pallas as pl
from jax.experimental.pallas import tpu as pltpu
from jax.sharding import PartitionSpec as P

HEADP = 64
NSTATE = 128
GROUP = 256
MOST = 2000
STEP = 4
HALO = 16
NORM_EPSILON = 1e-05
ADAM_EPSILON = 1e-08
BETA_FIRST = 0.5
BETA_SECOND = 0.5
LEARN_RATE = 0.02
WEIGHT_DECAY = 0.1
FAR = -1e30

F32 = jnp.float32
BF16 = jnp.bfloat16


def dot(a, b, ca, cb):
    return lax.dot_general(a, b, (((ca,), (cb,)), ((), ())), preferred_element_type=F32)


def mm(a, b):
    return dot(a, b, 1, 0)


def mm_nt(a, b):
    return dot(a, b, 1, 1)


def mm_tn(a, b):
    return dot(a, b, 0, 0)


def sigmoid(v):
    return 0.5 * jnp.tanh(0.5 * v) + 0.5


def halves(v):
    high = v.astype(BF16)
    return high, (v - high.astype(F32)).astype(BF16)


def stack_parts(v, count):
    parts = []
    for _ in range(count):
        high = v.astype(BF16).astype(F32)
        parts.append(high)
        v = v - high
    return parts


def expand(rows, spread):
    high, low = stack_parts(rows, 2)
    return mm_tn(jnp.concatenate([high, low], 0).astype(BF16), spread)


def head_sums(v, spread):
    high, low = halves(v)
    sums = mm_nt(spread, high) + mm_nt(spread, low)
    return sums[: sums.shape[0] // 2]


def lane_sums(v):
    total = v[:, :128]
    for at in range(128, v.shape[1], 128):
        total = total + v[:, at : at + 128]
    high, low = halves(total)
    return mm_nt(jnp.ones((16, 256), BF16), jnp.concatenate([high, low], 1))[:8]


def running(rows, triangle, product=mm):
    count = rows.shape[0]
    parts = stack_parts(rows, 3) + [jnp.zeros_like(rows)]
    sums = product(jnp.concatenate(parts, 0).astype(BF16), triangle)
    return sums[:count] + sums[count : 2 * count] + sums[2 * count : 3 * count]


def softplus(v):
    return jnp.maximum(v, 0.0) + jnp.log1p(jnp.exp(-jnp.abs(v)))


def turned(row, count):
    return jnp.broadcast_to(row, (8, count)).T[:, 0:1]


def chunk_decay(cum, rates, tok):
    last = cum[:, GROUP - 1 : GROUP]
    tail = (tok[0:1] == tok[0:1, GROUP - 1 : GROUP]).astype(F32)
    to_end = jnp.exp(last - cum) * tail
    enter = jnp.exp(cum) * tok[7:8]
    return to_end, enter


def fwd1_kernel(
    x_ref, xh_ref, gain_ref, wmain_ref, wstate_ref, wrate_ref, tok_ref, head_ref,
    kin_ref, kst_ref, tri_ref, spread_ref,
    gate_ref, pre_ref, st_ref, uv_ref, us_ref, bc_ref, rows_ref, sent_ref, prod_ref, fin_ref, total_ref, preh_ref, sth_ref, rinvh_ref,
    ext, state, prod,
):
    k = pl.program_id(0)
    width = x_ref.shape[0]
    hl = gate_ref.shape[1]
    heads = hl // HEADP

    def project(x):
        xf = x.astype(F32)
        rinv = lax.rsqrt(jnp.sum(xf * xf, axis=0, keepdims=True) / width + NORM_EPSILON)
        gain = gain_ref[...]
        if x.shape[1] > 128:
            gain = jnp.concatenate([gain] * (x.shape[1] // 128), 1)
        xn = (xf * gain).astype(BF16)
        col = turned(rinv, x.shape[1])
        return xn, rinv, col, mm_tn(xn, wmain_ref[...]) * col, (mm_tn(xn, wstate_ref[...]) * col).astype(BF16)

    @pl.when(k == 0)
    def _():
        _, _, rinv, main, state_in = project(xh_ref[...])
        at = slice(128 - HALO, 128)
        pre = main[at, hl:]
        preh_ref[...] = pre.astype(BF16)
        sth_ref[...] = state_in[at]
        rinvh_ref[...] = jnp.broadcast_to(rinv[at], (HALO, 128))
        ext[0:8, :hl] = pre[HALO - 8 :]
        ext[0:8, hl:] = state_in.astype(F32)[128 - 8 :]
        state[...] = jnp.zeros_like(state)
        prod[...] = jnp.ones_like(prod)

    xn, rinv, _, main, state_in = project(x_ref[...])
    gate_ref[...] = main[:, :hl]
    pre = main[:, hl:]
    pre_ref[...] = pre
    st_ref[...] = state_in
    ext[8:, :hl] = pre.astype(F32)
    ext[8:, hl:] = state_in.astype(F32)
    tok = tok_ref[...]
    cols = tok.T
    kernel = jnp.concatenate([kin_ref[...], kst_ref[...]], 1)
    u = ext[8:, :] * kernel[0:1] + kernel[4:5]
    for j in range(1, 4):
        u = u + ext[pl.ds(8 - j, GROUP), :] * cols[:, j : j + 1] * kernel[j : j + 1]
    ext[0:8, :] = ext[GROUP : GROUP + 8, :]
    uv_ref[...] = u[:, :hl]
    us_ref[...] = u[:, hl:]
    u = u.astype(F32)
    act = u * sigmoid(u)
    values = act[:, :hl]
    bc = act[:, hl:].astype(BF16)
    bc_ref[...] = bc
    rate = mm(wrate_ref[...], xn)
    rinv_row = jnp.broadcast_to(rinv, (heads, GROUP))
    rin = rate[:heads] * rinv_row + head_ref[heads : 2 * heads, 0:1]
    rates = softplus(rin)
    cum = running(head_ref[0:heads, 0:1] * rates, tri_ref[...])
    rows_ref[0:heads] = rin
    rows_ref[heads : 2 * heads] = rates
    rows_ref[2 * heads : 3 * heads] = cum
    rows_ref[3 * heads :] = rinv_row
    to_end, _ = chunk_decay(cum, rates, tok)
    both = expand(to_end * rates, spread_ref[...])
    scaled = (values * both).astype(BF16)
    carry = jnp.exp(cum[:, GROUP - 1 :]) * tok[7:8, GROUP - 1 :]
    carry = expand(jnp.broadcast_to(carry, (heads, 128)), spread_ref[...])[0:8]
    sent_ref[0] = state[...].astype(BF16)
    prod_ref[0] = prod[...]
    state[...] = state[...] * carry[0:1] + mm_tn(bc[:, :NSTATE], scaled)
    prod[...] = prod[...] * carry
    fin_ref[...] = state[...]
    total_ref[...] = prod[...]


def pair_lanes(shape):
    return lax.broadcasted_iota(jnp.int32, shape, 1) < HEADP


def chunk_mask(tok, cols):
    rowpos = lax.broadcasted_iota(jnp.int32, (GROUP, GROUP), 0)
    colpos = lax.broadcasted_iota(jnp.int32, (GROUP, GROUP), 1)
    same = (cols[:, 0:1] == tok[0:1, :]) & (colpos <= rowpos)
    return jnp.where(same, 0.0, FAR)


def fwd2_kernel(
    gate_ref, uv_ref, bc_ref, rows_ref, tok_ref, sent_ref, prod_ref, sin_ref, cot_ref, post_ref, skip_ref,
    woutt_ref, spread_ref,
    scan_ref, out_ref, dn_ref, stat_ref,
):
    row = lax.axis_index("row")
    hl = gate_ref.shape[1]
    heads = hl // HEADP
    blocks, depth, _ = out_ref.shape
    tok = tok_ref[...]
    cum = rows_ref[2 * heads : 3 * heads]
    rates = rows_ref[heads : 2 * heads]
    _, enter = chunk_decay(cum, rates, tok)
    spread = spread_ref[...]
    cols = jnp.concatenate([tok, cum], 0).T
    mask = chunk_mask(tok, cols)
    bm, cm = bc_ref[:, :NSTATE], bc_ref[:, NSTATE:]
    scores = mm_nt(cm, bm)
    u = uv_ref[...].astype(F32)
    values = u * sigmoid(u)
    scaled = (values * expand(rates, spread)).astype(BF16)
    entering = (sent_ref[0].astype(F32) + prod_ref[0, 0:1] * sin_ref[...]).astype(BF16)
    outer = mm(cm, entering) * expand(enter, spread)
    first = pair_lanes((GROUP, 128))
    pieces = []
    for pair in range(heads // 2):
        vp = scaled[:, pair * 128 : (pair + 1) * 128]
        ys = []
        for h in (2 * pair, 2 * pair + 1):
            decay = jnp.exp(cols[:, 8 + h : 9 + h] - cum[h : h + 1, :] + mask)
            ys.append(mm((scores * decay).astype(BF16), vp))
        pieces.append(jnp.where(first, ys[0], ys[1]))
    scan = jnp.concatenate(pieces, 1) + outer
    scan_ref[...] = scan
    g = gate_ref[...].astype(F32)
    gated = (scan + skip_ref[...] * values) * (g * sigmoid(g))
    post = post_ref[...]
    dn = mm_tn(cot_ref[...], woutt_ref[...])
    dn = dn.astype(BF16)
    dn_ref[...] = dn
    normed = gated * post
    squares, inner = lane_sums(gated * gated), lane_sums(dn.astype(F32) * normed)
    stat_ref[...] = jnp.where(
        lax.broadcasted_iota(jnp.int32, squares.shape, 0) == 0, squares, inner
    )
    normed = normed.astype(BF16)
    for i in range(blocks):
        block = mm_nt(woutt_ref[pl.ds(i * depth, depth), :], normed)
        out_ref[jnp.bitwise_xor(row, i)] = block.astype(BF16)


def bwd1_kernel(
    gate_ref, uv_ref, bc_ref, rows_ref, tok_ref, scan_ref, dn_ref, scal_ref, cot_ref, post_ref, skip_ref, spread_ref,
    dy_ref, dg_ref, leave_ref, prodb_ref, first_ref, gout_ref, sums_ref, root_ref,
    adj, prod, gacc,
):
    step = pl.program_id(0)
    hl = gate_ref.shape[1]
    heads = hl // HEADP
    tok = tok_ref[...]
    cum = rows_ref[2 * heads : 3 * heads]
    spread = spread_ref[...]

    @pl.when(step == 0)
    def _():
        adj[...] = jnp.zeros_like(adj)
        prod[...] = jnp.ones_like(prod)
        gacc[...] = jnp.zeros_like(gacc)
        sums_ref[...] = jnp.zeros_like(sums_ref)

    enter = jnp.exp(cum) * tok[7:8]
    scal = scal_ref[...]
    cols = jnp.concatenate([scal, rows_ref[3 * heads :]], 0).T
    rootgate, pull, rinv = cols[:, 0:1], cols[:, 1:2], cols[:, 8:9]
    u = uv_ref[...].astype(F32)
    values = u * sigmoid(u)
    mixed = scan_ref[...] + skip_ref[...] * values
    g = gate_ref[...].astype(F32)
    sg = sigmoid(g)
    act = g * sg
    gated = mixed * act
    post = post_ref[...]
    dn = dn_ref[...].astype(F32)
    dgated = rootgate * (dn * post) - gated * pull
    dy = dgated * act
    dyb = dy.astype(BF16)
    dy_ref[...] = dyb
    dgate = dgated * mixed * (sg + act * (1.0 - sg)) * rinv
    dg_ref[...] = dgate.astype(BF16)
    root_ref[...] = lane_sums(dgate * g)
    ng = gated * rootgate
    sums_ref[0:8] += jnp.sum((dn * ng).reshape(GROUP // 8, 8, hl), 0)
    sums_ref[8:16] += jnp.sum((dy * values).reshape(GROUP // 8, 8, hl), 0)
    normout = (ng * post).astype(BF16)
    gacc[...] += mm(cot_ref[...], normout)

    @pl.when(step == pl.num_programs(0) - 1)
    def _():
        gout_ref[...] = gacc[...].astype(BF16)

    cm = bc_ref[:, NSTATE:]
    weighted = (dyb.astype(F32) * expand(enter, spread)).astype(BF16)
    carry = jnp.exp(cum[:, GROUP - 1 :]) * tok[7:8, GROUP - 1 :]
    carry = expand(jnp.broadcast_to(carry, (heads, 128)), spread)[0:8]
    leave_ref[0] = adj[...].astype(BF16)
    prodb_ref[0] = prod[...]
    adj[...] = adj[...] * carry[0:1] + mm_tn(cm, weighted)
    prod[...] = prod[...] * carry
    first_ref[...] = adj[...]


class Delivery:
    def __init__(self, dims, refs, scal):
        nrow, ncol, ndp, fold = self.dims = dims
        (
            self.out, self.gout, self.home, self.hout,
            self.own, self.ra, self.rb, self.sb, self.sc, self.gv, self.ry, self.sy, self.rz, self.fin, self.rdp,
            send, recv, self.local,
        ) = refs
        self.scal = scal
        self.step, self.last = pl.program_id(0), pl.num_programs(0) - 1
        row, col, dp = (lax.axis_index(a) for a in ("row", "col", "dp"))
        w = self.w = Wires(send, recv)
        near, far, other, half = flip(row, 1), flip(row, 2), flip(dp, 1), lax.rem(dp, 2)
        self.plan = plan = order(ncol)[::-1]
        cols = [lax.rem(col + d, ncol) for d in range(ncol)]
        back = [lax.rem(col - d + ncol, ncol) for d in range(ncol)]
        tokens = self.out.shape[3]
        hs, sh = self.fin.shape[0], self.hout.shape[2]
        places = [pl.ds(pl.multiple_of(c * tokens, 128), tokens) for c in back]
        rows = [pl.ds(half * hs, hs), pl.ds((1 - half) * hs, hs)]
        self.starts = {name: [] for name in ("a", "y", "b", "c", "z", "h")}
        self.takes = {name: [] for name in ("a0", "a1", "y", "b", "c", "z", "h")}

        def wire(kind, at, src, dst, to, when=None):
            slot = w.slot()
            self.starts[kind].append((at, w.copy(slot, src, dst, to), when))
            w.sent.append(None)
            return slot

        def take(kind, at, slot, ref, to, when=None):
            self.takes[kind].append((at, w.copy(slot, ref, ref, to), when))

        for d in plan:
            take("a1", d, wire("a", d, self.out.at[3, cols[d]], self.ra.at[1, d], {"row": near}), self.ra.at[1, d], {"row": near})
            take("a0", d, wire("a", d, self.out.at[1, cols[d]], self.ra.at[0, d], {"row": near}), self.ra.at[0, d], {"row": near})
            take("y", d, wire("y", d, self.gout.at[cols[d], 1 - half], self.ry.at[d], {"dp": other}), self.ry.at[d], {"dp": other})
            take("b", d, wire("b", d, self.sb.at[d], self.rb.at[d], {"row": far}), self.rb.at[d], {"row": far})
            if d:
                to, come = {"col": cols[d]}, {"col": back[d]}
                slot = wire("c", d, self.sc.at[d], self.home.at[:, places[0]], to)
                take("c", d, slot, self.home.at[:, places[d]], come)
                take("z", d, wire("z", d, self.sy.at[d], self.rz.at[d], to), self.rz.at[d], come)
        self.cols = cols
        self.stays = pltpu.make_async_copy(self.sc.at[0], self.home.at[:, places[0]], self.local.at[3])
        self.loads = [
            pltpu.make_async_copy(self.out.at[0], self.own.at[0], self.local.at[0]),
            pltpu.make_async_copy(self.out.at[2], self.own.at[1], self.local.at[1]),
            pltpu.make_async_copy(self.gout.at[:, half], self.gv, self.local.at[2]),
        ]
        self.hops = []
        for i, bit in enumerate(bits(ndp)[1:]):
            to = {"dp": flip(dp, bit)}
            self.hops.append(w.copy(w.slot(), self.rdp.at[2 * i], self.rdp.at[2 * i + 1], to))
            w.sent.append(None)
        self.keeps = []
        for i in range(fold):
            orow, ocol = col // fold, row * fold + i
            away = (orow != row) | (ocol != col)
            src = self.fin.at[:, pl.ds(i * sh, sh)]
            for j in range(fold):
                this = lax.rem(col, fold) == j
                dst = self.hout.at[j, rows[0]]
                near_slot, far_slot = w.slot(), w.slot()
                if i == 0:
                    self.slots = getattr(self, "slots", []) + [(near_slot, far_slot)]
                near_slot, far_slot = self.slots[j]
                to = {"row": orow, "col": ocol}
                self.starts["h"].append((j, w.copy(near_slot, src, dst, to), away & this))
                w.sent.append(None)
                self.starts["h"].append((j, w.copy(far_slot, src, dst, to | {"dp": other}), this))
                w.sent.append(None)
                keep = pltpu.make_async_copy(src, dst, self.local.at[4])
                self.keeps.append((keep, ~away & this))
        for j in range(fold):
            srow, scol = col // fold, row * fold + j
            to = {"row": srow, "col": scol}
            take("h", j, self.slots[j][0], self.hout.at[j, rows[0]], to, (srow != row) | (scol != col))
            take("h", j, self.slots[j][1], self.hout.at[j, rows[1]], to | {"dp": other})

    def go(self, kind, at=None):
        for d, copy, when in self.starts[kind]:
            if at is None or d == at:
                copy.start() if when is None else pl.when(when)(copy.start)

    def come(self, kind, at=None):
        for d, copy, when in self.takes[kind]:
            if at is None or d == at:
                copy.wait_recv() if when is None else pl.when(when)(copy.wait_recv)

    def before(self):
        nrow, ncol, ndp, fold = self.dims
        step, last, plan = self.step, self.last, self.plan

        @pl.when(step == 0)
        def _():
            greet(nrow, ncol, ndp)
            self.go("a")
            self.go("y")
            for load in self.loads:
                load.start()

        @pl.when(step == 1)
        def _():
            for load in self.loads:
                load.wait()
            for d in plan:
                self.come("a1", d)
                self.sb[d] = (self.own[1, self.cols[d]].astype(F32) + self.ra[1, d].astype(F32)).astype(BF16)
                self.go("b", d)

        for i, d in enumerate(plan):

            @pl.when(step == jnp.minimum(2 + i, last - 1))
            def _():
                self.come("a0", d)
                self.come("b", d)
                total = self.own[0, self.cols[d]].astype(F32) + self.ra[0, d].astype(F32) + self.rb[d].astype(F32)
                self.sc[d] = (total * self.scal[0:1]).astype(BF16)
                if d:
                    self.go("c", d)
                else:
                    self.stays.start()

        @pl.when(step == jnp.minimum(3, last - 1))
        def _():
            for d in plan:
                self.come("y", d)
                self.sy[d] = (self.gv[self.cols[d]].astype(F32) + self.ry[d].astype(F32)).astype(BF16)
                if d:
                    self.go("z", d)

        @pl.when(step == last)
        def _():
            total = self.sy[0].astype(F32)
            for d in range(1, ncol):
                self.come("z", d)
                total = total + self.rz[d].astype(F32)
            for i, hop in enumerate(self.hops):
                self.rdp[2 * i] = total
                hop.start()
                hop.wait_recv()
                total = total + self.rdp[2 * i + 1]
            self.fin[...] = total.astype(BF16)
            self.go("h")
            for keep, when in self.keeps:
                pl.when(when)(keep.start)

    def after(self):
        @pl.when(self.step == self.last)
        def _():
            for keep, when in self.keeps:
                pl.when(when)(keep.wait)
            self.come("h")
            self.come("c")
            self.stays.wait()
            for hop in self.hops:
                hop.wait_send()
            for copies in self.starts.values():
                for _, copy, when in copies:
                    copy.wait_send() if when is None else pl.when(when)(copy.wait_send)


def delivery_scratch(nrow, ncol, ndp, fold, own, tokens, hs, hl):
    nb = len(bits(ndp))
    slots = 8 * ncol + nb + 2 * fold * fold + 4
    return [
        pltpu.VMEM((2, ncol, own, tokens), BF16),
        pltpu.VMEM((2, ncol, own, tokens), BF16),
        pltpu.VMEM((ncol, own, tokens), BF16),
        pltpu.VMEM((ncol, own, tokens), BF16),
        pltpu.VMEM((ncol, own, tokens), BF16),
        pltpu.VMEM((ncol, hs, hl), BF16),
        pltpu.VMEM((ncol, hs, hl), BF16),
        pltpu.VMEM((ncol, hs, hl), BF16),
        pltpu.VMEM((ncol, hs, hl), BF16),
        pltpu.VMEM((hs, hl), BF16),
        pltpu.VMEM((max(2 * nb - 2, 1), hs if ndp > 2 else 8, hl), F32),
        pltpu.SemaphoreType.DMA((slots,)),
        pltpu.SemaphoreType.DMA((slots,)),
        pltpu.SemaphoreType.DMA((5,)),
    ]


def bwd2_kernel(
    dims,
    x_ref, xh_ref, gain_ref, wmain_ref, wstate_ref, wrate_ref, tok_ref, head_ref, hmask_ref, hrinv_ref,
    kin_ref, kst_ref, tri_ref, spread_ref, skip_ref,
    pre_ref, st_ref, preh_ref, sth_ref, uv_ref, us_ref, bc_ref, rows_ref, sent_ref, prod_ref, sin_ref,
    scan_ref, dy_ref, dg_ref, leave_ref, prodb_ref, din_ref, root_ref, scal_ref, outs_ref, gout_ref,
    home_ref, hout_ref, gin_ref, ginh_ref, gw_ref, gs_ref, gr_ref, gk_ref, gh_ref, gp_ref,
    ext, gacc, *more,
):
    delivery = Delivery(dims, (outs_ref, gout_ref, home_ref, hout_ref) + more, scal_ref)
    delivery.before()
    step = pl.program_id(0)
    steps = pl.num_programs(0)
    row = lax.axis_index("row")
    hl = uv_ref.shape[1]
    heads = hl // HEADP
    width = x_ref.shape[0]
    blocks, depth, _ = gin_ref.shape
    tok = tok_ref[...]
    spread = spread_ref[...]
    rin = rows_ref[0:heads]
    rates = rows_ref[heads : 2 * heads]
    cum = rows_ref[2 * heads : 3 * heads]
    rinv_row = rows_ref[3 * heads :]
    cols = jnp.concatenate([tok, cum, rinv_row], 0).T
    rinv = cols[:, 16:17]

    @pl.when(step == 0)
    def _():
        ext[GROUP:, :] = jnp.zeros_like(ext[GROUP:, :])
        gacc[...] = jnp.zeros_like(gacc)
        gr_ref[...] = jnp.zeros_like(gr_ref)
        gk_ref[...] = jnp.zeros_like(gk_ref)
        gh_ref[...] = jnp.zeros_like(gh_ref)
        gp_ref[...] = jnp.zeros_like(gp_ref)

    to_end, enter = chunk_decay(cum, rates, tok)
    mask = chunk_mask(tok, cols)
    bm, cm = bc_ref[:, :NSTATE], bc_ref[:, NSTATE:]
    scores = mm_nt(cm, bm)
    u = uv_ref[...].astype(F32)
    sg = sigmoid(u)
    values = u * sg
    rexp = expand(rates, spread)
    scaled = (values * rexp).astype(BF16)
    dyb = dy_ref[...]
    entering = (sent_ref[0].astype(F32) + prod_ref[0, 0:1] * sin_ref[...]).astype(BF16)
    leaving = (leave_ref[0].astype(F32) + prodb_ref[0, 0:1] * din_ref[...]).astype(BF16)

    first = pair_lanes((GROUP, 128))
    dscores = jnp.zeros((GROUP, GROUP), F32)
    pieces = []
    for pair in range(heads // 2):
        vp = scaled[:, pair * 128 : (pair + 1) * 128]
        dp = dyb[:, pair * 128 : (pair + 1) * 128]
        dvs = []
        for h in (2 * pair, 2 * pair + 1):
            decay = jnp.exp(cols[:, 8 + h : 9 + h] - cum[h : h + 1, :] + mask)
            weight = (scores * decay).astype(BF16)
            own = first if h % 2 == 0 else ~first
            dh = jnp.where(own, dp, jnp.zeros_like(dp))
            dscores = dscores + mm_nt(dh, vp) * decay
            dvs.append(mm_tn(weight, dp))
        pieces.append(jnp.where(first, dvs[0], dvs[1]))
    tend = expand(to_end, spread)
    inside = jnp.concatenate(pieces, 1)
    onward = mm(bm, leaving) * tend
    dscaled = inside + onward
    dsb = dscores.astype(BF16)
    dyf = dyb.astype(F32)
    weighted = (dyf * expand(enter, spread)).astype(BF16)
    ended = (values * (tend * rexp)).astype(BF16)
    dcm = mm(dsb, bm) + mm_nt(weighted, entering)
    dbm = mm_tn(dsb, cm) + mm_nt(ended, leaving)
    dvalues = dscaled * rexp + skip_ref[...] * dyf

    kept = scaled.astype(F32)
    dcum = head_sums(dyf * scan_ref[...] - kept * inside, spread)
    dend = head_sums(kept * onward, spread)
    drates = head_sums(values * dscaled, spread)
    through = leaving.astype(F32) * entering.astype(F32)
    through = head_sums(jnp.sum(through.reshape(NSTATE // 8, 8, hl), 0), spread)
    through = jnp.sum(through, axis=1, keepdims=True) * (
        jnp.exp(cum[:, GROUP - 1 :]) * tok[7:8, GROUP - 1 :]
    )
    ddec = running(dcum, tri_ref[...], mm_nt) + running(dend, tri_ref[...]) - dend + through
    drates = drates + head_ref[0:heads, 0:1] * ddec
    drin = drates * sigmoid(rin)
    gh_ref[0:heads] += ddec * (head_ref[0:heads, 0:1] * rates)
    gh_ref[heads : 2 * heads] += drin

    us = us_ref[...].astype(F32)
    ss = sigmoid(us)
    dstates = jnp.concatenate([dbm, dcm], 1)
    ext[0:GROUP, :hl] = dvalues * (sg + values * (1.0 - sg))
    ext[0:GROUP, hl:] = dstates * (ss + us * ss * (1.0 - ss))
    kernel = jnp.concatenate([kin_ref[...], kst_ref[...]], 1)
    source = jnp.concatenate([pre_ref[...], st_ref[...]], 1).astype(F32)
    du = ext[0:GROUP, :]
    gk_ref[32:40] += jnp.sum(du.reshape(GROUP // 8, 8, du.shape[1]), 0)
    gk_ref[0:8] += jnp.sum((du * source).reshape(GROUP // 8, 8, du.shape[1]), 0)
    dsource = du * kernel[0:1]
    for j in range(1, 4):
        moved = ext[pl.ds(j, GROUP), :] * cols[:, 3 + j : 4 + j]
        gk_ref[8 * j : 8 * j + 8] += jnp.sum(
            (moved * source).reshape(GROUP // 8, 8, du.shape[1]), 0
        )
        dsource = dsource + moved * kernel[j : j + 1]
    low = dsource * rinv
    lowb = low.astype(BF16)
    root = lane_sums(low * source) + root_ref[...] + jnp.sum(
        drin * (rin - head_ref[heads : 2 * heads, 0:1]), 0, keepdims=True
    ) * rinv_row[0:1]
    root = root[0:1] * rinv_row[0:1] / width
    ratelow = (drin * rinv_row).astype(F32)
    ratelow = jnp.concatenate([ratelow, jnp.zeros_like(ratelow)], 0).astype(BF16)
    gates = dg_ref[...]
    xf = x_ref[...].astype(F32)
    gain = jnp.concatenate([gain_ref[...]] * (GROUP // 128), 1)
    xn = (xf * gain).astype(BF16)
    gacc[:, 0:hl] += mm(xn, gates)
    gacc[:, hl:] += mm(xn, lowb)
    gr_ref[...] += mm_nt(ratelow, xn)
    dn = (
        mm_nt(wmain_ref[:, 0:hl], gates)
        + mm_nt(wmain_ref[:, hl:], lowb[:, :hl])
        + mm_nt(wstate_ref[...], lowb[:, hl:])
        + mm_tn(wrate_ref[...], ratelow)
    )
    both = dn * xf
    for at in range(0, GROUP, 128):
        gp_ref[...] += both[:, at : at + 128]
    grad = (dn * gain - xf * root).astype(BF16)
    for i in range(blocks):
        gin_ref[jnp.bitwise_xor(row, i)] = grad[i * depth : (i + 1) * depth]

    ext[GROUP : GROUP + 8, :] = ext[0:8, :]

    @pl.when(step == steps - 1)
    def _():
        wide = ext.shape[1]
        source_h = jnp.concatenate([preh_ref[...], sth_ref[...]], 1).astype(F32)
        head8 = ext[GROUP : GROUP + 8, :]
        ext[0:HALO, :] = jnp.zeros((HALO, wide), F32)
        ext[HALO : HALO + 8, :] = head8
        dsource_h = jnp.zeros((HALO, wide), F32)
        for j in range(1, 4):
            moved = ext[pl.ds(j, HALO), :] * hmask_ref[:, j : j + 1]
            gk_ref[8 * j : 8 * j + 8] += jnp.sum(
                (moved * source_h).reshape(HALO // 8, 8, wide), 0
            )
            dsource_h = dsource_h + moved * kernel[j : j + 1]
        rinv_h = hrinv_ref[:, 0:1]
        low_h = dsource_h * rinv_h
        root_h = jnp.sum(low_h * source_h, axis=1, keepdims=True) * rinv_h / width
        fill = jnp.zeros((128 - HALO, wide), F32)
        lowb_h = jnp.concatenate([fill, low_h], 0).astype(BF16)
        root_h = jnp.concatenate([jnp.zeros((128 - HALO, 1), F32), root_h], 0)
        root_h = jnp.broadcast_to(root_h, (128, 128)).T[0:1]
        xf = xh_ref[...].astype(F32)
        gain = gain_ref[...]
        gacc[:, hl:] += mm((xf * gain).astype(BF16), lowb_h)
        dn = mm_nt(wmain_ref[:, hl:], lowb_h[:, :hl]) + mm_nt(wstate_ref[...], lowb_h[:, hl:])
        gp_ref[...] += dn * xf
        grad = (dn * gain - xf * root_h).astype(BF16)
        for i in range(blocks):
            ginh_ref[jnp.bitwise_xor(row, i)] = grad[i * depth : (i + 1) * depth]
        gw_ref[...] = gacc[:, 0 : 2 * hl].astype(BF16)
        gs_ref[...] = gacc[:, 2 * hl :].astype(BF16)

    delivery.after()


MESH = pl.DeviceIdType.MESH


class Wires:
    def __init__(self, send, recv):
        self.sends, self.recv, self.used, self.sent = send, recv, 0, []

    def slot(self):
        self.used += 1
        return self.used - 1

    def copy(self, slot, src, dst, to):
        return pltpu.make_async_remote_copy(
            src_ref=src,
            dst_ref=dst,
            send_sem=self.sends.at[len(self.sent)],
            recv_sem=self.recv.at[slot],
            device_id=to,
            device_id_type=MESH,
        )

    def start(self, slot, src, dst, to, when=None):
        copy = self.copy(slot, src, dst, to)
        if when is None:
            copy.start()
        else:
            pl.when(when)(copy.start)
        self.sent.append((copy, when))

    def arrived(self, slot, ref, to):
        pltpu.make_async_remote_copy(
            src_ref=ref,
            dst_ref=ref,
            send_sem=self.sends.at[0],
            recv_sem=self.recv.at[slot],
            device_id=to,
            device_id_type=MESH,
        ).wait_recv()

    def finish(self):
        for copy, when in self.sent:
            if when is None:
                copy.wait_send()
            else:
                pl.when(when)(copy.wait_send)


def greet(nrow, ncol, ndp):
    row, col, dp = (lax.axis_index(a) for a in ("row", "col", "dp"))
    sem = pltpu.get_barrier_semaphore()
    total = 0
    for i in range(nrow):
        for j in range(ncol):
            if i or j:
                to = {"row": lax.rem(row + i, nrow), "col": lax.rem(col + j, ncol)}
                pl.semaphore_signal(sem, 1, device_id=to, device_id_type=MESH)
                total += 1
    for bit in bits(ndp):
        pl.semaphore_signal(sem, 1, device_id={"dp": flip(dp, bit)}, device_id_type=MESH)
        total += 1
    pl.semaphore_wait(sem, total)


def bits(size):
    found, bit = [], 1
    while bit < size:
        found.append(bit)
        bit *= 2
    return found


def flip(index, bit):
    return index + bit - 2 * bit * lax.rem(index // bit, 2)


def order(ncol):
    near = [0]
    for d in range(1, ncol // 2 + 1):
        near.extend([d, ncol - d] if ncol - d != d else [d])
    return near


class Spread:
    def __init__(self, wires, ncol, source, out):
        self.w, self.ncol, self.source, self.out = wires, ncol, source, out
        self.row, self.col = lax.axis_index("row"), lax.axis_index("col")
        self.far, self.near = flip(self.row, 2), flip(self.row, 1)
        self.a = [wires.slot() for _ in range(ncol)]
        self.b = [wires.slot() for _ in range(ncol)]
        self.e = [wires.slot() for _ in range(ncol)]
        self.f = [wires.slot() for _ in range(ncol)]

    def begin(self):
        for d in order(self.ncol)[:0:-1]:
            to = lax.rem(self.col + d, self.ncol)
            self.w.start(self.a[d], self.source(to), self.out.at[self.row, self.col], {"col": to})

    def forward(self, d):
        at = lax.rem(self.col - d + self.ncol, self.ncol)
        place = self.out.at[self.row, at]
        src = place
        if d:
            self.w.arrived(self.a[d], place, {"col": at})
        else:
            src = self.source(self.col)
        self.w.start(self.b[d], src, place, {"row": self.far})
        self.w.start(self.e[d], src, place, {"row": self.near})

    def relay(self, d):
        at = lax.rem(self.col - d + self.ncol, self.ncol)
        place = self.out.at[self.far, at]
        self.w.arrived(self.b[d], place, {"row": self.far})
        self.w.start(self.f[d], place, place, {"row": self.near})

    def end(self):
        for d in range(self.ncol):
            at = lax.rem(self.col - d + self.ncol, self.ncol)
            self.w.arrived(self.e[d], self.out.at[self.near, at], {"row": self.near})
            self.w.arrived(self.f[d], self.out.at[flip(self.near, 2), at], {"row": self.near})


def moved(src, mid, dst, sem):
    pltpu.make_async_copy(src, mid, sem).start()
    pltpu.make_async_copy(src, mid, sem).wait()
    pltpu.make_async_copy(mid, dst, sem).start()


def enter_kernel(nrow, ncol, ndp, fold, xs, cs, ws, ss, xo, ho, co, wo, so, xv, hv, cv, wv, sv, send, recv, local):
    row, col, dp = (lax.axis_index(a) for a in ("row", "col", "dp"))
    w = Wires(send, recv)
    greet(nrow, ncol, ndp)
    tokens = xo.shape[3]

    def tokens_of(ref, to):
        return ref.at[:, pl.ds(pl.multiple_of(to * tokens, 128), tokens)]

    def before(ref, to):
        at = jnp.maximum(to * tokens - 128, 0)
        return ref.at[:, pl.ds(pl.multiple_of(at, 128), 128)]

    spreads = [
        Spread(w, ncol, lambda to: ss, so),
        Spread(w, ncol, lambda to: before(xs, to), ho),
        Spread(w, ncol, lambda to: tokens_of(xs, to), xo),
        Spread(w, ncol, lambda to: tokens_of(cs, to), co),
    ]
    half, other = lax.rem(dp, 2), flip(dp, 1)
    hs = ws.shape[1] // 2
    mine, theirs = pl.ds(half * hs, hs), pl.ds((1 - half) * hs, hs)
    w1 = [w.slot() for _ in range(fold)]
    left = [w.slot() for _ in range(ncol)]
    right = [w.slot() for _ in range(ncol)]
    cross = [w.slot() for _ in range(2 * ncol)]

    for j in range(fold):
        tr, tc = col // fold, row * fold + j
        away = (tr != row) | (tc != col)
        for i in range(fold):
            w.start(
                w1[i], ws.at[j, mine], wo.at[tc, i, mine], {"row": tr, "col": tc},
                away & (lax.rem(col, fold) == i),
            )

        @pl.when(~away)
        def _():
            i = lax.rem(col, fold)
            moved(ws.at[j, mine], wv, wo.at[col, i, mine], local.at[0])
            pltpu.make_async_copy(wv, wo.at[col, i, mine], local.at[0]).wait()

    for s in spreads:
        s.begin()
    moved(ss, sv, so.at[row, col], local.at[1])
    moved(tokens_of(xs, col), xv, xo.at[row, col], local.at[2])
    moved(tokens_of(cs, col), cv, co.at[row, col], local.at[3])
    moved(before(xs, col), hv, ho.at[row, col], local.at[4])
    for s in spreads:
        s.forward(0)
    for i in range(fold):
        sr, sc = col // fold, row * fold + i

        @pl.when((sr != row) | (sc != col))
        def _():
            w.arrived(w1[i], wo.at[col, i, mine], {"row": sr, "col": sc})

    def unit(c, rows):
        return wo.at[c, :, rows]

    own = unit(col, mine)
    w.start(left[1], own, own, {"col": col + 1}, col + 1 < ncol)
    w.start(right[1], own, own, {"col": col - 1}, col >= 1)
    w.start(cross[0], own, own, {"dp": other})
    steps = order(ncol)
    for at in range(1, ncol):
        d = steps[at]
        for s in spreads:
            s.forward(d)
        for s in spreads:
            s.relay(steps[at - 1])

        @pl.when(col >= at)
        def _():
            w.arrived(left[at], unit(col - at, mine), {"col": col - 1})

        got = unit(col - at, mine)
        w.start(left[min(at + 1, ncol - 1)], got, got, {"col": col + 1}, (col >= at) & (col + 1 < ncol))
        w.start(cross[at], got, got, {"dp": other}, col >= at)

        @pl.when(col + at < ncol)
        def _():
            w.arrived(right[at], unit(col + at, mine), {"col": col + 1})

        got = unit(col + at, mine)
        w.start(right[min(at + 1, ncol - 1)], got, got, {"col": col - 1}, (col + at < ncol) & (col >= 1))
        w.start(cross[ncol + at], got, got, {"dp": other}, col + at < ncol)
    for s in spreads:
        s.relay(steps[-1])
    w.arrived(cross[0], unit(col, theirs), {"dp": other})
    for at in range(1, ncol):

        @pl.when(col >= at)
        def _():
            w.arrived(cross[at], unit(col - at, theirs), {"dp": other})

        @pl.when(col + at < ncol)
        def _():
            w.arrived(cross[ncol + at], unit(col + at, theirs), {"dp": other})

    for s in spreads:
        s.end()
    pltpu.make_async_copy(sv, so.at[row, col], local.at[1]).wait()
    pltpu.make_async_copy(xv, xo.at[row, col], local.at[2]).wait()
    pltpu.make_async_copy(cv, co.at[row, col], local.at[3]).wait()
    pltpu.make_async_copy(hv, ho.at[row, col], local.at[4]).wait()
    w.finish()


ANYWHERE = pl.BlockSpec(memory_space=pl.ANY)
ONCHIP = pl.BlockSpec(memory_space=pltpu.VMEM)


def enter(nrow, ncol, ndp, fold, xs, cs, ws, ss):
    own, tokens = xs.shape[0], xs.shape[1] // ncol
    slots = 16 * ncol + fold + 4 * ncol
    return pl.pallas_call(
        functools.partial(enter_kernel, nrow, ncol, ndp, fold),
        out_shape=[
            jax.ShapeDtypeStruct((nrow, ncol, own, tokens), BF16),
            jax.ShapeDtypeStruct((nrow, ncol, own, 128), BF16),
            jax.ShapeDtypeStruct((nrow, ncol, own, tokens), BF16),
            jax.ShapeDtypeStruct((ncol,) + ws.shape, BF16),
            jax.ShapeDtypeStruct((nrow, ncol) + ss.shape, BF16),
        ],
        in_specs=[ANYWHERE] * 4,
        out_specs=[ANYWHERE] * 5,
        scratch_shapes=[
            pltpu.VMEM((own, tokens), BF16),
            pltpu.VMEM((own, 128), BF16),
            pltpu.VMEM((own, tokens), BF16),
            pltpu.VMEM((ws.shape[1] // 2, ws.shape[2]), BF16),
            pltpu.VMEM(ss.shape, BF16),
            pltpu.SemaphoreType.DMA((20 * ncol + 8 + fold * fold,)),
            pltpu.SemaphoreType.DMA((slots,)),
            pltpu.SemaphoreType.DMA((5,)),
        ],
        compiler_params=pltpu.CompilerParams(collective_id=0, has_side_effects=True),
        name="enter",
    )(xs, cs, ws, ss)


def shift_kernel(ncol, by, src, dst, buf, send, recv, local):
    col = lax.axis_index("col")
    to, back = col + by, col - by
    sends = (to >= 0) & (to < ncol)
    takes = (back >= 0) & (back < ncol)
    sem = pltpu.get_barrier_semaphore()

    @pl.when(takes)
    def _():
        pl.semaphore_signal(sem, 1, device_id={"col": back}, device_id_type=MESH)

    def wire():
        return pltpu.make_async_remote_copy(
            src_ref=src, dst_ref=buf, send_sem=send, recv_sem=recv,
            device_id={"col": to}, device_id_type=MESH,
        )

    @pl.when(sends)
    def _():
        pl.semaphore_wait(sem, 1)
        wire().start()

    @pl.when(~takes)
    def _():
        buf[...] = jnp.zeros_like(buf)

    @pl.when(takes)
    def _():
        wire().wait_recv()

    @pl.when(sends)
    def _():
        wire().wait_send()

    dst[...] = buf[...]


def shift(ncol, by, block, ident):
    return pl.pallas_call(
        functools.partial(shift_kernel, ncol, by),
        out_shape=jax.ShapeDtypeStruct(block.shape, block.dtype),
        in_specs=[ONCHIP],
        out_specs=ONCHIP,
        scratch_shapes=[
            pltpu.VMEM(block.shape, block.dtype),
            pltpu.SemaphoreType.DMA(()),
            pltpu.SemaphoreType.DMA(()),
            pltpu.SemaphoreType.DMA(()),
        ],
        compiler_params=pltpu.CompilerParams(collective_id=ident, has_side_effects=True),
        name=f"shift{ident}",
    )(block)


def gather_kernel(nrow, count, stat, scal, buf, send, recv):
    row = lax.axis_index("row")
    sem = pltpu.get_barrier_semaphore()
    for d in range(1, nrow):
        pl.semaphore_signal(sem, 1, device_id={"row": lax.rem(row + d, nrow)}, device_id_type=MESH)
    pl.semaphore_wait(sem, nrow - 1)
    w = Wires(send, recv)
    for d in range(1, nrow):
        w.start(d, stat, buf.at[d], {"row": lax.rem(row + d, nrow)})
    total = stat[...]
    for d in range(1, nrow):
        w.arrived(d, buf.at[d], {"row": lax.rem(row + d, nrow)})
        total = total + buf[d]
    w.finish()
    rootgate = lax.rsqrt(total[0:1] / count + NORM_EPSILON)
    pull = rootgate * rootgate * rootgate * total[1:2] / count
    first = lax.broadcasted_iota(jnp.int32, total.shape, 0) == 0
    scal[...] = jnp.where(first, rootgate, pull)


def gather_stat(nrow, count, stat):
    return pl.pallas_call(
        functools.partial(gather_kernel, nrow, count),
        out_shape=jax.ShapeDtypeStruct(stat.shape, F32),
        in_specs=[ONCHIP],
        out_specs=ONCHIP,
        scratch_shapes=[
            pltpu.VMEM((nrow,) + stat.shape, F32),
            pltpu.SemaphoreType.DMA((nrow,)),
            pltpu.SemaphoreType.DMA((nrow,)),
        ],
        compiler_params=pltpu.CompilerParams(collective_id=1, has_side_effects=True),
        name="stat",
    )(stat)


def leave_kernel(
    nrow, ncol, ndp, fold,
    gin, ginh, gw, gs, sm,
    go, gho, ho, so, smo,
    own, ra, rb, sb, sc, hown, hra, hrb, hsb, hsc, gwv, ry, sy, rz, fin, rdp, gsv, rs1, ss1, rs2, rs3, smb, smr, send, recv, local,
):
    row, col, dp = (lax.axis_index(a) for a in ("row", "col", "dp"))
    w = Wires(send, recv)
    greet(nrow, ncol, ndp)
    near, far, other, half = flip(row, 1), flip(row, 2), flip(dp, 1), lax.rem(dp, 2)
    cols = [lax.rem(col + d, ncol) for d in range(ncol)]
    from_col = [lax.rem(col - d + ncol, ncol) for d in range(ncol)]
    plan = order(ncol)[::-1]

    loads = {}

    def load(name, src, dst, at):
        loads[name] = pltpu.make_async_copy(src, dst, local.at[at])
        loads[name].start()

    a0 = [w.slot() for _ in range(ncol)]
    a1 = [w.slot() for _ in range(ncol)]
    b = [w.slot() for _ in range(ncol)]
    c_ = [w.slot() for _ in range(ncol)]
    y = [w.slot() for _ in range(ncol)]
    z = [w.slot() for _ in range(ncol)]
    tokens = gin.shape[3]
    ha, hb = [w.slot() for _ in range(2)], w.slot()
    hc = [w.slot() for _ in range(ncol)]
    w.start(ha[1], ginh.at[3], hra.at[1], {"row": near})
    w.start(ha[0], ginh.at[1], hra.at[0], {"row": near})
    load("h0", ginh.at[0], hown.at[0], 8)
    load("h1", ginh.at[2], hown.at[1], 9)
    place = pl.ds(pl.multiple_of(col * tokens, 128), tokens)
    for d in plan:
        w.start(a1[d], gin.at[3, cols[d]], ra.at[1, d], {"row": near})
        w.start(a0[d], gin.at[1, cols[d]], ra.at[0, d], {"row": near})
    for d in plan:
        w.start(y[d], gw.at[cols[d], 1 - half], ry.at[d], {"dp": other})
    load("own0", gin.at[0], own.at[0], 0)
    load("own1", gin.at[2], own.at[1], 1)
    load("gw", gw.at[:, half], gwv, 2)
    load("gs", gs.at[row], gsv, 3)
    load("sm", sm, smb.at[0], 4)
    s1 = [w.slot() for _ in range(nrow)]
    for d in range(1, nrow):
        to = lax.rem(row + d, nrow)
        w.start(s1[d], gs.at[to], rs1.at[d], {"row": to})

    loads["sm"].wait()
    hops = [("dp", bit) for bit in bits(ndp)] + [("col", bit) for bit in bits(ncol)]
    sms = [w.slot() for _ in hops]
    at = {"dp": dp, "col": col}

    def small_send(i):
        axis, bit = hops[i]
        w.start(sms[i], smb.at[i], smr.at[i], {axis: flip(at[axis], bit)})

    def small_take(i):
        axis, bit = hops[i]
        w.arrived(sms[i], smr.at[i], {axis: flip(at[axis], bit)})
        smb[i + 1] = smb[i] + smr[i]

    small_send(0)

    loads["own0"].wait()
    loads["own1"].wait()
    loads["h0"].wait()
    loads["h1"].wait()
    w.arrived(ha[1], hra.at[1], {"row": near})
    hsb[...] = (hown[1].astype(F32) + hra[1].astype(F32)).astype(BF16)
    w.start(hb, hsb, hrb, {"row": far})
    for d in plan:
        w.arrived(a1[d], ra.at[1, d], {"row": near})
        sb[d] = (own[1, cols[d]].astype(F32) + ra[1, d].astype(F32)).astype(BF16)
        w.start(b[d], sb.at[d], rb.at[d], {"row": far})
    small_take(0)
    if len(hops) > 1:
        small_send(1)

    loads["gw"].wait()

    def features(d):
        w.arrived(a0[d], ra.at[0, d], {"row": near})
        w.arrived(b[d], rb.at[d], {"row": far})
        total = own[0, cols[d]].astype(F32) + ra[0, d].astype(F32) + rb[d].astype(F32)
        sc[d] = total.astype(BF16)
        if d:
            w.start(c_[d], sc.at[d], go.at[:, place], {"col": cols[d]})
            w.start(hc[d], hsc.at[cols[d]], gho.at[col], {"col": cols[d]})
        else:
            pltpu.make_async_copy(sc.at[0], go.at[:, place], local.at[5]).start()
            pltpu.make_async_copy(hsc.at[col], gho.at[col], local.at[10]).start()

    def weights(d):
        w.arrived(y[d], ry.at[d], {"dp": other})
        sy[d] = (gwv[cols[d]].astype(F32) + ry[d].astype(F32)).astype(BF16)
        if d:
            w.start(z[d], sy.at[d], rz.at[d], {"col": cols[d]})

    w.arrived(ha[0], hra.at[0], {"row": near})
    w.arrived(hb, hrb, {"row": far})
    hsc[...] = (hown[0].astype(F32) + hra[0].astype(F32) + hrb[...].astype(F32)).astype(BF16)
    for d in plan:
        features(d)
        weights(d)

    loads["gs"].wait()
    total = gsv[...].astype(F32)
    for d in range(1, nrow):
        w.arrived(s1[d], rs1.at[d], {"row": lax.rem(row - d + nrow, nrow)})
        total = total + rs1[d].astype(F32)
    ss1[...] = total.astype(BF16)
    part = so.shape[0]
    s2 = [w.slot() for _ in range(ncol)]
    for d in plan[:-1]:
        w.start(s2[d], ss1.at[pl.ds(cols[d] * part, part)], rs2.at[d], {"col": cols[d]})
    for i in range(1, len(hops)):
        small_take(i)
        if i + 1 < len(hops):
            small_send(i + 1)
    last = len(hops)
    s4 = [w.slot() for _ in range(nrow)]
    for d in range(1, nrow):
        w.start(s4[d], smb.at[last], smo.at[row], {"row": lax.rem(row + d, nrow)})
    pltpu.make_async_copy(smb.at[last], smo.at[row], local.at[6]).start()

    total = ss1[pl.ds(pl.multiple_of(col * part, part), part), :].astype(F32)
    for d in range(1, ncol):
        w.arrived(s2[d], rs2.at[d], {"col": from_col[d]})
        total = total + rs2[d].astype(F32)
    rs3[0] = total
    s3 = [w.slot() for _ in bits(ndp)]
    for i, bit in enumerate(bits(ndp)):
        w.start(s3[i], rs3.at[2 * i], rs3.at[2 * i + 1], {"dp": flip(dp, bit)})
        w.arrived(s3[i], rs3.at[2 * i + 1], {"dp": flip(dp, bit)})
        total = total + rs3[2 * i + 1]
        rs3[2 * i + 2] = total
    so[...] = total

    total = sy[0].astype(F32)
    for d in range(1, ncol):
        w.arrived(z[d], rz.at[d], {"col": from_col[d]})
        total = total + rz[d].astype(F32)
    if ndp > 2:
        fin[...] = total.astype(BF16)
        for i, bit in enumerate(bits(ndp)[1:]):
            slot = w.slot()
            rdp[2 * i] = total
            w.start(slot, rdp.at[2 * i], rdp.at[2 * i + 1], {"dp": flip(dp, bit)})
            w.arrived(slot, rdp.at[2 * i + 1], {"dp": flip(dp, bit)})
            total = total + rdp[2 * i + 1]
    fin[...] = total.astype(BF16)
    hs = fin.shape[0]
    sh = ho.shape[3]
    mine, theirs = pl.ds(half * hs, hs), pl.ds((1 - half) * hs, hs)
    count = ho.shape[0]
    h1 = [[w.slot() for _ in range(fold)] for _ in range(count)]
    h2 = [[w.slot() for _ in range(fold)] for _ in range(count)]
    for i in range(fold):
        orow, ocol = col // fold, row * fold + i
        away = (orow != row) | (ocol != col)
        for p in range(count):
            src = fin.at[:, pl.ds((p * fold + i) * sh, sh)]
            for j in range(fold):
                this = lax.rem(col, fold) == j
                dst = ho.at[p, j, mine]
                w.start(h1[p][j], src, dst, {"row": orow, "col": ocol}, away & this)
                w.start(h2[p][j], src, dst, {"row": orow, "col": ocol, "dp": other}, this)

                @pl.when(~away & this)
                def _():
                    copy = pltpu.make_async_copy(src, dst, local.at[7])
                    copy.start()
                    copy.wait()

    for j in range(fold):
        srow, scol = col // fold, row * fold + j
        for p in range(count):

            @pl.when((srow != row) | (scol != col))
            def _():
                w.arrived(h1[p][j], ho.at[p, j, mine], {"row": srow, "col": scol})

            w.arrived(h2[p][j], ho.at[p, j, theirs], {"row": srow, "col": scol, "dp": other})
    for d in range(1, ncol):
        came = pl.ds(pl.multiple_of(from_col[d] * tokens, 128), tokens)
        w.arrived(c_[d], go.at[:, came], {"col": from_col[d]})
        w.arrived(hc[d], gho.at[from_col[d]], {"col": from_col[d]})
    for d in range(1, nrow):
        w.arrived(s4[d], smo.at[lax.rem(row - d + nrow, nrow)], {"row": lax.rem(row - d + nrow, nrow)})
    pltpu.make_async_copy(sc.at[0], go.at[:, place], local.at[5]).wait()
    pltpu.make_async_copy(hsc.at[col], gho.at[col], local.at[10]).wait()
    pltpu.make_async_copy(smb.at[last], smo.at[row], local.at[6]).wait()
    w.finish()


def leave(nrow, ncol, ndp, fold, gin, ginh, gw, gs, sm):
    unit = gin.shape[2:]
    hs, wide = gw.shape[2:]
    sh = wide // 2 // fold
    part = gs.shape[1] // ncol
    nb, nd = len(bits(ndp)), len(bits(ndp)) + len(bits(ncol))
    slots = 8 * ncol + 2 * nrow + nd + 2 * nb + 6 * fold + 12
    edge = ginh.shape[1:]
    return pl.pallas_call(
        functools.partial(leave_kernel, nrow, ncol, ndp, fold),
        out_shape=[
            jax.ShapeDtypeStruct((unit[0], ncol * unit[1]), BF16),
            jax.ShapeDtypeStruct(edge, BF16),
            jax.ShapeDtypeStruct((2, fold, 2 * hs, sh), BF16),
            jax.ShapeDtypeStruct((part, gs.shape[2]), F32),
            jax.ShapeDtypeStruct((nrow,) + sm.shape, F32),
        ],
        in_specs=[ANYWHERE] * 5,
        out_specs=[ANYWHERE, ANYWHERE, ANYWHERE, ONCHIP, ANYWHERE],
        scratch_shapes=[
            pltpu.VMEM((2, ncol) + unit, BF16),
            pltpu.VMEM((2, ncol) + unit, BF16),
            pltpu.VMEM((ncol,) + unit, BF16),
            pltpu.VMEM((ncol,) + unit, BF16),
            pltpu.VMEM((ncol,) + unit, BF16),
            pltpu.VMEM((2,) + edge, BF16),
            pltpu.VMEM((2,) + edge, BF16),
            pltpu.VMEM(edge, BF16),
            pltpu.VMEM(edge, BF16),
            pltpu.VMEM(edge, BF16),
            pltpu.VMEM((ncol, hs, wide), BF16),
            pltpu.VMEM((ncol, hs, wide), BF16),
            pltpu.VMEM((ncol, hs, wide), BF16),
            pltpu.VMEM((ncol, hs, wide), BF16),
            pltpu.VMEM((hs, wide), BF16),
            pltpu.VMEM((max(2 * nb - 2, 1), hs if ndp > 2 else 8, wide), F32),
            pltpu.VMEM(gs.shape[1:], BF16),
            pltpu.VMEM((nrow,) + gs.shape[1:], BF16),
            pltpu.VMEM(gs.shape[1:], BF16),
            pltpu.VMEM((ncol, part, gs.shape[2]), BF16),
            pltpu.VMEM((2 * nb + 1, part, gs.shape[2]), F32),
            pltpu.VMEM((nd + 1,) + sm.shape, F32),
            pltpu.VMEM((nd,) + sm.shape, F32),
            pltpu.SemaphoreType.DMA((9 * ncol + 20 + nd + 2 * nb + 6 * fold * fold,)),
            pltpu.SemaphoreType.DMA((slots,)),
            pltpu.SemaphoreType.DMA((11,)),
        ],
        compiler_params=pltpu.CompilerParams(
            collective_id=2, has_side_effects=True, vmem_limit_bytes=60 * 1024 * 1024
        ),
        name="leave",
    )(gin, ginh, gw, gs, sm)


def finish_kernel(x_ref, c_ref, r_ref, g_ref, h_ref, res_ref, gin_ref):
    step, steps = pl.program_id(0), pl.num_programs(0)
    tokens = x_ref.shape[1]
    res_ref[...] = x_ref[...].astype(F32) + r_ref[...].astype(F32)
    gin_ref[...] = c_ref[...].astype(F32) + g_ref[...].astype(F32)
    at = slice(tokens - 128, tokens)

    @pl.when(step < steps - 1)
    def _():
        gin_ref[:, at] += h_ref[0].astype(F32)


def adam_kernel(*refs):
    for i in range(len(refs) // 8):
        grad_ref, moment_ref, square_ref, weight_ref = refs[4 * i : 4 * i + 4]
        outs = refs[len(refs) // 2 + 4 * i : len(refs) // 2 + 4 * i + 4]
        grad = grad_ref[...].astype(F32)
        outs[0][...] = grad
        for out, value in zip(
            outs[1:], adamw_step(grad, moment_ref[...], square_ref[...], weight_ref[...].astype(F32))
        ):
            out[...] = value


def adam(sets, steps):
    ins, outs = [], []
    for arrays in sets:
        shape = arrays[1].shape
        block = (shape[0] // steps,) + shape[1:]
        ins += [(array, block, 0) for array in arrays]
        outs += [(shape, F32, block, 0)] * 4
    return call(adam_kernel, steps, ins, outs, [], False, "adam", 5)


def call(kernel, steps, ins, outs, scratch, reverse, name, cost, ident=None):
    def spec(block, axis, base=None):
        def index(step):
            at = steps - 1 - step if reverse else step
            return tuple(
                at if a == axis else (base[a] if base else 0) for a in range(len(block))
            )

        return pl.BlockSpec(block, index) if block is not None else ANYWHERE

    return pl.pallas_call(
        kernel,
        grid=(steps,),
        in_specs=[spec(*item[1:]) for item in ins],
        out_specs=[spec(block, axis) for _, _, block, axis in outs],
        out_shape=[jax.ShapeDtypeStruct(shape, dtype) for shape, dtype, _, _ in outs],
        scratch_shapes=scratch,
        compiler_params=pltpu.CompilerParams(
            dimension_semantics=("arbitrary",),
            vmem_limit_bytes=60 * 1024 * 1024,
            collective_id=ident,
            has_side_effects=ident is not None,
        ),
        cost_estimate=pl.CostEstimate(
            flops=int(cost * 1e9), bytes_accessed=int(cost * 1e6), transcendentals=0
        ),
        name=name,
    )(*[item[0] for item in ins])


def whole(array):
    return (array, array.shape, None)


def raw(array):
    return (array, None, None)


def part(array, block, base):
    return (array, block, None, base)


def lanes(array):
    return (array, array.shape[:-1] + (GROUP,), array.ndim - 1)


def sublanes(array, rows=GROUP):
    return (array, array.shape[:-2] + (rows,) + array.shape[-1:], array.ndim - 2)


def each(array):
    return (array, (1,) + array.shape[1:], 0)


def out_whole(shape, dtype):
    return (shape, dtype, shape, None)


def out_sub(shape, dtype, rows=GROUP):
    return (shape, dtype, shape[:-2] + (rows,) + shape[-1:], len(shape) - 2)


def out_lanes(shape, dtype):
    return (shape, dtype, shape[:-1] + (GROUP,), len(shape) - 1)


def out_each(shape, dtype):
    return (shape, dtype, (1,) + shape[1:], 0)


def adamw_step(grad, moment, square, weight):
    first_new = BETA_FIRST * moment + (1.0 - BETA_FIRST) * grad
    second_new = BETA_SECOND * square + (1.0 - BETA_SECOND) * grad * grad
    fix_first = 1.0 - BETA_FIRST**STEP
    fix_second = 1.0 - BETA_SECOND**STEP
    delta = -LEARN_RATE * (
        first_new / fix_first / (jnp.sqrt(second_new / fix_second) + ADAM_EPSILON)
        + WEIGHT_DECAY * weight
    )
    return (first_new, second_new, delta)


def local(
    inputs, segments, cotangent, pregain, innerweight, rateweight, stateweight, innerconv, stateconv, headparams,
    postgain, outweight, *moments,
):
    nrow, ncol, ndp = (lax.axis_size(a) for a in ("row", "col", "dp"))
    row, col = lax.axis_index("row"), lax.axis_index("col")
    length, own = inputs.shape[1], inputs.shape[2]
    width = own * nrow * ncol
    stored = innerweight.shape[1]
    total_heads = stored * ncol
    heads = total_heads // nrow
    hl = heads * HEADP
    count = total_heads * HEADP
    tokens = length // ncol
    steps = tokens // GROUP
    depth = width // nrow
    fold = ncol // nrow
    hops = (MOST - 2) // tokens + 1

    window = jnp.pad(segments[0], (HALO, HALO), constant_values=-1)
    window = lax.dynamic_slice_in_dim(window, col * tokens, tokens + 2 * HALO, 0)
    mine = window[HALO : HALO + tokens]
    flags = [mine]
    for j in (-1, -2, -3, 1, 2, 3):
        flags.append(window[HALO + j : HALO + j + tokens] == mine)
    before = window[HALO - 1 : HALO - 1 + tokens : GROUP]
    flags.append((mine.reshape(steps, GROUP) == before[:, None]).reshape(tokens))
    tok = jnp.stack([f.astype(F32) for f in flags])
    hmask = jnp.stack([(window[j : j + HALO] == window[:HALO]).astype(F32) for j in range(8)], 1)
    hmask = jnp.pad(hmask, ((0, 0), (0, 120)))

    block_heads = headparams.shape[1]
    xs, cs = inputs[0].T, cotangent[0].T
    smalls = [pregain, innerconv, headparams, postgain, rateweight, stateweight]
    flat = jnp.concatenate([a.reshape(-1) for a in smalls])
    ss = jnp.pad(flat, (0, -flat.size % 2048)).reshape(-1, 128)
    sub = depth // fold
    sh = stored * HEADP
    split = innerweight.reshape(depth, stored, 2, HEADP)
    ws = jnp.concatenate(
        [
            split[:, :, 0].reshape(depth, sh),
            split[:, :, 1].reshape(depth, sh),
            outweight.reshape(sh, depth).T,
        ],
        1,
    ).reshape(fold, sub, 3 * sh)

    x, xh, cot, weights, gathered = enter(nrow, ncol, ndp, fold, xs, cs, ws, ss)

    if fold > 1:
        weights = weights.reshape(ncol, fold, sub, 3, sh).transpose(0, 2, 3, 1, 4)
    weights = weights.reshape(width, 3 * hl)
    x, xh, cot = (a.reshape(width, a.shape[3]) for a in (x, xh, cot))
    gathered = gathered.reshape(nrow, ncol, -1)
    parts, at = [], 0
    for array in smalls:
        parts.append(gathered[:, :, at : at + array.size])
        at += array.size
    gain = jnp.broadcast_to(parts[0].reshape(width, 1).astype(F32), (width, 128))
    iconv = parts[1].reshape(nrow, ncol, 5, block_heads, HEADP).transpose(2, 1, 0, 3, 4)
    iconv = lax.dynamic_slice_in_dim(iconv.reshape(5, count), row * hl, hl, 1).astype(F32)
    hp = parts[2].reshape(nrow, ncol, 3, block_heads).transpose(2, 1, 0, 3)
    hp = lax.dynamic_slice_in_dim(hp.reshape(3, total_heads), row * heads, heads, 1).astype(F32)
    post = parts[3].reshape(nrow, ncol, block_heads * HEADP).transpose(1, 0, 2)
    post = lax.dynamic_slice_in_dim(post.reshape(1, count), row * hl, hl, 1).astype(F32)
    wrate = parts[4].reshape(nrow, ncol, depth, stored)
    wrate = wrate.transpose(1, 3, 0, 2).reshape(total_heads, width)
    wrate = lax.dynamic_slice_in_dim(wrate, row * heads, heads, 0)
    wrate = jnp.pad(wrate, ((0, 16 - heads), (0, 0)))
    wstate = parts[5].reshape(width, 2 * NSTATE)
    sconv = stateconv.astype(F32)
    head = jnp.broadcast_to(
        jnp.concatenate([-jnp.exp(hp[0]), hp[1]])[:, None], (2 * heads, 128)
    )
    skip = jnp.repeat(hp[2], HEADP)[None]

    spread = jnp.repeat(jnp.eye(heads, dtype=BF16), HEADP, 1)
    spread = jnp.concatenate([spread, spread], 0)
    triangle = jnp.triu(jnp.ones((GROUP, GROUP), BF16))
    ns2 = 2 * NSTATE
    x_in, xh_in, cot_in = lanes(x), whole(xh), lanes(cot)
    wmain = part(weights, (width, 2 * hl), (0, 0))
    woutt = part(weights, (width, hl), (0, 2))

    gate, pre, st, uv, us, bc, rows, states, prod, fin, total, preh, sth, rinvh = call(
        fwd1_kernel,
        steps,
        [x_in, xh_in, whole(gain), wmain, whole(wstate), whole(wrate), lanes(tok), whole(head),
         whole(iconv), whole(sconv), whole(triangle), whole(spread)],
        [out_sub((tokens, hl), F32), out_sub((tokens, hl), F32), out_sub((tokens, ns2), BF16),
         out_sub((tokens, hl), F32), out_sub((tokens, ns2), F32), out_sub((tokens, ns2), BF16),
         out_lanes((4 * heads, tokens), F32),
         out_each((steps, NSTATE, hl), BF16), out_each((steps, 8, hl), F32),
         out_whole((NSTATE, hl), F32), out_whole((8, hl), F32), out_whole((HALO, hl), BF16),
         out_whole((HALO, ns2), BF16), out_whole((HALO, 128), F32)],
        [pltpu.VMEM((GROUP + 8, hl + ns2), F32), pltpu.VMEM((NSTATE, hl), F32), pltpu.VMEM((8, hl), F32)],
        False,
        "fwd1",
        22,
    )
    total = total[0:1]
    sin = shift(ncol, 1, fin.astype(BF16), 3).astype(F32)
    for _ in range(hops - 1):
        sin = shift(ncol, 1, (fin + total * sin).astype(BF16), 3).astype(F32)

    scan, out, dn, stat = call(
        fwd2_kernel,
        steps,
        [sublanes(gate), sublanes(uv), sublanes(bc), lanes(rows), lanes(tok), each(states), each(prod), whole(sin),
         cot_in, whole(post), whole(skip), woutt, whole(spread)],
        [out_sub((tokens, hl), F32), out_lanes((nrow, depth, tokens), BF16), out_sub((tokens, hl), BF16),
         out_lanes((8, tokens), F32)],
        [],
        False,
        "fwd2",
        18,
    )
    scal = gather_stat(nrow, count, stat)

    dy, dg, leaving, prodb, first, gout, sums, root = call(
        bwd1_kernel,
        steps,
        [sublanes(gate), sublanes(uv), sublanes(bc), lanes(rows), lanes(tok), sublanes(scan), sublanes(dn),
         lanes(scal), cot_in, whole(post), whole(skip), whole(spread)],
        [out_sub((tokens, hl), BF16), out_sub((tokens, hl), BF16), out_each((steps, NSTATE, hl), BF16),
         out_each((steps, 8, hl), F32), out_whole((NSTATE, hl), F32), out_whole((width, hl), BF16),
         out_whole((16, hl), F32), out_lanes((8, tokens), F32)],
        [pltpu.VMEM((NSTATE, hl), F32), pltpu.VMEM((8, hl), F32), pltpu.VMEM((width, hl), F32)],
        True,
        "bwd1",
        15,
    )
    din = shift(ncol, -1, first.astype(BF16), 4).astype(F32)
    for _ in range(hops - 1):
        din = shift(ncol, -1, (first + total * din).astype(BF16), 4).astype(F32)

    hs = sub // 2
    home, ghout, gin, ginh, gw, gs, gr, gk, gh, gp = call(
        functools.partial(bwd2_kernel, (nrow, ncol, ndp, fold)),
        steps,
        [x_in, xh_in, whole(gain), wmain, whole(wstate), whole(wrate), lanes(tok), whole(head),
         whole(hmask), whole(rinvh), whole(iconv), whole(sconv), whole(triangle), whole(spread), whole(skip),
         sublanes(pre), sublanes(st), whole(preh), whole(sth), sublanes(uv), sublanes(us), sublanes(bc), lanes(rows),
         each(states), each(prod), whole(sin), sublanes(scan), sublanes(dy), sublanes(dg),
         each(leaving), each(prodb), whole(din), lanes(root), whole(scal),
         raw(out.reshape(nrow, ncol, own, tokens)), raw(gout.reshape(ncol, 2, hs, hl))],
        [((own, length), BF16, None, None), ((fold, sub, sh), BF16, None, None),
         out_lanes((nrow, depth, tokens), BF16), out_whole((nrow, depth, 128), BF16), out_whole((width, 2 * hl), BF16),
         out_whole((width, ns2), BF16), out_whole((16, width), F32), out_whole((40, hl + ns2), F32),
         out_whole((2 * heads, GROUP), F32), out_whole((width, 128), F32)],
        [pltpu.VMEM((GROUP + 8, hl + ns2), F32), pltpu.VMEM((width, 2 * hl + ns2), F32)]
        + delivery_scratch(nrow, ncol, ndp, fold, own, tokens, hs, hl),
        True,
        "bwd2",
        50,
        5,
    )

    gk = jnp.sum(gk.reshape(5, 8, -1), 1)
    gh = jnp.sum(gh, 1).reshape(2, heads)
    sums = jnp.sum(sums.reshape(2, 8, hl), 1)
    gskip = jnp.sum(sums[1].reshape(1, heads, HEADP), 2)
    small = [
        jnp.sum(gp, 1),
        gr[:heads],
        gk[:, :hl],
        gk[:, hl:],
        jnp.concatenate([gh, gskip]),
        sums[0],
    ]
    flat = jnp.concatenate([a.reshape(-1) for a in small])
    flat = jnp.pad(flat, (0, -flat.size % 1024)).reshape(-1, 128)
    gin, edge, ghome, gstate, flat = leave(
        nrow, ncol, ndp, fold,
        gin.reshape(nrow, ncol, own, tokens), ginh.reshape(nrow, ncol, own, 128),
        gw.reshape(ncol, 2, hs, 2 * hl), gs.reshape(nrow, depth, ns2), flat,
    )
    edge = jnp.concatenate([edge[1:], edge[:1]], 0)
    result, grad_input = call(
        finish_kernel,
        ncol,
        [(a, (own, tokens), 1) for a in (xs, cs, home, gin)] + [each(edge)],
        [((own, length), F32, (own, tokens), 1)] * 2,
        [],
        False,
        "finish",
        5,
    )
    result, grad_input = result.T[None], grad_input.T[None]

    ghome = ghome.reshape(2, depth, stored, HEADP)
    ginner = jnp.concatenate([ghome[0], ghome[1]], 2)
    gout = ghout.reshape(depth, sh).T.reshape(stored, HEADP, depth)
    updated = adam(
        [(ginner, moments[2], moments[3], innerweight), (gout, moments[16], moments[17], outweight)], 4
    )
    flat = flat.reshape(nrow, -1)
    parts, at = [], 0
    for array in small:
        parts.append(flat[:, at : at + array.size].reshape((nrow,) + array.shape))
        at += array.size
    feature = (row * ncol + col) * own
    block = col * nrow + row
    gpre = lax.dynamic_slice_in_dim(jnp.sum(parts[0], 0).reshape(-1), feature, own, 0)
    grate = lax.dynamic_slice(
        parts[1], (col // fold, (col % fold) * stored, row * depth), (1, stored, depth)
    )[0].T
    giconv = parts[2].transpose(1, 0, 2).reshape(5, count)
    wide = block_heads * HEADP
    giconv = lax.dynamic_slice_in_dim(giconv, block * wide, wide, 1)
    giconv = giconv.reshape(5, block_heads, HEADP)
    gsconv = jnp.sum(parts[3], 0)
    ghead = parts[4].transpose(1, 0, 2).reshape(3, total_heads)
    ghead = lax.dynamic_slice_in_dim(ghead, block * block_heads, block_heads, 1)
    gpost = lax.dynamic_slice_in_dim(parts[5].reshape(count), block * wide, wide, 0)
    gpost = gpost.reshape(block_heads, HEADP)

    grads = (gpre, None, grate, gstate, giconv, gsconv, ghead, gpost, None)
    params = (
        pregain, innerweight, rateweight, stateweight, innerconv, stateconv, headparams, postgain, outweight,
    )
    ready = {1: updated[:4], 8: updated[4:]}
    outputs = [result, grad_input]
    for i, (grad, param) in enumerate(zip(grads, params)):
        if i in ready:
            outputs.extend(ready[i])
            continue
        outputs.append(grad)
        outputs.extend(adamw_step(grad, moments[2 * i], moments[2 * i + 1], param.astype(F32)))
    return tuple(outputs)


def solution(mesh):
    tokens = P("dp", None, ("row", "col"))
    weights = (
        P(("row", "col")),
        P("row", "col", None),
        P("row", "col"),
        P(("row", "col"), None),
        P(None, ("col", "row"), None),
        P(),
        P(None, ("col", "row")),
        P(("col", "row"), None),
        P("col", None, "row"),
    )
    return jax.shard_map(
        local,
        mesh=mesh,
        in_specs=(tokens, P("dp", None), tokens)
        + weights
        + tuple(w for w in weights for _ in range(2)),
        out_specs=(tokens, tokens) + tuple(w for w in weights for _ in range(4)),
        check_vma=False,
    )
```

```python
import functools

import jax
import jax.numpy as jnp
from jax import lax
from jax.experimental import pallas as pl
from jax.experimental.pallas import tpu as pltpu
from jax.sharding import PartitionSpec as P

HEADP = 64
NSTATE = 128
GROUP = 256
MOST = 2000
STEP = 4
HALO = 16
NORM_EPSILON = 1e-05
ADAM_EPSILON = 1e-08
BETA_FIRST = 0.5
BETA_SECOND = 0.5
LEARN_RATE = 0.02
WEIGHT_DECAY = 0.1
FAR = -1e30

F32 = jnp.float32
BF16 = jnp.bfloat16


def dot(a, b, ca, cb):
    return lax.dot_general(a, b, (((ca,), (cb,)), ((), ())), preferred_element_type=F32)


def mm(a, b):
    return dot(a, b, 1, 0)


def mm_nt(a, b):
    return dot(a, b, 1, 1)


def mm_tn(a, b):
    return dot(a, b, 0, 0)


def sigmoid(v):
    return 0.5 * jnp.tanh(0.5 * v) + 0.5


def halves(v):
    high = v.astype(BF16)
    return high, (v - high.astype(F32)).astype(BF16)


def stack_parts(v, count):
    parts = []
    for _ in range(count):
        high = v.astype(BF16).astype(F32)
        parts.append(high)
        v = v - high
    return parts


def expand(rows, spread):
    high, low = stack_parts(rows, 2)
    return mm_tn(jnp.concatenate([high, low], 0).astype(BF16), spread)


def head_sums(v, spread):
    high, low = halves(v)
    sums = mm_nt(spread, high) + mm_nt(spread, low)
    return sums[: sums.shape[0] // 2]


def lane_sums(v):
    total = v[:, :128]
    for at in range(128, v.shape[1], 128):
        total = total + v[:, at : at + 128]
    high, low = halves(total)
    return mm_nt(jnp.ones((16, 256), BF16), jnp.concatenate([high, low], 1))[:8]


def running(rows, triangle, product=mm):
    count = rows.shape[0]
    parts = stack_parts(rows, 3) + [jnp.zeros_like(rows)]
    sums = product(jnp.concatenate(parts, 0).astype(BF16), triangle)
    return sums[:count] + sums[count : 2 * count] + sums[2 * count : 3 * count]


def softplus(v):
    return jnp.maximum(v, 0.0) + jnp.log1p(jnp.exp(-jnp.abs(v)))


def turned(row, count):
    return jnp.broadcast_to(row, (8, count)).T[:, 0:1]


def chunk_decay(cum, rates, tok):
    last = cum[:, GROUP - 1 : GROUP]
    tail = (tok[0:1] == tok[0:1, GROUP - 1 : GROUP]).astype(F32)
    to_end = jnp.exp(last - cum) * tail
    enter = jnp.exp(cum) * tok[7:8]
    return to_end, enter


def fwd1_kernel(
    x_ref, xh_ref, gain_ref, wmain_ref, wstate_ref, wrate_ref, tok_ref, head_ref,
    kin_ref, kst_ref, tri_ref, spread_ref,
    gate_ref, pre_ref, st_ref, uv_ref, us_ref, bc_ref, rows_ref, sent_ref, prod_ref, fin_ref, total_ref, preh_ref, sth_ref, rinvh_ref,
    ext, state, prod,
):
    k = pl.program_id(0)
    width = x_ref.shape[0]
    hl = gate_ref.shape[1]
    heads = hl // HEADP

    def project(x):
        xf = x.astype(F32)
        rinv = lax.rsqrt(jnp.sum(xf * xf, axis=0, keepdims=True) / width + NORM_EPSILON)
        gain = gain_ref[...]
        if x.shape[1] > 128:
            gain = jnp.concatenate([gain] * (x.shape[1] // 128), 1)
        xn = (xf * gain).astype(BF16)
        col = turned(rinv, x.shape[1])
        return xn, rinv, col, mm_tn(xn, wmain_ref[...]) * col, (mm_tn(xn, wstate_ref[...]) * col).astype(BF16)

    @pl.when(k == 0)
    def _():
        _, _, rinv, main, state_in = project(xh_ref[...])
        at = slice(128 - HALO, 128)
        pre = main[at, hl:]
        preh_ref[...] = pre.astype(BF16)
        sth_ref[...] = state_in[at]
        rinvh_ref[...] = jnp.broadcast_to(rinv[at], (HALO, 128))
        ext[0:8, :hl] = pre[HALO - 8 :]
        ext[0:8, hl:] = state_in.astype(F32)[128 - 8 :]
        state[...] = jnp.zeros_like(state)
        prod[...] = jnp.ones_like(prod)

    xn, rinv, _, main, state_in = project(x_ref[...])
    gate_ref[...] = main[:, :hl]
    pre = main[:, hl:]
    pre_ref[...] = pre
    st_ref[...] = state_in
    ext[8:, :hl] = pre.astype(F32)
    ext[8:, hl:] = state_in.astype(F32)
    tok = tok_ref[...]
    cols = tok.T
    kernel = jnp.concatenate([kin_ref[...], kst_ref[...]], 1)
    u = ext[8:, :] * kernel[0:1] + kernel[4:5]
    for j in range(1, 4):
        u = u + ext[pl.ds(8 - j, GROUP), :] * cols[:, j : j + 1] * kernel[j : j + 1]
    ext[0:8, :] = ext[GROUP : GROUP + 8, :]
    uv_ref[...] = u[:, :hl]
    us_ref[...] = u[:, hl:]
    u = u.astype(F32)
    act = u * sigmoid(u)
    values = act[:, :hl]
    bc = act[:, hl:].astype(BF16)
    bc_ref[...] = bc
    rate = mm(wrate_ref[...], xn)
    rinv_row = jnp.broadcast_to(rinv, (heads, GROUP))
    rin = rate[:heads] * rinv_row + head_ref[heads : 2 * heads, 0:1]
    rates = softplus(rin)
    cum = running(head_ref[0:heads, 0:1] * rates, tri_ref[...])
    rows_ref[0:heads] = rin
    rows_ref[heads : 2 * heads] = rates
    rows_ref[2 * heads : 3 * heads] = cum
    rows_ref[3 * heads :] = rinv_row
    to_end, _ = chunk_decay(cum, rates, tok)
    both = expand(to_end * rates, spread_ref[...])
    scaled = (values * both).astype(BF16)
    carry = jnp.exp(cum[:, GROUP - 1 :]) * tok[7:8, GROUP - 1 :]
    carry = expand(jnp.broadcast_to(carry, (heads, 128)), spread_ref[...])[0:8]
    sent_ref[0] = state[...].astype(BF16)
    prod_ref[0] = prod[...]
    state[...] = state[...] * carry[0:1] + mm_tn(bc[:, :NSTATE], scaled)
    prod[...] = prod[...] * carry
    fin_ref[...] = state[...].astype(BF16)
    total_ref[...] = prod[...]


def pair_lanes(shape):
    return lax.broadcasted_iota(jnp.int32, shape, 1) < HEADP


def chunk_mask(tok, cols):
    rowpos = lax.broadcasted_iota(jnp.int32, (GROUP, GROUP), 0)
    colpos = lax.broadcasted_iota(jnp.int32, (GROUP, GROUP), 1)
    same = (cols[:, 0:1] == tok[0:1, :]) & (colpos <= rowpos)
    return jnp.where(same, 0.0, FAR)


def fwd2_kernel(
    gate_ref, uv_ref, bc_ref, rows_ref, tok_ref, sent_ref, prod_ref, sin_ref, cot_ref, post_ref, skip_ref,
    woutt_ref, spread_ref,
    scan_ref, out_ref, dn_ref, stat_ref,
):
    row = lax.axis_index("row")
    hl = gate_ref.shape[1]
    heads = hl // HEADP
    blocks, depth, _ = out_ref.shape
    tok = tok_ref[...]
    cum = rows_ref[2 * heads : 3 * heads]
    rates = rows_ref[heads : 2 * heads]
    _, enter = chunk_decay(cum, rates, tok)
    spread = spread_ref[...]
    cols = jnp.concatenate([tok, cum], 0).T
    mask = chunk_mask(tok, cols)
    bm, cm = bc_ref[:, :NSTATE], bc_ref[:, NSTATE:]
    scores = mm_nt(cm, bm)
    u = uv_ref[...].astype(F32)
    values = u * sigmoid(u)
    scaled = (values * expand(rates, spread)).astype(BF16)
    entering = (sent_ref[0].astype(F32) + prod_ref[0, 0:1] * sin_ref[...].astype(F32)).astype(BF16)
    outer = mm(cm, entering) * expand(enter, spread)
    first = pair_lanes((GROUP, 128))
    pieces = []
    for pair in range(heads // 2):
        vp = scaled[:, pair * 128 : (pair + 1) * 128]
        ys = []
        for h in (2 * pair, 2 * pair + 1):
            decay = jnp.exp(cols[:, 8 + h : 9 + h] - cum[h : h + 1, :] + mask)
            ys.append(mm((scores * decay).astype(BF16), vp))
        pieces.append(jnp.where(first, ys[0], ys[1]))
    scan = jnp.concatenate(pieces, 1) + outer
    scan_ref[...] = scan
    g = gate_ref[...].astype(F32)
    gated = (scan + skip_ref[...] * values) * (g * sigmoid(g))
    post = post_ref[...]
    dn = mm_tn(cot_ref[...], woutt_ref[...])
    dn = dn.astype(BF16)
    dn_ref[...] = dn
    normed = gated * post
    squares, inner = lane_sums(gated * gated), lane_sums(dn.astype(F32) * normed)
    stat_ref[...] = jnp.where(
        lax.broadcasted_iota(jnp.int32, squares.shape, 0) == 0, squares, inner
    )
    normed = normed.astype(BF16)
    for i in range(blocks):
        block = mm_nt(woutt_ref[pl.ds(i * depth, depth), :], normed)
        out_ref[jnp.bitwise_xor(row, i)] = block.astype(BF16)


def bwd1_kernel(
    gate_ref, uv_ref, bc_ref, rows_ref, tok_ref, scan_ref, dn_ref, scal_ref, cot_ref, post_ref, skip_ref, spread_ref,
    dy_ref, dg_ref, leave_ref, prodb_ref, first_ref, gout_ref, sums_ref, root_ref,
    adj, prod, gacc,
):
    step = pl.program_id(0)
    hl = gate_ref.shape[1]
    heads = hl // HEADP
    tok = tok_ref[...]
    cum = rows_ref[2 * heads : 3 * heads]
    spread = spread_ref[...]

    @pl.when(step == 0)
    def _():
        adj[...] = jnp.zeros_like(adj)
        prod[...] = jnp.ones_like(prod)
        gacc[...] = jnp.zeros_like(gacc)
        sums_ref[...] = jnp.zeros_like(sums_ref)

    enter = jnp.exp(cum) * tok[7:8]
    scal = scal_ref[...]
    cols = jnp.concatenate([scal, rows_ref[3 * heads :]], 0).T
    rootgate, pull, rinv = cols[:, 0:1], cols[:, 1:2], cols[:, 8:9]
    u = uv_ref[...].astype(F32)
    values = u * sigmoid(u)
    mixed = scan_ref[...] + skip_ref[...] * values
    g = gate_ref[...].astype(F32)
    sg = sigmoid(g)
    act = g * sg
    gated = mixed * act
    post = post_ref[...]
    dn = dn_ref[...].astype(F32)
    dgated = rootgate * (dn * post) - gated * pull
    dy = dgated * act
    dyb = dy.astype(BF16)
    dy_ref[...] = dyb
    dgate = dgated * mixed * (sg + act * (1.0 - sg)) * rinv
    dg_ref[...] = dgate.astype(BF16)
    root_ref[...] = lane_sums(dgate * g)
    ng = gated * rootgate
    sums_ref[0:8] += jnp.sum((dn * ng).reshape(GROUP // 8, 8, hl), 0)
    sums_ref[8:16] += jnp.sum((dy * values).reshape(GROUP // 8, 8, hl), 0)
    normout = (ng * post).astype(BF16)
    gacc[...] += mm(cot_ref[...], normout)

    @pl.when(step == pl.num_programs(0) - 1)
    def _():
        gout_ref[...] = gacc[...].astype(BF16)

    cm = bc_ref[:, NSTATE:]
    weighted = (dyb.astype(F32) * expand(enter, spread)).astype(BF16)
    carry = jnp.exp(cum[:, GROUP - 1 :]) * tok[7:8, GROUP - 1 :]
    carry = expand(jnp.broadcast_to(carry, (heads, 128)), spread)[0:8]
    leave_ref[0] = adj[...].astype(BF16)
    prodb_ref[0] = prod[...]
    adj[...] = adj[...] * carry[0:1] + mm_tn(cm, weighted)
    prod[...] = prod[...] * carry
    first_ref[...] = adj[...].astype(BF16)


class Delivery:
    def __init__(self, dims, refs, scal):
        nrow, ncol, ndp, fold = self.dims = dims
        (
            self.out, self.gout, self.home, self.hout,
            self.own, self.ra, self.rb, self.sb, self.sc, self.gv, self.ry, self.sy, self.rz, self.fin, self.rdp,
            send, recv, self.local,
        ) = refs
        self.scal = scal
        self.step, self.last = pl.program_id(0), pl.num_programs(0) - 1
        row, col, dp = (lax.axis_index(a) for a in ("row", "col", "dp"))
        w = self.w = Wires(send, recv)
        near, far, other, half = flip(row, 1), flip(row, 2), flip(dp, 1), lax.rem(dp, 2)
        self.plan = plan = order(ncol)[::-1]
        cols = [lax.rem(col + d, ncol) for d in range(ncol)]
        back = [lax.rem(col - d + ncol, ncol) for d in range(ncol)]
        tokens = self.out.shape[3]
        hs, sh = self.fin.shape[0], self.hout.shape[2]
        places = [pl.ds(pl.multiple_of(c * tokens, 128), tokens) for c in back]
        rows = [pl.ds(half * hs, hs), pl.ds((1 - half) * hs, hs)]
        self.starts = {name: [] for name in ("a", "y", "b", "c", "z", "h")}
        self.takes = {name: [] for name in ("a0", "a1", "y", "b", "c", "z", "h")}

        def wire(kind, at, src, dst, to, when=None):
            slot = w.slot()
            self.starts[kind].append((at, w.copy(slot, src, dst, to), when))
            w.sent.append(None)
            return slot

        def take(kind, at, slot, ref, to, when=None):
            self.takes[kind].append((at, w.copy(slot, ref, ref, to), when))

        for d in plan:
            take("a1", d, wire("a", d, self.out.at[3, cols[d]], self.ra.at[1, d], {"row": near}), self.ra.at[1, d], {"row": near})
            take("a0", d, wire("a", d, self.out.at[1, cols[d]], self.ra.at[0, d], {"row": near}), self.ra.at[0, d], {"row": near})
            take("y", d, wire("y", d, self.gout.at[cols[d], 1 - half], self.ry.at[d], {"dp": other}), self.ry.at[d], {"dp": other})
            take("b", d, wire("b", d, self.sb.at[d], self.rb.at[d], {"row": far}), self.rb.at[d], {"row": far})
            if d:
                to, come = {"col": cols[d]}, {"col": back[d]}
                slot = wire("c", d, self.sc.at[d], self.home.at[:, places[0]], to)
                take("c", d, slot, self.home.at[:, places[d]], come)
                take("z", d, wire("z", d, self.sy.at[d], self.rz.at[d], to), self.rz.at[d], come)
        self.cols = cols
        self.stays = pltpu.make_async_copy(self.sc.at[0], self.home.at[:, places[0]], self.local.at[3])
        self.loads = [
            pltpu.make_async_copy(self.out.at[0], self.own.at[0], self.local.at[0]),
            pltpu.make_async_copy(self.out.at[2], self.own.at[1], self.local.at[1]),
            pltpu.make_async_copy(self.gout.at[:, half], self.gv, self.local.at[2]),
        ]
        self.hops = []
        for i, bit in enumerate(bits(ndp)[1:]):
            to = {"dp": flip(dp, bit)}
            self.hops.append(w.copy(w.slot(), self.rdp.at[2 * i], self.rdp.at[2 * i + 1], to))
            w.sent.append(None)
        self.keeps = []
        for i in range(fold):
            orow, ocol = col // fold, row * fold + i
            away = (orow != row) | (ocol != col)
            src = self.fin.at[:, pl.ds(i * sh, sh)]
            for j in range(fold):
                this = lax.rem(col, fold) == j
                dst = self.hout.at[j, rows[0]]
                near_slot, far_slot = w.slot(), w.slot()
                if i == 0:
                    self.slots = getattr(self, "slots", []) + [(near_slot, far_slot)]
                near_slot, far_slot = self.slots[j]
                to = {"row": orow, "col": ocol}
                self.starts["h"].append((j, w.copy(near_slot, src, dst, to), away & this))
                w.sent.append(None)
                self.starts["h"].append((j, w.copy(far_slot, src, dst, to | {"dp": other}), this))
                w.sent.append(None)
                keep = pltpu.make_async_copy(src, dst, self.local.at[4])
                self.keeps.append((keep, ~away & this))
        for j in range(fold):
            srow, scol = col // fold, row * fold + j
            to = {"row": srow, "col": scol}
            take("h", j, self.slots[j][0], self.hout.at[j, rows[0]], to, (srow != row) | (scol != col))
            take("h", j, self.slots[j][1], self.hout.at[j, rows[1]], to | {"dp": other})

    def go(self, kind, at=None):
        for d, copy, when in self.starts[kind]:
            if at is None or d == at:
                copy.start() if when is None else pl.when(when)(copy.start)

    def come(self, kind, at=None):
        for d, copy, when in self.takes[kind]:
            if at is None or d == at:
                copy.wait_recv() if when is None else pl.when(when)(copy.wait_recv)

    def before(self):
        nrow, ncol, ndp, fold = self.dims
        step, last, plan = self.step, self.last, self.plan

        @pl.when(step == 0)
        def _():
            greet(nrow, ncol, ndp)
            self.go("a")
            self.go("y")
            for load in self.loads:
                load.start()

        @pl.when(step == 1)
        def _():
            for load in self.loads:
                load.wait()
            for d in plan:
                self.come("a1", d)
                self.sb[d] = (self.own[1, self.cols[d]].astype(F32) + self.ra[1, d].astype(F32)).astype(BF16)
                self.go("b", d)

        for i, d in enumerate(plan):

            @pl.when(step == jnp.minimum(2 + i, last - 1))
            def _():
                if i == 0:
                    self.weights()
                self.come("a0", d)
                self.come("b", d)
                total = self.own[0, self.cols[d]].astype(F32) + self.ra[0, d].astype(F32) + self.rb[d].astype(F32)
                self.sc[d] = (total * self.scal[0:1]).astype(BF16)
                if d:
                    self.go("c", d)
                else:
                    self.stays.start()

        @pl.when(step == jnp.minimum(6, last))
        def _():
            self.homeward()

    def weights(self):
        if True:
            for d in self.plan:
                self.come("y", d)
                self.sy[d] = (self.gv[self.cols[d]].astype(F32) + self.ry[d].astype(F32)).astype(BF16)
                if d:
                    self.go("z", d)

    def homeward(self):
        if True:
            total = self.sy[0].astype(F32)
            for d in range(1, self.dims[1]):
                self.come("z", d)
                total = total + self.rz[d].astype(F32)
            for i, hop in enumerate(self.hops):
                self.rdp[2 * i] = total
                hop.start()
                hop.wait_recv()
                total = total + self.rdp[2 * i + 1]
            self.fin[...] = total.astype(BF16)
            self.go("h")
            for keep, when in self.keeps:
                pl.when(when)(keep.start)

    def after(self):
        @pl.when(self.step == self.last)
        def _():
            for keep, when in self.keeps:
                pl.when(when)(keep.wait)
            self.come("h")
            self.come("c")
            self.stays.wait()
            for hop in self.hops:
                hop.wait_send()
            for copies in self.starts.values():
                for _, copy, when in copies:
                    copy.wait_send() if when is None else pl.when(when)(copy.wait_send)


def delivery_scratch(nrow, ncol, ndp, fold, own, tokens, hs, hl):
    nb = len(bits(ndp))
    slots = 8 * ncol + nb + 2 * fold * fold + 4
    return [
        pltpu.VMEM((2, ncol, own, tokens), BF16),
        pltpu.VMEM((2, ncol, own, tokens), BF16),
        pltpu.VMEM((ncol, own, tokens), BF16),
        pltpu.VMEM((ncol, own, tokens), BF16),
        pltpu.VMEM((ncol, own, tokens), BF16),
        pltpu.VMEM((ncol, hs, hl), BF16),
        pltpu.VMEM((ncol, hs, hl), BF16),
        pltpu.VMEM((ncol, hs, hl), BF16),
        pltpu.VMEM((ncol, hs, hl), BF16),
        pltpu.VMEM((hs, hl), BF16),
        pltpu.VMEM((max(2 * nb - 2, 1), hs if ndp > 2 else 8, hl), F32),
        pltpu.SemaphoreType.DMA((slots,)),
        pltpu.SemaphoreType.DMA((slots,)),
        pltpu.SemaphoreType.DMA((5,)),
    ]


def bwd2_kernel(
    dims,
    x_ref, xh_ref, gain_ref, wmain_ref, wstate_ref, wrate_ref, tok_ref, head_ref, hmask_ref, hrinv_ref,
    kin_ref, kst_ref, tri_ref, spread_ref, skip_ref,
    pre_ref, st_ref, preh_ref, sth_ref, uv_ref, us_ref, bc_ref, rows_ref, sent_ref, prod_ref, sin_ref,
    scan_ref, dy_ref, dg_ref, leave_ref, prodb_ref, din_ref, root_ref, scal_ref, outs_ref, gout_ref,
    home_ref, hout_ref, gin_ref, ginh_ref, gw_ref, gs_ref, gr_ref, gk_ref, gh_ref, gp_ref,
    ext, gacc, *more,
):
    delivery = Delivery(dims, (outs_ref, gout_ref, home_ref, hout_ref) + more, scal_ref)
    delivery.before()
    step = pl.program_id(0)
    steps = pl.num_programs(0)
    row = lax.axis_index("row")
    hl = uv_ref.shape[1]
    heads = hl // HEADP
    width = x_ref.shape[0]
    blocks, depth, _ = gin_ref.shape
    tok = tok_ref[...]
    spread = spread_ref[...]
    rin = rows_ref[0:heads]
    rates = rows_ref[heads : 2 * heads]
    cum = rows_ref[2 * heads : 3 * heads]
    rinv_row = rows_ref[3 * heads :]
    cols = jnp.concatenate([tok, cum, rinv_row], 0).T
    rinv = cols[:, 16:17]

    @pl.when(step == 0)
    def _():
        ext[GROUP:, :] = jnp.zeros_like(ext[GROUP:, :])
        gacc[...] = jnp.zeros_like(gacc)
        gr_ref[...] = jnp.zeros_like(gr_ref)
        gk_ref[...] = jnp.zeros_like(gk_ref)
        gh_ref[...] = jnp.zeros_like(gh_ref)
        gp_ref[...] = jnp.zeros_like(gp_ref)

    to_end, enter = chunk_decay(cum, rates, tok)
    mask = chunk_mask(tok, cols)
    bm, cm = bc_ref[:, :NSTATE], bc_ref[:, NSTATE:]
    scores = mm_nt(cm, bm)
    u = uv_ref[...].astype(F32)
    sg = sigmoid(u)
    values = u * sg
    rexp = expand(rates, spread)
    scaled = (values * rexp).astype(BF16)
    dyb = dy_ref[...]
    entering = (sent_ref[0].astype(F32) + prod_ref[0, 0:1] * sin_ref[...].astype(F32)).astype(BF16)
    leaving = (leave_ref[0].astype(F32) + prodb_ref[0, 0:1] * din_ref[...].astype(F32)).astype(BF16)

    first = pair_lanes((GROUP, 128))
    dscores = jnp.zeros((GROUP, GROUP), F32)
    pieces = []
    for pair in range(heads // 2):
        vp = scaled[:, pair * 128 : (pair + 1) * 128]
        dp = dyb[:, pair * 128 : (pair + 1) * 128]
        dvs = []
        for h in (2 * pair, 2 * pair + 1):
            decay = jnp.exp(cols[:, 8 + h : 9 + h] - cum[h : h + 1, :] + mask)
            weight = (scores * decay).astype(BF16)
            own = first if h % 2 == 0 else ~first
            dh = jnp.where(own, dp, jnp.zeros_like(dp))
            dscores = dscores + mm_nt(dh, vp) * decay
            dvs.append(mm_tn(weight, dp))
        pieces.append(jnp.where(first, dvs[0], dvs[1]))
    tend = expand(to_end, spread)
    inside = jnp.concatenate(pieces, 1)
    onward = mm(bm, leaving) * tend
    dscaled = inside + onward
    dsb = dscores.astype(BF16)
    dyf = dyb.astype(F32)
    weighted = (dyf * expand(enter, spread)).astype(BF16)
    ended = (values * (tend * rexp)).astype(BF16)
    dcm = mm(dsb, bm) + mm_nt(weighted, entering)
    dbm = mm_tn(dsb, cm) + mm_nt(ended, leaving)
    dvalues = dscaled * rexp + skip_ref[...] * dyf

    kept = scaled.astype(F32)
    dcum = head_sums(dyf * scan_ref[...] - kept * inside, spread)
    dend = head_sums(kept * onward, spread)
    drates = head_sums(values * dscaled, spread)
    through = leaving.astype(F32) * entering.astype(F32)
    through = head_sums(jnp.sum(through.reshape(NSTATE // 8, 8, hl), 0), spread)
    through = jnp.sum(through, axis=1, keepdims=True) * (
        jnp.exp(cum[:, GROUP - 1 :]) * tok[7:8, GROUP - 1 :]
    )
    ddec = running(dcum, tri_ref[...], mm_nt) + running(dend, tri_ref[...]) - dend + through
    drates = drates + head_ref[0:heads, 0:1] * ddec
    drin = drates * sigmoid(rin)
    gh_ref[0:heads] += ddec * (head_ref[0:heads, 0:1] * rates)
    gh_ref[heads : 2 * heads] += drin

    us = us_ref[...].astype(F32)
    ss = sigmoid(us)
    dstates = jnp.concatenate([dbm, dcm], 1)
    ext[0:GROUP, :hl] = dvalues * (sg + values * (1.0 - sg))
    ext[0:GROUP, hl:] = dstates * (ss + us * ss * (1.0 - ss))
    kernel = jnp.concatenate([kin_ref[...], kst_ref[...]], 1)
    source = jnp.concatenate([pre_ref[...], st_ref[...]], 1).astype(F32)
    du = ext[0:GROUP, :]
    gk_ref[32:40] += jnp.sum(du.reshape(GROUP // 8, 8, du.shape[1]), 0)
    gk_ref[0:8] += jnp.sum((du * source).reshape(GROUP // 8, 8, du.shape[1]), 0)
    dsource = du * kernel[0:1]
    for j in range(1, 4):
        moved = ext[pl.ds(j, GROUP), :] * cols[:, 3 + j : 4 + j]
        gk_ref[8 * j : 8 * j + 8] += jnp.sum(
            (moved * source).reshape(GROUP // 8, 8, du.shape[1]), 0
        )
        dsource = dsource + moved * kernel[j : j + 1]
    low = dsource * rinv
    lowb = low.astype(BF16)
    root = lane_sums(low * source) + root_ref[...] + jnp.sum(
        drin * (rin - head_ref[heads : 2 * heads, 0:1]), 0, keepdims=True
    ) * rinv_row[0:1]
    root = root[0:1] * rinv_row[0:1] / width
    ratelow = (drin * rinv_row).astype(F32)
    ratelow = jnp.concatenate([ratelow, jnp.zeros_like(ratelow)], 0).astype(BF16)
    gates = dg_ref[...]
    xf = x_ref[...].astype(F32)
    gain = jnp.concatenate([gain_ref[...]] * (GROUP // 128), 1)
    xn = (xf * gain).astype(BF16)
    gacc[:, 0:hl] += mm(xn, gates)
    gacc[:, hl:] += mm(xn, lowb)
    gr_ref[...] += mm_nt(ratelow, xn)
    dn = (
        mm_nt(wmain_ref[:, 0:hl], gates)
        + mm_nt(wmain_ref[:, hl:], lowb[:, :hl])
        + mm_nt(wstate_ref[...], lowb[:, hl:])
        + mm_tn(wrate_ref[...], ratelow)
    )
    both = dn * xf
    for at in range(0, GROUP, 128):
        gp_ref[...] += both[:, at : at + 128]
    grad = (dn * gain - xf * root).astype(BF16)
    for i in range(blocks):
        gin_ref[jnp.bitwise_xor(row, i)] = grad[i * depth : (i + 1) * depth]

    ext[GROUP : GROUP + 8, :] = ext[0:8, :]

    @pl.when(step == steps - 1)
    def _():
        wide = ext.shape[1]
        source_h = jnp.concatenate([preh_ref[...], sth_ref[...]], 1).astype(F32)
        head8 = ext[GROUP : GROUP + 8, :]
        ext[0:HALO, :] = jnp.zeros((HALO, wide), F32)
        ext[HALO : HALO + 8, :] = head8
        dsource_h = jnp.zeros((HALO, wide), F32)
        for j in range(1, 4):
            moved = ext[pl.ds(j, HALO), :] * hmask_ref[:, j : j + 1]
            gk_ref[8 * j : 8 * j + 8] += jnp.sum(
                (moved * source_h).reshape(HALO // 8, 8, wide), 0
            )
            dsource_h = dsource_h + moved * kernel[j : j + 1]
        rinv_h = hrinv_ref[:, 0:1]
        low_h = dsource_h * rinv_h
        root_h = jnp.sum(low_h * source_h, axis=1, keepdims=True) * rinv_h / width
        fill = jnp.zeros((128 - HALO, wide), F32)
        lowb_h = jnp.concatenate([fill, low_h], 0).astype(BF16)
        root_h = jnp.concatenate([jnp.zeros((128 - HALO, 1), F32), root_h], 0)
        root_h = jnp.broadcast_to(root_h, (128, 128)).T[0:1]
        xf = xh_ref[...].astype(F32)
        gain = gain_ref[...]
        gacc[:, hl:] += mm((xf * gain).astype(BF16), lowb_h)
        dn = mm_nt(wmain_ref[:, hl:], lowb_h[:, :hl]) + mm_nt(wstate_ref[...], lowb_h[:, hl:])
        gp_ref[...] += dn * xf
        grad = (dn * gain - xf * root_h).astype(BF16)
        for i in range(blocks):
            ginh_ref[jnp.bitwise_xor(row, i)] = grad[i * depth : (i + 1) * depth]
        gw_ref[...] = gacc[:, 0 : 2 * hl].astype(BF16)
        gs_ref[...] = gacc[:, 2 * hl :].astype(BF16)

    delivery.after()


MESH = pl.DeviceIdType.MESH


class Wires:
    def __init__(self, send, recv):
        self.sends, self.recv, self.used, self.sent = send, recv, 0, []

    def slot(self):
        self.used += 1
        return self.used - 1

    def copy(self, slot, src, dst, to):
        return pltpu.make_async_remote_copy(
            src_ref=src,
            dst_ref=dst,
            send_sem=self.sends.at[len(self.sent)],
            recv_sem=self.recv.at[slot],
            device_id=to,
            device_id_type=MESH,
        )

    def start(self, slot, src, dst, to, when=None):
        copy = self.copy(slot, src, dst, to)
        if when is None:
            copy.start()
        else:
            pl.when(when)(copy.start)
        self.sent.append((copy, when))

    def arrived(self, slot, ref, to):
        pltpu.make_async_remote_copy(
            src_ref=ref,
            dst_ref=ref,
            send_sem=self.sends.at[0],
            recv_sem=self.recv.at[slot],
            device_id=to,
            device_id_type=MESH,
        ).wait_recv()

    def finish(self):
        for copy, when in self.sent:
            if when is None:
                copy.wait_send()
            else:
                pl.when(when)(copy.wait_send)


def greet(nrow, ncol, ndp):
    row, col, dp = (lax.axis_index(a) for a in ("row", "col", "dp"))
    sem = pltpu.get_barrier_semaphore()
    total = 0
    for i in range(nrow):
        for j in range(ncol):
            if i or j:
                to = {"row": lax.rem(row + i, nrow), "col": lax.rem(col + j, ncol)}
                pl.semaphore_signal(sem, 1, device_id=to, device_id_type=MESH)
                total += 1
    for bit in bits(ndp):
        pl.semaphore_signal(sem, 1, device_id={"dp": flip(dp, bit)}, device_id_type=MESH)
        total += 1
    pl.semaphore_wait(sem, total)


def bits(size):
    found, bit = [], 1
    while bit < size:
        found.append(bit)
        bit *= 2
    return found


def flip(index, bit):
    return index + bit - 2 * bit * lax.rem(index // bit, 2)


def order(ncol):
    near = [0]
    for d in range(1, ncol // 2 + 1):
        near.extend([d, ncol - d] if ncol - d != d else [d])
    return near


class Spread:
    def __init__(self, wires, ncol, source, out):
        self.w, self.ncol, self.source, self.out = wires, ncol, source, out
        self.row, self.col = lax.axis_index("row"), lax.axis_index("col")
        self.far, self.near = flip(self.row, 2), flip(self.row, 1)
        self.a = [wires.slot() for _ in range(ncol)]
        self.b = [wires.slot() for _ in range(ncol)]
        self.e = [wires.slot() for _ in range(ncol)]
        self.f = [wires.slot() for _ in range(ncol)]

    def begin(self):
        for d in order(self.ncol)[:0:-1]:
            to = lax.rem(self.col + d, self.ncol)
            self.w.start(self.a[d], self.source(to), self.out.at[self.row, self.col], {"col": to})

    def forward(self, d):
        at = lax.rem(self.col - d + self.ncol, self.ncol)
        place = self.out.at[self.row, at]
        src = place
        if d:
            self.w.arrived(self.a[d], place, {"col": at})
        else:
            src = self.source(self.col)
        self.w.start(self.b[d], src, place, {"row": self.far})
        self.w.start(self.e[d], src, place, {"row": self.near})

    def relay(self, d):
        at = lax.rem(self.col - d + self.ncol, self.ncol)
        place = self.out.at[self.far, at]
        self.w.arrived(self.b[d], place, {"row": self.far})
        self.w.start(self.f[d], place, place, {"row": self.near})

    def end(self):
        for d in range(self.ncol):
            at = lax.rem(self.col - d + self.ncol, self.ncol)
            self.w.arrived(self.e[d], self.out.at[self.near, at], {"row": self.near})
            self.w.arrived(self.f[d], self.out.at[flip(self.near, 2), at], {"row": self.near})


def moved(src, mid, dst, sem):
    pltpu.make_async_copy(src, mid, sem).start()
    pltpu.make_async_copy(src, mid, sem).wait()
    pltpu.make_async_copy(mid, dst, sem).start()


def enter_kernel(nrow, ncol, ndp, fold, xs, cs, ws, ss, ts, xo, ho, co, wo, so, to_, xv, hv, cv, wv, sv, tv, send, recv, local):
    row, col, dp = (lax.axis_index(a) for a in ("row", "col", "dp"))
    w = Wires(send, recv)
    greet(nrow, ncol, ndp)
    tokens = xo.shape[3]

    def tokens_of(ref, to):
        return ref.at[:, pl.ds(pl.multiple_of(to * tokens, 128), tokens)]

    def before(ref, to):
        at = jnp.maximum(to * tokens - 128, 0)
        return ref.at[:, pl.ds(pl.multiple_of(at, 128), 128)]

    spreads = [
        Spread(w, ncol, lambda to: ss, so),
        Spread(w, ncol, lambda to: ts, to_),
        Spread(w, ncol, lambda to: before(xs, to), ho),
        Spread(w, ncol, lambda to: tokens_of(xs, to), xo),
        Spread(w, ncol, lambda to: tokens_of(cs, to), co),
    ]
    half, other = lax.rem(dp, 2), flip(dp, 1)
    hs = ws.shape[1] // 2
    mine, theirs = pl.ds(half * hs, hs), pl.ds((1 - half) * hs, hs)
    w1 = [w.slot() for _ in range(fold)]
    left = [w.slot() for _ in range(ncol)]
    right = [w.slot() for _ in range(ncol)]
    cross = [w.slot() for _ in range(2 * ncol)]

    for j in range(fold):
        tr, tc = col // fold, row * fold + j
        away = (tr != row) | (tc != col)
        for i in range(fold):
            w.start(
                w1[i], ws.at[j, mine], wo.at[tc, i, mine], {"row": tr, "col": tc},
                away & (lax.rem(col, fold) == i),
            )

        @pl.when(~away)
        def _():
            i = lax.rem(col, fold)
            moved(ws.at[j, mine], wv, wo.at[col, i, mine], local.at[0])
            pltpu.make_async_copy(wv, wo.at[col, i, mine], local.at[0]).wait()

    for s in spreads:
        s.begin()
    moved(ss, sv, so.at[row, col], local.at[1])
    moved(ts, tv, to_.at[row, col], local.at[5])
    moved(tokens_of(xs, col), xv, xo.at[row, col], local.at[2])
    moved(tokens_of(cs, col), cv, co.at[row, col], local.at[3])
    moved(before(xs, col), hv, ho.at[row, col], local.at[4])
    for s in spreads:
        s.forward(0)
    for i in range(fold):
        sr, sc = col // fold, row * fold + i

        @pl.when((sr != row) | (sc != col))
        def _():
            w.arrived(w1[i], wo.at[col, i, mine], {"row": sr, "col": sc})

    def unit(c, rows):
        return wo.at[c, :, rows]

    own = unit(col, mine)
    w.start(left[1], own, own, {"col": col + 1}, col + 1 < ncol)
    w.start(right[1], own, own, {"col": col - 1}, col >= 1)
    w.start(cross[0], own, own, {"dp": other})
    steps = [0] + order(ncol)[:0:-1]
    for at in range(1, ncol):
        d = steps[at]
        for s in spreads:
            s.forward(d)
        for s in spreads:
            s.relay(steps[at - 1])

        @pl.when(col >= at)
        def _():
            w.arrived(left[at], unit(col - at, mine), {"col": col - 1})

        got = unit(col - at, mine)
        w.start(left[min(at + 1, ncol - 1)], got, got, {"col": col + 1}, (col >= at) & (col + 1 < ncol))
        w.start(cross[at], got, got, {"dp": other}, col >= at)

        @pl.when(col + at < ncol)
        def _():
            w.arrived(right[at], unit(col + at, mine), {"col": col + 1})

        got = unit(col + at, mine)
        w.start(right[min(at + 1, ncol - 1)], got, got, {"col": col - 1}, (col + at < ncol) & (col >= 1))
        w.start(cross[ncol + at], got, got, {"dp": other}, col + at < ncol)
    for s in spreads:
        s.relay(steps[-1])
    w.arrived(cross[0], unit(col, theirs), {"dp": other})
    for at in range(1, ncol):

        @pl.when(col >= at)
        def _():
            w.arrived(cross[at], unit(col - at, theirs), {"dp": other})

        @pl.when(col + at < ncol)
        def _():
            w.arrived(cross[ncol + at], unit(col + at, theirs), {"dp": other})

    for s in spreads:
        s.end()
    pltpu.make_async_copy(sv, so.at[row, col], local.at[1]).wait()
    pltpu.make_async_copy(tv, to_.at[row, col], local.at[5]).wait()
    pltpu.make_async_copy(xv, xo.at[row, col], local.at[2]).wait()
    pltpu.make_async_copy(cv, co.at[row, col], local.at[3]).wait()
    pltpu.make_async_copy(hv, ho.at[row, col], local.at[4]).wait()
    w.finish()


ANYWHERE = pl.BlockSpec(memory_space=pl.ANY)
ONCHIP = pl.BlockSpec(memory_space=pltpu.VMEM)


def enter(nrow, ncol, ndp, fold, xs, cs, ws, ss, ts):
    own, tokens = xs.shape[0], xs.shape[1] // ncol
    slots = 20 * ncol + fold + 4 * ncol
    return pl.pallas_call(
        functools.partial(enter_kernel, nrow, ncol, ndp, fold),
        out_shape=[
            jax.ShapeDtypeStruct((nrow, ncol, own, tokens), BF16),
            jax.ShapeDtypeStruct((nrow, ncol, own, 128), BF16),
            jax.ShapeDtypeStruct((nrow, ncol, own, tokens), BF16),
            jax.ShapeDtypeStruct((ncol,) + ws.shape, BF16),
            jax.ShapeDtypeStruct((nrow, ncol) + ss.shape, BF16),
            jax.ShapeDtypeStruct((nrow, ncol) + ts.shape, BF16),
        ],
        in_specs=[ANYWHERE] * 5,
        out_specs=[ANYWHERE] * 6,
        scratch_shapes=[
            pltpu.VMEM((own, tokens), BF16),
            pltpu.VMEM((own, 128), BF16),
            pltpu.VMEM((own, tokens), BF16),
            pltpu.VMEM((ws.shape[1] // 2, ws.shape[2]), BF16),
            pltpu.VMEM(ss.shape, BF16),
            pltpu.VMEM(ts.shape, BF16),
            pltpu.SemaphoreType.DMA((24 * ncol + 8 + fold * fold,)),
            pltpu.SemaphoreType.DMA((slots,)),
            pltpu.SemaphoreType.DMA((6,)),
        ],
        compiler_params=pltpu.CompilerParams(collective_id=0, has_side_effects=True),
        name="enter",
    )(xs, cs, ws, ss, ts)


def shift_kernel(ncol, by, src, dst, buf, send, recv, local):
    col = lax.axis_index("col")
    to, back = col + by, col - by
    sends = (to >= 0) & (to < ncol)
    takes = (back >= 0) & (back < ncol)
    sem = pltpu.get_barrier_semaphore()

    @pl.when(takes)
    def _():
        pl.semaphore_signal(sem, 1, device_id={"col": back}, device_id_type=MESH)

    def wire():
        return pltpu.make_async_remote_copy(
            src_ref=src, dst_ref=buf, send_sem=send, recv_sem=recv,
            device_id={"col": to}, device_id_type=MESH,
        )

    @pl.when(sends)
    def _():
        pl.semaphore_wait(sem, 1)
        wire().start()

    @pl.when(~takes)
    def _():
        buf[...] = jnp.zeros_like(buf)

    @pl.when(takes)
    def _():
        wire().wait_recv()

    @pl.when(sends)
    def _():
        wire().wait_send()

    dst[...] = buf[...]


def shift(ncol, by, block, ident):
    return pl.pallas_call(
        functools.partial(shift_kernel, ncol, by),
        out_shape=jax.ShapeDtypeStruct(block.shape, block.dtype),
        in_specs=[ONCHIP],
        out_specs=ONCHIP,
        scratch_shapes=[
            pltpu.VMEM(block.shape, block.dtype),
            pltpu.SemaphoreType.DMA(()),
            pltpu.SemaphoreType.DMA(()),
            pltpu.SemaphoreType.DMA(()),
        ],
        compiler_params=pltpu.CompilerParams(collective_id=ident, has_side_effects=True),
        name=f"shift{ident}",
    )(block)


def gather_kernel(nrow, count, stat, scal, buf, send, recv):
    row = lax.axis_index("row")
    sem = pltpu.get_barrier_semaphore()
    for d in range(1, nrow):
        pl.semaphore_signal(sem, 1, device_id={"row": lax.rem(row + d, nrow)}, device_id_type=MESH)
    pl.semaphore_wait(sem, nrow - 1)
    w = Wires(send, recv)
    for d in range(1, nrow):
        w.start(d, stat, buf.at[d], {"row": lax.rem(row + d, nrow)})
    total = stat[...]
    for d in range(1, nrow):
        w.arrived(d, buf.at[d], {"row": lax.rem(row + d, nrow)})
        total = total + buf[d]
    w.finish()
    rootgate = lax.rsqrt(total[0:1] / count + NORM_EPSILON)
    pull = rootgate * rootgate * rootgate * total[1:2] / count
    first = lax.broadcasted_iota(jnp.int32, total.shape, 0) == 0
    scal[...] = jnp.where(first, rootgate, pull)


def gather_stat(nrow, count, stat):
    return pl.pallas_call(
        functools.partial(gather_kernel, nrow, count),
        out_shape=jax.ShapeDtypeStruct(stat.shape, F32),
        in_specs=[ONCHIP],
        out_specs=ONCHIP,
        scratch_shapes=[
            pltpu.VMEM((nrow,) + stat.shape, F32),
            pltpu.SemaphoreType.DMA((nrow,)),
            pltpu.SemaphoreType.DMA((nrow,)),
        ],
        compiler_params=pltpu.CompilerParams(collective_id=1, has_side_effects=True),
        name="stat",
    )(stat)


def leave_kernel(
    nrow, ncol, ndp, fold,
    gin, ginh, gw, gs, sm,
    go, gho, ho, so, smo,
    own, ra, rb, sb, sc, hown, hra, hrb, hsb, hsc, gwv, ry, sy, rz, fin, rdp, gsv, rs1, ss1, rs2, rs3, smb, smr, send, recv, local,
):
    row, col, dp = (lax.axis_index(a) for a in ("row", "col", "dp"))
    w = Wires(send, recv)
    greet(nrow, ncol, ndp)
    near, far, other, half = flip(row, 1), flip(row, 2), flip(dp, 1), lax.rem(dp, 2)
    cols = [lax.rem(col + d, ncol) for d in range(ncol)]
    from_col = [lax.rem(col - d + ncol, ncol) for d in range(ncol)]
    plan = order(ncol)[::-1]

    loads = {}

    def load(name, src, dst, at):
        loads[name] = pltpu.make_async_copy(src, dst, local.at[at])
        loads[name].start()

    a0 = [w.slot() for _ in range(ncol)]
    a1 = [w.slot() for _ in range(ncol)]
    b = [w.slot() for _ in range(ncol)]
    c_ = [w.slot() for _ in range(ncol)]
    y = [w.slot() for _ in range(ncol)]
    z = [w.slot() for _ in range(ncol)]
    tokens = gin.shape[3]
    ha, hb = [w.slot() for _ in range(2)], w.slot()
    hc = [w.slot() for _ in range(ncol)]
    w.start(ha[1], ginh.at[3], hra.at[1], {"row": near})
    w.start(ha[0], ginh.at[1], hra.at[0], {"row": near})
    load("h0", ginh.at[0], hown.at[0], 8)
    load("h1", ginh.at[2], hown.at[1], 9)
    place = pl.ds(pl.multiple_of(col * tokens, 128), tokens)
    for d in plan:
        w.start(a1[d], gin.at[3, cols[d]], ra.at[1, d], {"row": near})
        w.start(a0[d], gin.at[1, cols[d]], ra.at[0, d], {"row": near})
    for d in plan:
        w.start(y[d], gw.at[cols[d], 1 - half], ry.at[d], {"dp": other})
    load("own0", gin.at[0], own.at[0], 0)
    load("own1", gin.at[2], own.at[1], 1)
    load("gw", gw.at[:, half], gwv, 2)
    load("gs", gs.at[row], gsv, 3)
    load("sm", sm, smb.at[0], 4)
    s1 = [w.slot() for _ in range(nrow)]
    for d in range(1, nrow):
        to = lax.rem(row + d, nrow)
        w.start(s1[d], gs.at[to], rs1.at[d], {"row": to})

    loads["sm"].wait()
    hops = [("dp", bit) for bit in bits(ndp)] + [("col", bit) for bit in bits(ncol)]
    sms = [w.slot() for _ in hops]
    at = {"dp": dp, "col": col}

    def small_send(i):
        axis, bit = hops[i]
        w.start(sms[i], smb.at[i], smr.at[i], {axis: flip(at[axis], bit)})

    def small_take(i):
        axis, bit = hops[i]
        w.arrived(sms[i], smr.at[i], {axis: flip(at[axis], bit)})
        smb[i + 1] = smb[i] + smr[i]

    small_send(0)

    loads["own0"].wait()
    loads["own1"].wait()
    loads["h0"].wait()
    loads["h1"].wait()
    w.arrived(ha[1], hra.at[1], {"row": near})
    hsb[...] = (hown[1].astype(F32) + hra[1].astype(F32)).astype(BF16)
    w.start(hb, hsb, hrb, {"row": far})
    for d in plan:
        w.arrived(a1[d], ra.at[1, d], {"row": near})
        sb[d] = (own[1, cols[d]].astype(F32) + ra[1, d].astype(F32)).astype(BF16)
        w.start(b[d], sb.at[d], rb.at[d], {"row": far})
    small_take(0)
    if len(hops) > 1:
        small_send(1)

    loads["gw"].wait()

    def features(d):
        w.arrived(a0[d], ra.at[0, d], {"row": near})
        w.arrived(b[d], rb.at[d], {"row": far})
        total = own[0, cols[d]].astype(F32) + ra[0, d].astype(F32) + rb[d].astype(F32)
        sc[d] = total.astype(BF16)
        if d:
            w.start(c_[d], sc.at[d], go.at[:, place], {"col": cols[d]})
            w.start(hc[d], hsc.at[cols[d]], gho.at[col], {"col": cols[d]})
        else:
            pltpu.make_async_copy(sc.at[0], go.at[:, place], local.at[5]).start()
            pltpu.make_async_copy(hsc.at[col], gho.at[col], local.at[10]).start()

    def weights(d):
        w.arrived(y[d], ry.at[d], {"dp": other})
        sy[d] = (gwv[cols[d]].astype(F32) + ry[d].astype(F32)).astype(BF16)
        if d:
            w.start(z[d], sy.at[d], rz.at[d], {"col": cols[d]})

    w.arrived(ha[0], hra.at[0], {"row": near})
    w.arrived(hb, hrb, {"row": far})
    hsc[...] = (hown[0].astype(F32) + hra[0].astype(F32) + hrb[...].astype(F32)).astype(BF16)
    for d in plan:
        features(d)
        weights(d)

    loads["gs"].wait()
    total = gsv[...].astype(F32)
    for d in range(1, nrow):
        w.arrived(s1[d], rs1.at[d], {"row": lax.rem(row - d + nrow, nrow)})
        total = total + rs1[d].astype(F32)
    ss1[...] = total.astype(BF16)
    part = so.shape[0]
    s2 = [w.slot() for _ in range(ncol)]
    for d in plan[:-1]:
        w.start(s2[d], ss1.at[pl.ds(cols[d] * part, part)], rs2.at[d], {"col": cols[d]})
    for i in range(1, len(hops)):
        small_take(i)
        if i + 1 < len(hops):
            small_send(i + 1)
    last = len(hops)
    s4 = [w.slot() for _ in range(nrow)]
    for d in range(1, nrow):
        w.start(s4[d], smb.at[last], smo.at[row], {"row": lax.rem(row + d, nrow)})
    pltpu.make_async_copy(smb.at[last], smo.at[row], local.at[6]).start()

    total = ss1[pl.ds(pl.multiple_of(col * part, part), part), :].astype(F32)
    for d in range(1, ncol):
        w.arrived(s2[d], rs2.at[d], {"col": from_col[d]})
        total = total + rs2[d].astype(F32)
    rs3[0] = total
    s3 = [w.slot() for _ in bits(ndp)]
    for i, bit in enumerate(bits(ndp)):
        w.start(s3[i], rs3.at[2 * i], rs3.at[2 * i + 1], {"dp": flip(dp, bit)})
        w.arrived(s3[i], rs3.at[2 * i + 1], {"dp": flip(dp, bit)})
        total = total + rs3[2 * i + 1]
        rs3[2 * i + 2] = total
    so[...] = total

    total = sy[0].astype(F32)
    for d in range(1, ncol):
        w.arrived(z[d], rz.at[d], {"col": from_col[d]})
        total = total + rz[d].astype(F32)
    if ndp > 2:
        fin[...] = total.astype(BF16)
        for i, bit in enumerate(bits(ndp)[1:]):
            slot = w.slot()
            rdp[2 * i] = total
            w.start(slot, rdp.at[2 * i], rdp.at[2 * i + 1], {"dp": flip(dp, bit)})
            w.arrived(slot, rdp.at[2 * i + 1], {"dp": flip(dp, bit)})
            total = total + rdp[2 * i + 1]
    fin[...] = total.astype(BF16)
    hs = fin.shape[0]
    sh = ho.shape[3]
    mine, theirs = pl.ds(half * hs, hs), pl.ds((1 - half) * hs, hs)
    count = ho.shape[0]
    h1 = [[w.slot() for _ in range(fold)] for _ in range(count)]
    h2 = [[w.slot() for _ in range(fold)] for _ in range(count)]
    for i in range(fold):
        orow, ocol = col // fold, row * fold + i
        away = (orow != row) | (ocol != col)
        for p in range(count):
            src = fin.at[:, pl.ds((p * fold + i) * sh, sh)]
            for j in range(fold):
                this = lax.rem(col, fold) == j
                dst = ho.at[p, j, mine]
                w.start(h1[p][j], src, dst, {"row": orow, "col": ocol}, away & this)

                @pl.when(~away & this)
                def _():
                    copy = pltpu.make_async_copy(src, dst, local.at[7])
                    copy.start()
                    copy.wait()

    for j in range(fold):
        srow, scol = col // fold, row * fold + j
        for p in range(count):
            got = ho.at[p, j, mine]

            @pl.when((srow != row) | (scol != col))
            def _():
                w.arrived(h1[p][j], got, {"row": srow, "col": scol})

            w.start(h2[p][j], got, got, {"dp": other})
    for j in range(fold):
        for p in range(count):
            w.arrived(h2[p][j], ho.at[p, j, theirs], {"dp": other})
    for d in range(1, ncol):
        came = pl.ds(pl.multiple_of(from_col[d] * tokens, 128), tokens)
        w.arrived(c_[d], go.at[:, came], {"col": from_col[d]})
        w.arrived(hc[d], gho.at[from_col[d]], {"col": from_col[d]})
    for d in range(1, nrow):
        w.arrived(s4[d], smo.at[lax.rem(row - d + nrow, nrow)], {"row": lax.rem(row - d + nrow, nrow)})
    pltpu.make_async_copy(sc.at[0], go.at[:, place], local.at[5]).wait()
    pltpu.make_async_copy(hsc.at[col], gho.at[col], local.at[10]).wait()
    pltpu.make_async_copy(smb.at[last], smo.at[row], local.at[6]).wait()
    w.finish()


def leave(nrow, ncol, ndp, fold, gin, ginh, gw, gs, sm):
    unit = gin.shape[2:]
    hs, wide = gw.shape[2:]
    sh = wide // 2 // fold
    part = gs.shape[1] // ncol
    nb, nd = len(bits(ndp)), len(bits(ndp)) + len(bits(ncol))
    slots = 8 * ncol + 2 * nrow + nd + 2 * nb + 6 * fold + 12
    edge = ginh.shape[1:]
    return pl.pallas_call(
        functools.partial(leave_kernel, nrow, ncol, ndp, fold),
        out_shape=[
            jax.ShapeDtypeStruct((unit[0], ncol * unit[1]), BF16),
            jax.ShapeDtypeStruct(edge, BF16),
            jax.ShapeDtypeStruct((2, fold, 2 * hs, sh), BF16),
            jax.ShapeDtypeStruct((part, gs.shape[2]), F32),
            jax.ShapeDtypeStruct((nrow,) + sm.shape, F32),
        ],
        in_specs=[ANYWHERE] * 5,
        out_specs=[ANYWHERE, ANYWHERE, ANYWHERE, ONCHIP, ANYWHERE],
        scratch_shapes=[
            pltpu.VMEM((2, ncol) + unit, BF16),
            pltpu.VMEM((2, ncol) + unit, BF16),
            pltpu.VMEM((ncol,) + unit, BF16),
            pltpu.VMEM((ncol,) + unit, BF16),
            pltpu.VMEM((ncol,) + unit, BF16),
            pltpu.VMEM((2,) + edge, BF16),
            pltpu.VMEM((2,) + edge, BF16),
            pltpu.VMEM(edge, BF16),
            pltpu.VMEM(edge, BF16),
            pltpu.VMEM(edge, BF16),
            pltpu.VMEM((ncol, hs, wide), BF16),
            pltpu.VMEM((ncol, hs, wide), BF16),
            pltpu.VMEM((ncol, hs, wide), BF16),
            pltpu.VMEM((ncol, hs, wide), BF16),
            pltpu.VMEM((hs, wide), BF16),
            pltpu.VMEM((max(2 * nb - 2, 1), hs if ndp > 2 else 8, wide), F32),
            pltpu.VMEM(gs.shape[1:], BF16),
            pltpu.VMEM((nrow,) + gs.shape[1:], BF16),
            pltpu.VMEM(gs.shape[1:], BF16),
            pltpu.VMEM((ncol, part, gs.shape[2]), BF16),
            pltpu.VMEM((2 * nb + 1, part, gs.shape[2]), F32),
            pltpu.VMEM((nd + 1,) + sm.shape, F32),
            pltpu.VMEM((nd,) + sm.shape, F32),
            pltpu.SemaphoreType.DMA((9 * ncol + 20 + nd + 2 * nb + 6 * fold * fold,)),
            pltpu.SemaphoreType.DMA((slots,)),
            pltpu.SemaphoreType.DMA((11,)),
        ],
        compiler_params=pltpu.CompilerParams(
            collective_id=2, has_side_effects=True, vmem_limit_bytes=60 * 1024 * 1024
        ),
        name="leave",
    )(gin, ginh, gw, gs, sm)


def finish_kernel(x_ref, c_ref, r_ref, g_ref, h_ref, res_ref, gin_ref):
    step, steps = pl.program_id(0), pl.num_programs(0)
    tokens = x_ref.shape[1]
    res_ref[...] = x_ref[...].astype(F32) + r_ref[...].astype(F32)
    gin_ref[...] = c_ref[...].astype(F32) + g_ref[...].astype(F32)
    at = slice(tokens - 128, tokens)

    @pl.when(step < steps - 1)
    def _():
        gin_ref[:, at] += h_ref[0].astype(F32)


def adam_kernel(*refs):
    for i in range(len(refs) // 8):
        grad_ref, moment_ref, square_ref, weight_ref = refs[4 * i : 4 * i + 4]
        outs = refs[len(refs) // 2 + 4 * i : len(refs) // 2 + 4 * i + 4]
        grad = grad_ref[...].astype(F32)
        outs[0][...] = grad
        for out, value in zip(
            outs[1:], adamw_step(grad, moment_ref[...], square_ref[...], weight_ref[...].astype(F32))
        ):
            out[...] = value


def adam(sets, steps):
    ins, outs = [], []
    for arrays in sets:
        shape = arrays[1].shape
        block = (shape[0] // steps,) + shape[1:]
        ins += [(array, block, 0) for array in arrays]
        outs += [(shape, F32, block, 0)] * 4
    return call(adam_kernel, steps, ins, outs, [], False, "adam", 5)


def call(kernel, steps, ins, outs, scratch, reverse, name, cost, ident=None):
    def spec(block, axis, base=None):
        def index(step):
            at = steps - 1 - step if reverse else step
            return tuple(
                at if a == axis else (base[a] if base else 0) for a in range(len(block))
            )

        return pl.BlockSpec(block, index) if block is not None else ANYWHERE

    return pl.pallas_call(
        kernel,
        grid=(steps,),
        in_specs=[spec(*item[1:]) for item in ins],
        out_specs=[spec(block, axis) for _, _, block, axis in outs],
        out_shape=[jax.ShapeDtypeStruct(shape, dtype) for shape, dtype, _, _ in outs],
        scratch_shapes=scratch,
        compiler_params=pltpu.CompilerParams(
            dimension_semantics=("arbitrary",),
            vmem_limit_bytes=60 * 1024 * 1024,
            collective_id=ident,
            has_side_effects=ident is not None,
        ),
        cost_estimate=pl.CostEstimate(
            flops=int(cost * 1e9), bytes_accessed=int(cost * 1e6), transcendentals=0
        ),
        name=name,
    )(*[item[0] for item in ins])


def whole(array):
    return (array, array.shape, None)


def raw(array):
    return (array, None, None)


def part(array, block, base):
    return (array, block, None, base)


def lanes(array):
    return (array, array.shape[:-1] + (GROUP,), array.ndim - 1)


def sublanes(array, rows=GROUP):
    return (array, array.shape[:-2] + (rows,) + array.shape[-1:], array.ndim - 2)


def each(array):
    return (array, (1,) + array.shape[1:], 0)


def out_whole(shape, dtype):
    return (shape, dtype, shape, None)


def out_sub(shape, dtype, rows=GROUP):
    return (shape, dtype, shape[:-2] + (rows,) + shape[-1:], len(shape) - 2)


def out_lanes(shape, dtype):
    return (shape, dtype, shape[:-1] + (GROUP,), len(shape) - 1)


def out_each(shape, dtype):
    return (shape, dtype, (1,) + shape[1:], 0)


def adamw_step(grad, moment, square, weight):
    first_new = BETA_FIRST * moment + (1.0 - BETA_FIRST) * grad
    second_new = BETA_SECOND * square + (1.0 - BETA_SECOND) * grad * grad
    fix_first = 1.0 - BETA_FIRST**STEP
    fix_second = 1.0 - BETA_SECOND**STEP
    delta = -LEARN_RATE * (
        first_new / fix_first / (jnp.sqrt(second_new / fix_second) + ADAM_EPSILON)
        + WEIGHT_DECAY * weight
    )
    return (first_new, second_new, delta)


def local(
    inputs, segments, cotangent, pregain, innerweight, rateweight, stateweight, innerconv, stateconv, headparams,
    postgain, outweight, *moments,
):
    nrow, ncol, ndp = (lax.axis_size(a) for a in ("row", "col", "dp"))
    row, col = lax.axis_index("row"), lax.axis_index("col")
    length, own = inputs.shape[1], inputs.shape[2]
    width = own * nrow * ncol
    stored = innerweight.shape[1]
    total_heads = stored * ncol
    heads = total_heads // nrow
    hl = heads * HEADP
    count = total_heads * HEADP
    tokens = length // ncol
    steps = tokens // GROUP
    depth = width // nrow
    fold = ncol // nrow
    hops = (MOST - 2) // tokens + 1

    window = jnp.pad(segments[0], (HALO, HALO), constant_values=-1)
    window = lax.dynamic_slice_in_dim(window, col * tokens, tokens + 2 * HALO, 0)
    mine = window[HALO : HALO + tokens]
    flags = [mine]
    for j in (-1, -2, -3, 1, 2, 3):
        flags.append(window[HALO + j : HALO + j + tokens] == mine)
    before = window[HALO - 1 : HALO - 1 + tokens : GROUP]
    flags.append((mine.reshape(steps, GROUP) == before[:, None]).reshape(tokens))
    tok = jnp.stack([f.astype(F32) for f in flags])
    hmask = jnp.stack([(window[j : j + HALO] == window[:HALO]).astype(F32) for j in range(8)], 1)
    hmask = jnp.pad(hmask, ((0, 0), (0, 120)))

    block_heads = headparams.shape[1]
    xs, cs = inputs[0].T, cotangent[0].T
    smalls = [pregain, innerconv, headparams, postgain, rateweight]
    flat = jnp.concatenate([a.reshape(-1) for a in smalls])
    ss = jnp.pad(flat, (0, -flat.size % 2048)).reshape(-1, 128)
    sub = depth // fold
    sh = stored * HEADP
    split = innerweight.reshape(depth, stored, 2, HEADP)
    ws = jnp.concatenate(
        [
            split[:, :, 0].reshape(depth, sh),
            split[:, :, 1].reshape(depth, sh),
            outweight.reshape(sh, depth).T,
        ],
        1,
    ).reshape(fold, sub, 3 * sh)

    x, xh, cot, weights, gathered, wstate = enter(nrow, ncol, ndp, fold, xs, cs, ws, ss, stateweight)

    if fold > 1:
        weights = weights.reshape(ncol, fold, sub, 3, sh).transpose(0, 2, 3, 1, 4)
    weights = weights.reshape(width, 3 * hl)
    x, xh, cot = (a.reshape(width, a.shape[3]) for a in (x, xh, cot))
    gathered = gathered.reshape(nrow, ncol, -1)
    parts, at = [], 0
    for array in smalls:
        parts.append(gathered[:, :, at : at + array.size])
        at += array.size
    gain = jnp.broadcast_to(parts[0].reshape(width, 1).astype(F32), (width, 128))
    iconv = parts[1].reshape(nrow, ncol, 5, block_heads, HEADP).transpose(2, 1, 0, 3, 4)
    iconv = lax.dynamic_slice_in_dim(iconv.reshape(5, count), row * hl, hl, 1).astype(F32)
    hp = parts[2].reshape(nrow, ncol, 3, block_heads).transpose(2, 1, 0, 3)
    hp = lax.dynamic_slice_in_dim(hp.reshape(3, total_heads), row * heads, heads, 1).astype(F32)
    post = parts[3].reshape(nrow, ncol, block_heads * HEADP).transpose(1, 0, 2)
    post = lax.dynamic_slice_in_dim(post.reshape(1, count), row * hl, hl, 1).astype(F32)
    wrate = parts[4].reshape(nrow, ncol, depth, stored)
    wrate = wrate.transpose(1, 3, 0, 2).reshape(total_heads, width)
    wrate = lax.dynamic_slice_in_dim(wrate, row * heads, heads, 0)
    wrate = jnp.pad(wrate, ((0, 16 - heads), (0, 0)))
    wstate = wstate.reshape(width, 2 * NSTATE)
    sconv = stateconv.astype(F32)
    head = jnp.broadcast_to(
        jnp.concatenate([-jnp.exp(hp[0]), hp[1]])[:, None], (2 * heads, 128)
    )
    skip = jnp.repeat(hp[2], HEADP)[None]

    spread = jnp.repeat(jnp.eye(heads, dtype=BF16), HEADP, 1)
    spread = jnp.concatenate([spread, spread], 0)
    triangle = jnp.triu(jnp.ones((GROUP, GROUP), BF16))
    ns2 = 2 * NSTATE
    x_in, xh_in, cot_in = lanes(x), whole(xh), lanes(cot)
    wmain = part(weights, (width, 2 * hl), (0, 0))
    woutt = part(weights, (width, hl), (0, 2))

    gate, pre, st, uv, us, bc, rows, states, prod, fin, total, preh, sth, rinvh = call(
        fwd1_kernel,
        steps,
        [x_in, xh_in, whole(gain), wmain, whole(wstate), whole(wrate), lanes(tok), whole(head),
         whole(iconv), whole(sconv), whole(triangle), whole(spread)],
        [out_sub((tokens, hl), F32), out_sub((tokens, hl), F32), out_sub((tokens, ns2), BF16),
         out_sub((tokens, hl), F32), out_sub((tokens, ns2), F32), out_sub((tokens, ns2), BF16),
         out_lanes((4 * heads, tokens), F32),
         out_each((steps, NSTATE, hl), BF16), out_each((steps, 8, hl), F32),
         out_whole((NSTATE, hl), BF16), out_whole((8, hl), F32), out_whole((HALO, hl), BF16),
         out_whole((HALO, ns2), BF16), out_whole((HALO, 128), F32)],
        [pltpu.VMEM((GROUP + 8, hl + ns2), F32), pltpu.VMEM((NSTATE, hl), F32), pltpu.VMEM((8, hl), F32)],
        False,
        "fwd1",
        22,
    )
    total = total[0:1]
    sin = shift(ncol, 1, fin, 3)
    for _ in range(hops - 1):
        sin = shift(ncol, 1, (fin.astype(F32) + total * sin.astype(F32)).astype(BF16), 3)

    scan, out, dn, stat = call(
        fwd2_kernel,
        steps,
        [sublanes(gate), sublanes(uv), sublanes(bc), lanes(rows), lanes(tok), each(states), each(prod), whole(sin),
         cot_in, whole(post), whole(skip), woutt, whole(spread)],
        [out_sub((tokens, hl), F32), out_lanes((nrow, depth, tokens), BF16), out_sub((tokens, hl), BF16),
         out_lanes((8, tokens), F32)],
        [],
        False,
        "fwd2",
        18,
    )
    scal = gather_stat(nrow, count, stat)

    dy, dg, leaving, prodb, first, gout, sums, root = call(
        bwd1_kernel,
        steps,
        [sublanes(gate), sublanes(uv), sublanes(bc), lanes(rows), lanes(tok), sublanes(scan), sublanes(dn),
         lanes(scal), cot_in, whole(post), whole(skip), whole(spread)],
        [out_sub((tokens, hl), BF16), out_sub((tokens, hl), BF16), out_each((steps, NSTATE, hl), BF16),
         out_each((steps, 8, hl), F32), out_whole((NSTATE, hl), BF16), out_whole((width, hl), BF16),
         out_whole((16, hl), F32), out_lanes((8, tokens), F32)],
        [pltpu.VMEM((NSTATE, hl), F32), pltpu.VMEM((8, hl), F32), pltpu.VMEM((width, hl), F32)],
        True,
        "bwd1",
        15,
    )
    din = shift(ncol, -1, first, 4)
    for _ in range(hops - 1):
        din = shift(ncol, -1, (first.astype(F32) + total * din.astype(F32)).astype(BF16), 4)

    hs = sub // 2
    home, ghout, gin, ginh, gw, gs, gr, gk, gh, gp = call(
        functools.partial(bwd2_kernel, (nrow, ncol, ndp, fold)),
        steps,
        [x_in, xh_in, whole(gain), wmain, whole(wstate), whole(wrate), lanes(tok), whole(head),
         whole(hmask), whole(rinvh), whole(iconv), whole(sconv), whole(triangle), whole(spread), whole(skip),
         sublanes(pre), sublanes(st), whole(preh), whole(sth), sublanes(uv), sublanes(us), sublanes(bc), lanes(rows),
         each(states), each(prod), whole(sin), sublanes(scan), sublanes(dy), sublanes(dg),
         each(leaving), each(prodb), whole(din), lanes(root), whole(scal),
         raw(out.reshape(nrow, ncol, own, tokens)), raw(gout.reshape(ncol, 2, hs, hl))],
        [((own, length), BF16, None, None), ((fold, sub, sh), BF16, None, None),
         out_lanes((nrow, depth, tokens), BF16), out_whole((nrow, depth, 128), BF16), out_whole((width, 2 * hl), BF16),
         out_whole((width, ns2), BF16), out_whole((16, width), F32), out_whole((40, hl + ns2), F32),
         out_whole((2 * heads, GROUP), F32), out_whole((width, 128), F32)],
        [pltpu.VMEM((GROUP + 8, hl + ns2), F32), pltpu.VMEM((width, 2 * hl + ns2), F32)]
        + delivery_scratch(nrow, ncol, ndp, fold, own, tokens, hs, hl),
        True,
        "bwd2",
        50,
        5,
    )

    gk = jnp.sum(gk.reshape(5, 8, -1), 1)
    gh = jnp.sum(gh, 1).reshape(2, heads)
    sums = jnp.sum(sums.reshape(2, 8, hl), 1)
    gskip = jnp.sum(sums[1].reshape(1, heads, HEADP), 2)
    small = [
        jnp.sum(gp, 1),
        gr[:heads],
        gk[:, :hl],
        gk[:, hl:],
        jnp.concatenate([gh, gskip]),
        sums[0],
    ]
    flat = jnp.concatenate([a.reshape(-1) for a in small])
    flat = jnp.pad(flat, (0, -flat.size % 1024)).reshape(-1, 128)
    gin, edge, ghome, gstate, flat = leave(
        nrow, ncol, ndp, fold,
        gin.reshape(nrow, ncol, own, tokens), ginh.reshape(nrow, ncol, own, 128),
        gw.reshape(ncol, 2, hs, 2 * hl), gs.reshape(nrow, depth, ns2), flat,
    )
    edge = jnp.concatenate([edge[1:], edge[:1]], 0)
    result, grad_input = call(
        finish_kernel,
        ncol,
        [(a, (own, tokens), 1) for a in (xs, cs, home, gin)] + [each(edge)],
        [((own, length), F32, (own, tokens), 1)] * 2,
        [],
        False,
        "finish",
        5,
    )
    result, grad_input = result.T[None], grad_input.T[None]

    ghome = ghome.reshape(2, depth, stored, HEADP)
    ginner = jnp.concatenate([ghome[0], ghome[1]], 2)
    gout = ghout.reshape(depth, sh).T.reshape(stored, HEADP, depth)
    updated = adam(
        [(ginner, moments[2], moments[3], innerweight), (gout, moments[16], moments[17], outweight)], 4
    )
    flat = flat.reshape(nrow, -1)
    parts, at = [], 0
    for array in small:
        parts.append(flat[:, at : at + array.size].reshape((nrow,) + array.shape))
        at += array.size
    feature = (row * ncol + col) * own
    block = col * nrow + row
    gpre = lax.dynamic_slice_in_dim(jnp.sum(parts[0], 0).reshape(-1), feature, own, 0)
    grate = lax.dynamic_slice(
        parts[1], (col // fold, (col % fold) * stored, row * depth), (1, stored, depth)
    )[0].T
    giconv = parts[2].transpose(1, 0, 2).reshape(5, count)
    wide = block_heads * HEADP
    giconv = lax.dynamic_slice_in_dim(giconv, block * wide, wide, 1)
    giconv = giconv.reshape(5, block_heads, HEADP)
    gsconv = jnp.sum(parts[3], 0)
    ghead = parts[4].transpose(1, 0, 2).reshape(3, total_heads)
    ghead = lax.dynamic_slice_in_dim(ghead, block * block_heads, block_heads, 1)
    gpost = lax.dynamic_slice_in_dim(parts[5].reshape(count), block * wide, wide, 0)
    gpost = gpost.reshape(block_heads, HEADP)

    grads = (gpre, None, grate, gstate, giconv, gsconv, ghead, gpost, None)
    params = (
        pregain, innerweight, rateweight, stateweight, innerconv, stateconv, headparams, postgain, outweight,
    )
    ready = {1: updated[:4], 8: updated[4:]}
    outputs = [result, grad_input]
    for i, (grad, param) in enumerate(zip(grads, params)):
        if i in ready:
            outputs.extend(ready[i])
            continue
        outputs.append(grad)
        outputs.extend(adamw_step(grad, moments[2 * i], moments[2 * i + 1], param.astype(F32)))
    return tuple(outputs)


def solution(mesh):
    tokens = P("dp", None, ("row", "col"))
    weights = (
        P(("row", "col")),
        P("row", "col", None),
        P("row", "col"),
        P(("row", "col"), None),
        P(None, ("col", "row"), None),
        P(),
        P(None, ("col", "row")),
        P(("col", "row"), None),
        P("col", None, "row"),
    )
    return jax.shard_map(
        local,
        mesh=mesh,
        in_specs=(tokens, P("dp", None), tokens)
        + weights
        + tuple(w for w in weights for _ in range(2)),
        out_specs=(tokens, tokens) + tuple(w for w in weights for _ in range(4)),
        check_vma=False,
    )
```
